128 devices in a mesh: grp: 4 (over z), kv: 16 (over x, y), tp: 2 (over core).
Axes of the slice: x: 4, y: 4, z: 4, core: 2. Of those that a mesh axis runs over, the one named last changes fastest.
Arguments:
- hidden_states: bfloat16 [512, 4096], P('grp', 'kv'), may hold values from -6 to 6
- attn_gain: float32 [4096], P('kv'), may hold values from 0.25 to 1.75
- mlp_gain: float32 [4096], replicated, may hold values from 0.25 to 1.75
- w_query: bfloat16 [4096, 4096], P('kv', 'tp'), may hold values from -0.09375 to 0.09375
- w_out: bfloat16 [32, 128, 4096], P('tp', 'kv'), may hold values from -1 to 1
- w_gate: bfloat16 [4096, 14336], P(None, ('kv', 'tp')), may hold values from -0.09375 to 0.09375
- w_up: bfloat16 [4096, 14336], P(None, ('kv', 'tp')), may hold values from -0.09375 to 0.09375
- w_down: bfloat16 [14336, 4096], P(('kv', 'tp')), may hold values from -0.046875 to 0.046875
- kv_pool: bfloat16 [1024, 2, 128, 1024], P(('grp', 'kv'), None, None, 'tp'), may hold values from -110 to 110
- resident_cache: bfloat16 [4, 128, 2, 128, 1024], P('grp', 'kv', None, None, 'tp'), may hold values from -110 to 110
- resident_slot: int32 [4, 128], P('grp', 'kv'), may hold values from 0 to 127
- resident_len: int32 [4, 128], P('grp', 'kv'), may hold values from 1 to 128
- new_owner: int32 [4, 256], replicated, may hold values from 0 to 63, as said below
- new_local: int32 [4, 256], replicated, may hold values from 0 to 15
- new_slot: int32 [4, 256], P('grp', 'kv'), may hold values from 0 to 127
- new_len: int32 [4, 256], P('grp', 'kv'), may hold values from 1 to 128
- token_kv: bfloat16 [512, 2, 1024], P('grp', None, 'tp'), may hold values from -6 to 6
Outputs:
- mixed: bfloat16 [512, 4096], P(('grp', 'kv', 'tp'))
- new_cache: bfloat16 [4, 256, 2, 128, 1024], P('grp', 'kv', None, None, 'tp')
The draws below stay inside these ranges and needn't reach their ends.
Inputs may be any that keep to these rules, and one draw needn't show every extreme that they name: New page c of group g is kept by the device of kv index c // 16 of group g and comes from the device whose index along grp+kv is new_owner[g, c]; every decode device receives exactly 4 new pages from the owners of each grp index; no owner sends more than 1 pages to the devices of one kv index over all groups, so at most 1 to one device; every owner sends each of its 16 pages exactly once.
All inputs are finite; a program needn't handle non-finite values.
Results may differ from the reference program's by a relative error of at most 0.018.
Values may be sent and summed in bfloat16 or wider, within the bound.
A program may use at most 128 MiB of HBM per device.

```python
import jax
import jax.numpy as jnp
from jax import lax

D = 4096
HEADS = 32
KV_HEADS = 8
HEAD_DIM = 128
FF = 14336
PAGE = 128
NPR = 4
SLOT_G = 128
GROUPS = 4
KV_RANKS = 16
SLOTS = 512
NEW_DEV = 16
CAP1 = 1
POOL = 1024
CACHE_G = 128
NEWC = 256


def page_values(key, count):
    width = KV_HEADS * HEAD_DIM
    values = jnp.clip(jax.random.normal(key, (count, 2, PAGE, width), jnp.float32), -6.0, 6.0)
    return values.astype(jnp.bfloat16)


def draw_kv_pool(key, part):
    return page_values(jax.random.fold_in(key, 3), POOL)


def draw_resident_cache(key, part):
    values = page_values(jax.random.fold_in(key, 5), GROUPS * CACHE_G)
    return values.reshape(GROUPS, CACHE_G, 2, PAGE, KV_HEADS * HEAD_DIM)


def batch_perms(key, count, length):
    subkeys = jax.random.split(key, count)
    return jax.vmap(lambda subkey: jax.random.permutation(subkey, length))(subkeys)


def route_tables(key):
    key = jax.random.fold_in(key, 11)
    keys = jax.random.split(key, 4)
    cap = CAP1
    col_perm = batch_perms(keys[0], GROUPS * KV_RANKS, KV_RANKS).reshape(GROUPS, KV_RANKS, KV_RANKS)
    shift = jax.random.randint(keys[1], (GROUPS, KV_RANKS), 0, KV_RANKS)
    dest_perm = batch_perms(keys[2], GROUPS * KV_RANKS, NEW_DEV).reshape(GROUPS, KV_RANKS, NEW_DEV)
    local_perm = batch_perms(keys[3], GROUPS * KV_RANKS, NEW_DEV)
    src_grp = jnp.arange(GROUPS).reshape(GROUPS, 1, 1, 1)
    dst_col = jnp.arange(KV_RANKS).reshape(1, KV_RANKS, 1, 1)
    dst_grp = jnp.arange(GROUPS).reshape(1, 1, GROUPS, 1)
    within = jnp.arange(NPR).reshape(1, 1, 1, NPR)
    flat = dst_grp * NPR + within
    turned = (flat + shift[src_grp, dst_col] * cap) % NEW_DEV
    block = turned // cap
    place = turned % cap
    src_col = col_perm[src_grp, dst_col, block]
    owner = src_grp * KV_RANKS + src_col
    local_ids = local_perm[owner, dst_col * cap + place]
    slot_in = dest_perm[dst_grp, dst_col, src_grp * NPR + within]
    column = dst_col * NEW_DEV + slot_in
    full_rows = jnp.broadcast_to(dst_grp, owner.shape)
    owners = jnp.zeros((GROUPS, KV_RANKS * NEW_DEV), jnp.int32).at[full_rows, column].set(owner.astype(jnp.int32))
    locals_out = jnp.zeros((GROUPS, KV_RANKS * NEW_DEV), jnp.int32).at[full_rows, column].set(local_ids.astype(jnp.int32))
    return (owners, locals_out)


def draw_new_owner(key, part):
    return route_tables(key)[0]


def draw_new_local(key, part):
    return route_tables(key)[1]


def set_ends(drawn, key, least, high):
    longest = drawn.shape.index(max(drawn.shape))
    spots = []
    for shift in (0, 1):
        where = [jax.random.randint(jax.random.fold_in(key, axis), (), 0, length) for axis, length in enumerate(drawn.shape)]
        where[longest] = (where[longest] + shift) % drawn.shape[longest]
        spots.append(tuple(where))
    return drawn.at[spots[0]].set(least).at[spots[1]].set(high)


def block_levels(key, dims, shards, smallest, largest):
    factor_of, own = 1.0, jax.random.fold_in(key, 6)
    for position, blocks in shards:
        steps = jnp.exp(jax.random.uniform(jax.random.fold_in(own, position), (blocks,), jnp.float32, smallest / len(shards), largest / len(shards)))
        factor_of = factor_of * jnp.repeat(steps, dims[position] // blocks).reshape([-1 if axis == position else 1 for axis in range(len(dims))])
    return factor_of


def gaussian(stream_key, shape, spread, most, pieces=(), held_as=jnp.bfloat16):
    values = spread * jax.random.normal(stream_key, shape, jnp.float32)
    if pieces:
        values = values * block_levels(stream_key, shape, pieces, -0.22, 0.18)
    return jnp.clip(values, -most, most).astype(held_as)


def setup_inputs(seed: int = 0) -> dict:
    key_list = jax.random.split(jax.random.key(seed), 18)
    return {
        "hidden_states": gaussian(key_list[0], (SLOTS, D), 1.0, 6.0, ((0, 4), (1, 16))),
        "attn_gain": jnp.clip(1.0 + 0.15 * jax.random.normal(key_list[1], (D,), jnp.float32), 0.25, 1.75),
        "mlp_gain": jnp.clip(1.0 + 0.15 * jax.random.normal(key_list[2], (D,), jnp.float32), 0.25, 1.75),
        "w_query": gaussian(key_list[3], (D, HEADS * HEAD_DIM), D ** -0.5, 0.09375, ((0, 16), (1, 2))),
        "w_out": gaussian(key_list[4], (HEADS, HEAD_DIM, D), HEADS ** -0.5, 1.0, ((0, 2), (1, 16))),
        "w_gate": gaussian(key_list[5], (D, FF), D ** -0.5, 0.09375, ((1, 32),)),
        "w_up": gaussian(key_list[6], (D, FF), D ** -0.5, 0.09375, ((1, 32),)),
        "w_down": gaussian(key_list[7], (FF, D), FF ** -0.5, 0.046875, ((0, 32),)),
        "kv_pool": draw_kv_pool(jax.random.fold_in(key_list[17], 71), 0),
        "resident_cache": draw_resident_cache(jax.random.fold_in(key_list[17], 71), 0),
        "resident_slot": set_ends(jax.random.randint(key_list[10], (GROUPS, CACHE_G), 0, SLOT_G), jax.random.fold_in(key_list[10], 1), 0, SLOT_G - 1).astype(jnp.int32),
        "resident_len": set_ends(jax.random.randint(key_list[11], (GROUPS, CACHE_G), 1, PAGE + 1), jax.random.fold_in(key_list[11], 1), 1, PAGE).astype(jnp.int32),
        "new_owner": draw_new_owner(jax.random.fold_in(key_list[17], 71), 0),
        "new_local": draw_new_local(jax.random.fold_in(key_list[17], 71), 0),
        "new_slot": set_ends(jax.random.randint(key_list[14], (GROUPS, NEWC), 0, SLOT_G), jax.random.fold_in(key_list[14], 1), 0, SLOT_G - 1).astype(jnp.int32),
        "new_len": set_ends(jax.random.randint(key_list[15], (GROUPS, NEWC), 1, PAGE + 1), jax.random.fold_in(key_list[15], 1), 1, PAGE).astype(jnp.int32),
        "token_kv": gaussian(key_list[16], (SLOTS, 2, KV_HEADS * HEAD_DIM), 1.0, 6.0, ((0, 4), (2, 2))),
    }


neg_fill = -1e+30
norm_eps = 1e-05

def local_partials(query, resident, arrived, res_slot, res_len, arr_slot, arr_len, token_kv, first):
    pages = jnp.concatenate([resident, arrived], axis=0)
    owner_slot = jnp.concatenate([res_slot, arr_slot]).astype(jnp.int32)
    filled = jnp.concatenate([res_len, arr_len]).astype(jnp.int32)
    count = pages.shape[0]
    tokens = pages.shape[2]
    kv_here = pages.shape[3] // HEAD_DIM
    slots = query.shape[0]
    ratio = HEADS // KV_HEADS
    keys = pages[:, 0].astype(jnp.float32).reshape(count, tokens, kv_here, HEAD_DIM)
    values = pages[:, 1].astype(jnp.float32).reshape(count, tokens, kv_here, HEAD_DIM)
    grouped = query.reshape(slots, kv_here, ratio, HEAD_DIM)
    picked = jnp.take(grouped, owner_slot, axis=0)
    scores = jnp.einsum('ikgd,itkd->ikgt', picked, keys, precision=lax.Precision.HIGHEST)
    usable = (jnp.arange(tokens, dtype=jnp.int32)[None, :] < filled[:, None])[:, None, None, :]
    scores = jnp.where(usable, scores, neg_fill)
    page_top = lax.optimization_barrier(jnp.max(scores, axis=3))
    member = owner_slot[None, :] == jnp.arange(slots, dtype=jnp.int32)[:, None]
    slot_top = lax.optimization_barrier(jnp.max(jnp.where(member[:, :, None, None], page_top[None], neg_fill), axis=1))
    own_keys = token_kv[:, 0].astype(jnp.float32).reshape(slots, kv_here, HEAD_DIM)
    own_values = token_kv[:, 1].astype(jnp.float32).reshape(slots, kv_here, HEAD_DIM)
    own_score = jnp.einsum('skgd,skd->skg', grouped, own_keys, precision=lax.Precision.HIGHEST)
    own_score = jnp.where(first, own_score, neg_fill)
    slot_top = jnp.maximum(slot_top, own_score)
    reach = jnp.take(slot_top, owner_slot, axis=0)
    weights = jnp.where(usable, jnp.exp(scores - reach[..., None]), 0.0)
    page_sum = lax.optimization_barrier(jnp.sum(weights, axis=3))
    page_acc = jnp.einsum('ikgt,itkd->ikgd', weights, values, precision=lax.Precision.HIGHEST)
    own_weight = jnp.where(first, jnp.exp(own_score - slot_top), 0.0)
    member_f = member.astype(jnp.float32)
    total = jnp.dot(member_f, page_sum.reshape(count, -1), precision=lax.Precision.HIGHEST)
    total = total + own_weight.reshape(slots, -1)
    weighted = jnp.dot(member_f, page_acc.reshape(count, -1), precision=lax.Precision.HIGHEST)
    weighted = weighted.reshape(slots, kv_here, ratio, HEAD_DIM) + own_weight[..., None] * own_values[:, :, None, :]
    return (slot_top.reshape(slots, -1), total, weighted.reshape(slots, kv_here * ratio, HEAD_DIM))

def reference(hidden_states, attn_gain, mlp_gain, w_query, w_out, w_gate, w_up, w_down, kv_pool, resident_cache, resident_slot, resident_len, new_owner, new_local, new_slot, new_len, token_kv):
    groups = SLOTS // SLOT_G
    features = hidden_states.astype(jnp.float32)
    attn_scale = lax.rsqrt(lax.optimization_barrier(jnp.sum(features * features, axis=1)) / D + norm_eps)
    normed = (features * attn_gain).astype(jnp.bfloat16)
    query = jnp.dot(normed, w_query, preferred_element_type=jnp.float32) * attn_scale[:, None] * HEAD_DIM ** (-0.5)
    index = (new_owner * NEW_DEV + new_local).reshape(-1).astype(jnp.int32)
    new_cache = jnp.take(kv_pool, index, axis=0).reshape(groups, NEWC, 2, PAGE, KV_HEADS * HEAD_DIM)

    def attend(packed):
        grp_query, resident, arrived, res_slot, res_len, arr_slot, arr_len, own_kv = packed
        top, total, weighted = local_partials(grp_query, resident, arrived, res_slot, res_len, arr_slot, arr_len, own_kv, True)
        return (weighted / total[..., None]).astype(jnp.bfloat16)
    attn = lax.map(attend, (query.reshape(groups, SLOT_G, HEADS * HEAD_DIM), resident_cache, new_cache, resident_slot, resident_len, new_slot, new_len, token_kv.reshape(groups, SLOT_G, 2, KV_HEADS * HEAD_DIM)))
    attn = attn.reshape(SLOTS, HEADS * HEAD_DIM)
    branch = jnp.dot(attn, w_out.reshape(HEADS * HEAD_DIM, D), preferred_element_type=jnp.float32)
    resid = (features + branch).astype(jnp.bfloat16)
    resid_f = resid.astype(jnp.float32)
    mlp_scale = lax.rsqrt(lax.optimization_barrier(jnp.sum(resid_f * resid_f, axis=1)) / D + norm_eps)
    normed_mlp = (resid_f * mlp_gain).astype(jnp.bfloat16)
    gate = jnp.dot(normed_mlp, w_gate, preferred_element_type=jnp.float32) * mlp_scale[:, None]
    upward = jnp.dot(normed_mlp, w_up, preferred_element_type=jnp.float32) * mlp_scale[:, None]
    hidden_units = (jax.nn.silu(gate) * upward).astype(jnp.bfloat16)
    mixed = (resid_f + jnp.dot(hidden_units, w_down, preferred_element_type=jnp.float32)).astype(jnp.bfloat16)
    return (mixed, new_cache)
```

```python
import jax
import jax.numpy as jnp
from jax import lax
from jax.experimental import pallas as pl
from jax.experimental.pallas import tpu as pltpu
from jax.sharding import PartitionSpec as P

D = 4096
HEADS = 32
KV_HEADS = 8
HEAD_DIM = 128
NPR = 4
KV = "kv"
KV_TP = ("kv", "tp")
GRP_KV = ("grp", "kv")
GRP_KV_TP = ("grp", "kv", "tp")


neg_fill = -1e30
norm_eps = 1e-05


def combined_by_axis(shard, axes, combine):
    for axis in axes:
        pieces = jax.tree.map(lambda part: lax.all_gather(part, axis), shard)
        shard = jax.tree.map(lambda part: part[0], pieces)
        for k in range(1, lax.axis_size(axis)):
            shard = combine(shard, jax.tree.map(lambda part: part[k], pieces))
    return shard


def split_up(shard, dim, peers):
    before, after = (shard.shape[:dim], shard.shape[dim + 1 :])
    return jnp.moveaxis(shard.reshape(*before, peers, -1, *after), dim, 0)


def summed_on_arrival(shard, axis, dim):
    tiles = split_up(shard, dim, lax.axis_size(axis))
    arrived = lax.all_to_all(tiles, axis, split_axis=0, concat_axis=0, tiled=True)
    return arrived.astype(jnp.float32).sum(axis=0)


def combine(earlier, later):
    top_a, sum_a, acc_a = earlier
    top_b, sum_b, acc_b = later
    top = jnp.maximum(top_a, top_b)
    fade_a = jnp.exp(top_a - top)
    fade_b = jnp.exp(top_b - top)
    return (
        top,
        sum_a * fade_a + sum_b * fade_b,
        acc_a * fade_a[..., None] + acc_b * fade_b[..., None],
    )


def nth_match(table, wanted, places):
    matched = (table == wanted).astype(jnp.int32)
    ranking = jnp.cumsum(matched, axis=1) - 1
    return (matched[:, None, :] == 1) & (ranking[:, None, :] == places[None, :, None])


def move_pages(kv_pool, new_owner, new_local):
    groups = lax.axis_size("grp")
    ranks = lax.axis_size(KV)
    per_dev = new_owner.shape[1] // ranks
    cap = groups * NPR // ranks
    grp_rank = lax.axis_index("grp")
    kv_rank = lax.axis_index(KV)
    owners = new_owner.reshape(groups * ranks, per_dev)
    myself = grp_rank * ranks + kv_rank
    places = jnp.arange(cap, dtype=jnp.int32)
    mine = lax.dynamic_index_in_dim(owners, myself, 0, keepdims=False)
    order = jnp.arange(per_dev, dtype=jnp.int32)
    by_col = (
        new_owner.reshape(groups, ranks, per_dev)
        .transpose(1, 0, 2)
        .reshape(ranks, groups * per_dev)
    )
    local_col = (
        new_local.reshape(groups, ranks, per_dev)
        .transpose(1, 0, 2)
        .reshape(ranks, groups * per_dev)
    )
    select = nth_match(by_col, myself, places)
    picked = jnp.sum(jnp.where(select, local_col[:, None, :], 0), axis=2)
    outgoing = jnp.take(kv_pool, picked.reshape(-1), axis=0)
    received = lax.all_to_all(outgoing, KV, split_axis=0, concat_axis=0, tiled=True)
    row_here = lax.dynamic_index_in_dim(by_col, kv_rank, 0, keepdims=False)
    sources = grp_rank * ranks + jnp.arange(ranks, dtype=jnp.int32)
    hits = nth_match(
        jnp.broadcast_to(row_here[None, :], (ranks, row_here.shape[0])), sources[:, None], places
    )
    spots = jnp.arange(row_here.shape[0], dtype=jnp.int32)
    where_f = jnp.sum(jnp.where(hits, spots[None, None, :], 0), axis=2).reshape(-1)
    dest_grp = where_f // per_dev
    dest_pos = where_f % per_dev
    same = (dest_grp[:, None] == dest_grp[None, :]) & (dest_pos[:, None] < dest_pos[None, :])
    rank_in = jnp.sum(same.astype(jnp.int32), axis=0)
    target = dest_grp * NPR + rank_in
    items = jnp.arange(target.shape[0], dtype=jnp.int32)
    inverse = jnp.sum(jnp.where(target[None, :] == items[:, None], items[None, :], 0), axis=1)
    sorted_pages = jnp.take(received, inverse, axis=0)
    arrived = lax.all_to_all(sorted_pages, "grp", split_axis=0, concat_axis=0, tiled=True)
    src_grp = mine // ranks
    earlier = (src_grp[:, None] == src_grp[None, :]) & (order[:, None] < order[None, :])
    before = jnp.sum(earlier.astype(jnp.int32), axis=0)
    return jnp.take(arrived, src_grp * NPR + before, axis=0)


def local_partials(query, resident, arrived, res_slot, res_len, arr_slot, arr_len, token_kv, first):
    pages = jnp.concatenate([resident, arrived], axis=0)
    owner_slot = jnp.concatenate([res_slot, arr_slot])
    filled = jnp.concatenate([res_len, arr_len])
    count = pages.shape[0]
    tokens = pages.shape[2]
    kv_here = pages.shape[3] // HEAD_DIM
    slots = query.shape[0]
    ratio = HEADS // KV_HEADS
    keys = pages[:, 0].astype(jnp.float32).reshape(count, tokens, kv_here, HEAD_DIM)
    values = pages[:, 1].astype(jnp.float32).reshape(count, tokens, kv_here, HEAD_DIM)
    grouped = query.reshape(slots, kv_here, ratio, HEAD_DIM)
    picked = jnp.take(grouped, owner_slot, axis=0)
    scores = jnp.einsum("ikgd,itkd->ikgt", picked, keys, precision=lax.Precision.HIGHEST)
    usable = (jnp.arange(tokens, dtype=jnp.int32)[None, :] < filled[:, None])[:, None, None, :]
    scores = jnp.where(usable, scores, neg_fill)
    page_top = jnp.max(scores, axis=3)
    member = owner_slot[None, :] == jnp.arange(slots, dtype=jnp.int32)[:, None]
    slot_top = jnp.max(jnp.where(member[:, :, None, None], page_top[None], neg_fill), axis=1)
    own_keys = token_kv[:, 0].astype(jnp.float32).reshape(slots, kv_here, HEAD_DIM)
    own_values = token_kv[:, 1].astype(jnp.float32).reshape(slots, kv_here, HEAD_DIM)
    own_score = jnp.einsum("skgd,skd->skg", grouped, own_keys, precision=lax.Precision.HIGHEST)
    own_score = jnp.where(first, own_score, neg_fill)
    slot_top = jnp.maximum(slot_top, own_score)
    reach = jnp.take(slot_top, owner_slot, axis=0)
    weights = jnp.where(usable, jnp.exp(scores - reach[..., None]), 0.0)
    page_sum = jnp.sum(weights, axis=3)
    page_acc = jnp.einsum("ikgt,itkd->ikgd", weights, values, precision=lax.Precision.HIGHEST)
    own_weight = jnp.where(first, jnp.exp(own_score - slot_top), 0.0)
    member_f = member.astype(jnp.float32)
    total = jnp.dot(member_f, page_sum.reshape(count, -1), precision=lax.Precision.HIGHEST)
    total = total + own_weight.reshape(slots, -1)
    weighted = jnp.dot(member_f, page_acc.reshape(count, -1), precision=lax.Precision.HIGHEST)
    weighted = (
        weighted.reshape(slots, kv_here, ratio, HEAD_DIM)
        + own_weight[..., None] * own_values[:, :, None, :]
    )
    return (slot_top.reshape(slots, -1), total, weighted.reshape(slots, kv_here * ratio, HEAD_DIM))


MESH = pl.DeviceIdType.MESH


def peer_of(x, y, k):
    return lax.rem(x + k // 4, 4) * 4 + lax.rem(y + k % 4, 4)


def source_of(x, y, k):
    return lax.rem(x + 4 - k // 4, 4) * 4 + lax.rem(y + 4 - k % 4, 4)


ORDER = sorted(range(1, 16), key=lambda k: (min(k // 4, 4 - k // 4) + min(k % 4, 4 - k % 4), k))


def tail_kernel(
    attn_ref, hid_ref, gain_ref, wout_hbm, wg_hbm, wu_hbm, wd_hbm, out_ref,
    wout, wg, wu, wd, pair_send, pair_recv, own_part, rs_send, rs_recv, ag, hunits,
    dp_send, dp_recv, dsum, d_send, d_recv, resrow,
    w_sem, pair_ss, pair_rs, rs_ss, rs_rs, ag_ss, ag_rs, fw_ss, fw_rs, dp_ss, dp_rs, d_ss, d_rs,
):
    f32, bf16 = jnp.float32, jnp.bfloat16
    grp, kv, tp = lax.axis_index("grp"), lax.axis_index("kv"), lax.axis_index("tp")
    x, y = kv // 4, lax.rem(kv, 4)
    other = 1 - tp
    partner = (grp, kv, other)

    def dev(k):
        return (grp, peer_of(x, y, k), tp)

    loads = [
        pltpu.make_async_copy(src, dst, w_sem.at[i])
        for i, (src, dst) in enumerate([(wout_hbm, wout), (wg_hbm, wg), (wu_hbm, wu), (wd_hbm, wd)])
    ]
    for load in loads:
        load.start()

    barrier = pltpu.get_barrier_semaphore()
    pl.semaphore_signal(barrier, inc=1, device_id=partner, device_id_type=MESH)
    for k in range(1, 16):
        pl.semaphore_signal(barrier, inc=1, device_id=dev(k), device_id_type=MESH)

    rho = lax.broadcasted_iota(jnp.int32, (128, 128), 0)
    col = lax.broadcasted_iota(jnp.int32, (128, 128), 1)
    slot = (lax.rem(rho, 64) // 4) * 8 + (rho // 64) * 4 + lax.rem(rho, 4)
    perm = jnp.where(col == slot, 1.0, 0.0).astype(bf16)
    attn = jnp.dot(perm, attn_ref[...], preferred_element_type=f32).astype(bf16)
    hid = jnp.dot(
        perm, hid_ref[:, pl.ds(pl.multiple_of(tp * 128, 128), 128)], preferred_element_type=f32
    )

    loads[0].wait()
    pl.semaphore_wait(barrier, 16)

    order = ORDER[::-1] + [0]
    pair_copies = []
    for g in range(4):
        for i in range(4):
            k = order[4 * g + i]
            dest = peer_of(x, y, k)
            part = jnp.dot(
                attn, wout[:, pl.ds(pl.multiple_of(dest * 256, 256), 256)], preferred_element_type=f32
            )
            low, high = part[:, :128], part[:, 128:]
            own_part[g, i] = jnp.where(tp == 0, low, high)
            pair_send[g, i] = jnp.where(tp == 0, high, low).astype(bf16)
        copy = pltpu.make_async_remote_copy(
            src_ref=pair_send.at[g], dst_ref=pair_recv.at[g], send_sem=pair_ss.at[g],
            recv_sem=pair_rs.at[g], device_id=partner, device_id_type=MESH,
        )
        copy.start()
        pair_copies.append(copy)
    rs_copies = {}
    block = None
    for g in range(4):
        pair_copies[g].wait_recv()
        for i in range(4):
            k = order[4 * g + i]
            total = own_part[g, i] + pair_recv[g, i].astype(f32)
            if k == 0:
                block = total + hid
            else:
                rs_send[k] = total.astype(bf16)
                copy = pltpu.make_async_remote_copy(
                    src_ref=rs_send.at[k], dst_ref=rs_recv.at[k], send_sem=rs_ss.at[k],
                    recv_sem=rs_rs.at[k], device_id=dev(k), device_id_type=MESH,
                )
                copy.start()
                rs_copies[k] = copy
    for k in ORDER:
        rs_copies[k].wait_recv()
        block = block + rs_recv[k].astype(f32)
    ag[0, tp] = block.astype(bf16)

    ag_copies = {}
    fw_copies = {}

    def forward(k):
        copy = pltpu.make_async_remote_copy(
            src_ref=ag.at[k, tp], dst_ref=ag.at[k, tp], send_sem=fw_ss.at[k],
            recv_sem=fw_rs.at[k], device_id=partner, device_id_type=MESH,
        )
        copy.start()
        fw_copies[k] = copy

    for k in ORDER[::-1]:
        copy = pltpu.make_async_remote_copy(
            src_ref=ag.at[0, tp], dst_ref=ag.at[k, tp], send_sem=ag_ss.at[k],
            recv_sem=ag_rs.at[k], device_id=dev(k), device_id_type=MESH,
        )
        copy.start()
        ag_copies[k] = copy
    forward(0)
    for g in range(4):
        pair_copies[g].wait_send()
    loads[1].wait()
    loads[2].wait()
    seq = [0] + ORDER
    gate = jnp.zeros((128, 448), f32)
    upward = jnp.zeros((128, 448), f32)
    squares = jnp.zeros((128, 128), f32)
    mine = lax.broadcasted_iota(jnp.int32, (8, 128), 0) + tp * 64 + kv * 4
    pick = jnp.where(lax.broadcasted_iota(jnp.int32, (8, 128), 1) == mine, 1.0, 0.0).astype(bf16)
    for n, k in enumerate(seq):
        if n + 1 < 16:
            ag_copies[seq[n + 1]].wait_recv()
            forward(seq[n + 1])
        fw_copies[k].wait_recv()
        src = source_of(x, y, k)
        both = jnp.concatenate([ag[k, 0], ag[k, 1]], axis=1)
        wide = both.astype(f32)
        squares = squares + wide[:, :128] * wide[:, :128] + wide[:, 128:] * wide[:, 128:]
        normed = (wide * gain_ref[pl.ds(src, 1), :]).astype(bf16)
        rows = pl.ds(pl.multiple_of(src * 256, 256), 256)
        gate = gate + jnp.dot(normed, wg[rows, :], preferred_element_type=f32)
        upward = upward + jnp.dot(normed, wu[rows, :], preferred_element_type=f32)
    scale = lax.rsqrt(jnp.sum(squares, axis=1, keepdims=True) / D + norm_eps)
    gate = gate * scale
    upward = upward * scale
    hunits[...] = (gate / (1.0 + jnp.exp(-gate)) * upward).astype(bf16)

    loads[3].wait()
    dp_copies = []
    for c in range(4):
        cols = pl.ds(c * 1024, 1024)
        part = jnp.dot(hunits[...], wd[:, cols], preferred_element_type=f32)
        first, second = part[:64], part[64:]
        dsum[:, cols] = jnp.where(tp == 0, first, second)
        dp_send[c] = jnp.where(tp == 0, second, first).astype(bf16)
        copy = pltpu.make_async_remote_copy(
            src_ref=dp_send.at[c], dst_ref=dp_recv.at[c], send_sem=dp_ss.at[c],
            recv_sem=dp_rs.at[c], device_id=partner, device_id_type=MESH,
        )
        copy.start()
        dp_copies.append(copy)
    for c in range(4):
        dp_copies[c].wait_recv()
        cols = pl.ds(c * 1024, 1024)
        dsum[:, cols] = dsum[:, cols] + dp_recv[c].astype(f32)
    for j in range(16):
        d_send[j] = dsum[4 * j : 4 * j + 4, :].astype(bf16)
    d_copies = {}
    for k in ORDER[::-1]:
        copy = pltpu.make_async_remote_copy(
            src_ref=d_send.at[peer_of(x, y, k)], dst_ref=d_recv.at[k], send_sem=d_ss.at[k],
            recv_sem=d_rs.at[k], device_id=dev(k), device_id_type=MESH,
        )
        copy.start()
        d_copies[k] = copy
    for k in range(16):
        for t in range(2):
            cols = pl.ds(pl.multiple_of((source_of(x, y, k) * 2 + t) * 128, 128), 128)
            resrow[:, cols] = jnp.dot(pick, ag[k, t], preferred_element_type=f32)
    pick64 = lax.broadcasted_iota(jnp.int32, (8, 64), 0) + kv * 4
    total = resrow[...][:4]
    lane = lax.broadcasted_iota(jnp.int32, (4, 4096), 0)
    own = jnp.zeros((4, 4096), f32)
    for j in range(16):
        own = jnp.where(kv == j, dsum[4 * j : 4 * j + 4, :], own)
    total = total + own
    for k in ORDER:
        d_copies[k].wait_recv()
        total = total + d_recv[k].astype(f32)
    out_ref[...] = total.astype(bf16)

    for k in range(1, 16):
        rs_copies[k].wait_send()
        ag_copies[k].wait_send()
        d_copies[k].wait_send()
    for k in range(16):
        fw_copies[k].wait_send()
    for c in range(4):
        dp_copies[c].wait_send()


def tail(attn, hidden, gain, w_out, w_gate, w_up, w_down):
    bf16, f32 = jnp.bfloat16, jnp.float32
    vmem = pl.BlockSpec(memory_space=pltpu.VMEM)
    hbm = pl.BlockSpec(memory_space=pl.ANY)
    dma = pltpu.SemaphoreType.DMA
    return pl.pallas_call(
        tail_kernel,
        name="tail",
        out_shape=jax.ShapeDtypeStruct((4, 4096), bf16),
        in_specs=[vmem, vmem, vmem, hbm, hbm, hbm, hbm],
        out_specs=vmem,
        scratch_shapes=[
            pltpu.VMEM((128, 4096), bf16),
            pltpu.VMEM((4096, 448), bf16),
            pltpu.VMEM((4096, 448), bf16),
            pltpu.VMEM((448, 4096), bf16),
            pltpu.VMEM((4, 4, 128, 128), bf16),
            pltpu.VMEM((4, 4, 128, 128), bf16),
            pltpu.VMEM((4, 4, 128, 128), f32),
            pltpu.VMEM((16, 128, 128), bf16),
            pltpu.VMEM((16, 128, 128), bf16),
            pltpu.VMEM((16, 2, 128, 128), bf16),
            pltpu.VMEM((128, 448), bf16),
            pltpu.VMEM((4, 64, 1024), bf16),
            pltpu.VMEM((4, 64, 1024), bf16),
            pltpu.VMEM((64, 4096), f32),
            pltpu.VMEM((16, 4, 4096), bf16),
            pltpu.VMEM((16, 4, 4096), bf16),
            pltpu.VMEM((8, 4096), f32),
            dma((4,)), dma((4,)), dma((4,)), dma((16,)), dma((16,)), dma((16,)), dma((16,)),
            dma((16,)), dma((16,)), dma((4,)), dma((4,)), dma((16,)), dma((16,)),
        ],
        compiler_params=pltpu.CompilerParams(
            collective_id=0, has_side_effects=True, vmem_limit_bytes=60 * 1024 * 1024
        ),
    )(attn, hidden, gain, w_out, w_gate, w_up, w_down)


def per_device(
    hidden_states,
    attn_gain,
    mlp_gain,
    w_query,
    w_out,
    w_gate,
    w_up,
    w_down,
    kv_pool,
    resident_cache,
    resident_slot,
    resident_len,
    new_owner,
    new_local,
    new_slot,
    new_len,
    token_kv,
):
    ranks = lax.axis_size(KV)
    pairs = lax.axis_size("tp")
    kv_rank = lax.axis_index(KV)
    tp_rank = lax.axis_index("tp")
    features = hidden_states.astype(jnp.float32)
    partial_query = jnp.dot(
        (features * attn_gain).astype(jnp.bfloat16), w_query, preferred_element_type=jnp.float32
    )
    squares = jnp.sum(features * features, axis=1)
    partial_query, squares = lax.psum((partial_query, squares), KV)
    attn_scale = lax.rsqrt(squares / D + norm_eps)
    query = partial_query * attn_scale[:, None] * HEAD_DIM ** (-0.5)
    new_pages = move_pages(kv_pool, new_owner, new_local)
    top, total, weighted = local_partials(
        query,
        resident_cache[0],
        new_pages,
        resident_slot[0],
        resident_len[0],
        new_slot[0],
        new_len[0],
        token_kv,
        kv_rank == 0,
    )
    top, total, weighted = combined_by_axis((top, total, weighted), (KV,), combine)
    attn = (weighted / total[..., None]).astype(jnp.bfloat16)
    slots = attn.shape[0]
    heads_here = attn.shape[1]
    span = HEAD_DIM // ranks
    piece = lax.dynamic_slice_in_dim(attn, kv_rank * span, span, 2)
    mixed = tail(
        piece.reshape(slots, heads_here * span),
        hidden_states,
        mlp_gain.reshape(16, 256),
        w_out.reshape(heads_here * span, w_out.shape[2]),
        w_gate,
        w_up,
        w_down,
    )
    return (mixed, new_pages[None])


def solution(mesh):
    return jax.shard_map(
        per_device,
        mesh=mesh,
        in_specs=(
            P("grp", KV),
            P(KV),
            P(),
            P(KV, "tp"),
            P("tp", KV, None),
            P(None, KV_TP),
            P(None, KV_TP),
            P(KV_TP, None),
            P(GRP_KV, None, None, "tp"),
            P("grp", KV, None, None, "tp"),
            P("grp", KV),
            P("grp", KV),
            P(),
            P(),
            P("grp", KV),
            P("grp", KV),
            P("grp", None, "tp"),
        ),
        out_specs=(P(GRP_KV_TP, None), P("grp", KV, None, None, "tp")),
        check_vma=False,
    )
```

```python
import jax
import jax.numpy as jnp
from jax import lax
from jax.experimental import pallas as pl
from jax.experimental.pallas import tpu as pltpu
from jax.sharding import PartitionSpec as P

D = 4096
HEADS = 32
KV_HEADS = 8
HEAD_DIM = 128
KV_TP = ("kv", "tp")
GRP_KV = ("grp", "kv")
GRP_KV_TP = ("grp", "kv", "tp")


neg_fill = -1e30
norm_eps = 1e-05
MESH = pl.DeviceIdType.MESH


def peer_of(x, y, k):
    return lax.rem(x + k // 4, 4) * 4 + lax.rem(y + k % 4, 4)


def source_of(x, y, k):
    return lax.rem(x + 4 - k // 4, 4) * 4 + lax.rem(y + 4 - k % 4, 4)


ORDER = sorted(range(1, 16), key=lambda k: (min(k // 4, 4 - k // 4) + min(k % 4, 4 - k % 4), k))


def tail_kernel(
    attn_ref, hid_ref, gain_ref, wout_hbm, wg_hbm, wu_hbm, wd_hbm, out_ref,
    wout, wg, wu, wd, pair_send, pair_recv, own_part, rs_send, rs_recv, ag, hunits,
    dp_send, dp_recv, dsum, d_send, d_recv, resrow,
    w_sem, pair_ss, pair_rs, rs_ss, rs_rs, ag_ss, ag_rs, fw_ss, fw_rs, dp_ss, dp_rs, d_ss, d_rs,
):
    f32, bf16 = jnp.float32, jnp.bfloat16
    grp, kv, tp = lax.axis_index("grp"), lax.axis_index("kv"), lax.axis_index("tp")
    x, y = kv // 4, lax.rem(kv, 4)
    other = 1 - tp
    partner = (grp, kv, other)

    def dev(k):
        return (grp, peer_of(x, y, k), tp)

    loads = [
        pltpu.make_async_copy(src, dst, w_sem.at[i])
        for i, (src, dst) in enumerate([(wout_hbm, wout), (wg_hbm, wg), (wu_hbm, wu), (wd_hbm, wd)])
    ]
    for load in loads:
        load.start()

    barrier = pltpu.get_barrier_semaphore()
    pl.semaphore_signal(barrier, inc=1, device_id=partner, device_id_type=MESH)
    for k in range(1, 16):
        pl.semaphore_signal(barrier, inc=1, device_id=dev(k), device_id_type=MESH)

    rho = lax.broadcasted_iota(jnp.int32, (128, 128), 0)
    col = lax.broadcasted_iota(jnp.int32, (128, 128), 1)
    slot = (lax.rem(rho, 64) // 4) * 8 + (rho // 64) * 4 + lax.rem(rho, 4)
    perm = jnp.where(col == slot, 1.0, 0.0).astype(bf16)
    attn = jnp.dot(perm, attn_ref[...], preferred_element_type=f32).astype(bf16)
    hid = jnp.dot(
        perm, hid_ref[:, pl.ds(pl.multiple_of(tp * 128, 128), 128)], preferred_element_type=f32
    )

    loads[0].wait()
    pl.semaphore_wait(barrier, 16)

    order = ORDER[::-1] + [0]
    pair_copies = []
    for g in range(4):
        for i in range(4):
            k = order[4 * g + i]
            dest = peer_of(x, y, k)
            part = jnp.dot(
                attn, wout[:, pl.ds(pl.multiple_of(dest * 256, 256), 256)], preferred_element_type=f32
            )
            low, high = part[:, :128], part[:, 128:]
            own_part[g, i] = jnp.where(tp == 0, low, high)
            pair_send[g, i] = jnp.where(tp == 0, high, low).astype(bf16)
        copy = pltpu.make_async_remote_copy(
            src_ref=pair_send.at[g], dst_ref=pair_recv.at[g], send_sem=pair_ss.at[g],
            recv_sem=pair_rs.at[g], device_id=partner, device_id_type=MESH,
        )
        copy.start()
        pair_copies.append(copy)
    rs_copies = {}
    block = None
    for g in range(4):
        pair_copies[g].wait_recv()
        for i in range(4):
            k = order[4 * g + i]
            total = own_part[g, i] + pair_recv[g, i].astype(f32)
            if k == 0:
                block = total + hid
            else:
                rs_send[k] = total.astype(bf16)
                copy = pltpu.make_async_remote_copy(
                    src_ref=rs_send.at[k], dst_ref=rs_recv.at[k], send_sem=rs_ss.at[k],
                    recv_sem=rs_rs.at[k], device_id=dev(k), device_id_type=MESH,
                )
                copy.start()
                rs_copies[k] = copy
    for k in ORDER:
        rs_copies[k].wait_recv()
        block = block + rs_recv[k].astype(f32)
    ag[0, tp] = block.astype(bf16)

    ag_copies = {}
    fw_copies = {}

    def forward(k):
        copy = pltpu.make_async_remote_copy(
            src_ref=ag.at[k, tp], dst_ref=ag.at[k, tp], send_sem=fw_ss.at[k],
            recv_sem=fw_rs.at[k], device_id=partner, device_id_type=MESH,
        )
        copy.start()
        fw_copies[k] = copy

    for k in ORDER[::-1]:
        copy = pltpu.make_async_remote_copy(
            src_ref=ag.at[0, tp], dst_ref=ag.at[k, tp], send_sem=ag_ss.at[k],
            recv_sem=ag_rs.at[k], device_id=dev(k), device_id_type=MESH,
        )
        copy.start()
        ag_copies[k] = copy
    forward(0)
    for g in range(4):
        pair_copies[g].wait_send()
    loads[1].wait()
    loads[2].wait()
    seq = [0] + ORDER
    gate = jnp.zeros((128, 448), f32)
    upward = jnp.zeros((128, 448), f32)
    squares = jnp.zeros((128, 128), f32)
    mine = lax.broadcasted_iota(jnp.int32, (8, 128), 0) + tp * 64 + kv * 4
    pick = jnp.where(lax.broadcasted_iota(jnp.int32, (8, 128), 1) == mine, 1.0, 0.0).astype(bf16)
    for n, k in enumerate(seq):
        if n + 1 < 16:
            ag_copies[seq[n + 1]].wait_recv()
            forward(seq[n + 1])
        fw_copies[k].wait_recv()
        src = source_of(x, y, k)
        both = jnp.concatenate([ag[k, 0], ag[k, 1]], axis=1)
        wide = both.astype(f32)
        squares = squares + wide[:, :128] * wide[:, :128] + wide[:, 128:] * wide[:, 128:]
        normed = (wide * gain_ref[pl.ds(src, 1), :]).astype(bf16)
        rows = pl.ds(pl.multiple_of(src * 256, 256), 256)
        gate = gate + jnp.dot(normed, wg[rows, :], preferred_element_type=f32)
        upward = upward + jnp.dot(normed, wu[rows, :], preferred_element_type=f32)
    scale = lax.rsqrt(jnp.sum(squares, axis=1, keepdims=True) / D + norm_eps)
    gate = gate * scale
    upward = upward * scale
    hunits[...] = (gate / (1.0 + jnp.exp(-gate)) * upward).astype(bf16)

    loads[3].wait()
    dp_copies = []
    for c in range(4):
        cols = pl.ds(c * 1024, 1024)
        part = jnp.dot(hunits[...], wd[:, cols], preferred_element_type=f32)
        first, second = part[:64], part[64:]
        dsum[:, cols] = jnp.where(tp == 0, first, second)
        dp_send[c] = jnp.where(tp == 0, second, first).astype(bf16)
        copy = pltpu.make_async_remote_copy(
            src_ref=dp_send.at[c], dst_ref=dp_recv.at[c], send_sem=dp_ss.at[c],
            recv_sem=dp_rs.at[c], device_id=partner, device_id_type=MESH,
        )
        copy.start()
        dp_copies.append(copy)
    for c in range(4):
        dp_copies[c].wait_recv()
        cols = pl.ds(c * 1024, 1024)
        dsum[:, cols] = dsum[:, cols] + dp_recv[c].astype(f32)
    for j in range(16):
        d_send[j] = dsum[4 * j : 4 * j + 4, :].astype(bf16)
    d_copies = {}
    for k in ORDER[::-1]:
        copy = pltpu.make_async_remote_copy(
            src_ref=d_send.at[peer_of(x, y, k)], dst_ref=d_recv.at[k], send_sem=d_ss.at[k],
            recv_sem=d_rs.at[k], device_id=dev(k), device_id_type=MESH,
        )
        copy.start()
        d_copies[k] = copy
    for k in range(16):
        for t in range(2):
            cols = pl.ds(pl.multiple_of((source_of(x, y, k) * 2 + t) * 128, 128), 128)
            resrow[:, cols] = jnp.dot(pick, ag[k, t], preferred_element_type=f32)
    pick64 = lax.broadcasted_iota(jnp.int32, (8, 64), 0) + kv * 4
    total = resrow[...][:4]
    lane = lax.broadcasted_iota(jnp.int32, (4, 4096), 0)
    own = jnp.zeros((4, 4096), f32)
    for j in range(16):
        own = jnp.where(kv == j, dsum[4 * j : 4 * j + 4, :], own)
    total = total + own
    for k in ORDER:
        d_copies[k].wait_recv()
        total = total + d_recv[k].astype(f32)
    out_ref[...] = total.astype(bf16)

    for k in range(1, 16):
        rs_copies[k].wait_send()
        ag_copies[k].wait_send()
        d_copies[k].wait_send()
    for k in range(16):
        fw_copies[k].wait_send()
    for c in range(4):
        dp_copies[c].wait_send()


def tail(attn, hidden, gain, w_out, w_gate, w_up, w_down):
    bf16, f32 = jnp.bfloat16, jnp.float32
    vmem = pl.BlockSpec(memory_space=pltpu.VMEM)
    hbm = pl.BlockSpec(memory_space=pl.ANY)
    dma = pltpu.SemaphoreType.DMA
    return pl.pallas_call(
        tail_kernel,
        name="tail",
        out_shape=jax.ShapeDtypeStruct((4, 4096), bf16),
        in_specs=[vmem, vmem, vmem, hbm, hbm, hbm, hbm],
        out_specs=vmem,
        scratch_shapes=[
            pltpu.VMEM((128, 4096), bf16),
            pltpu.VMEM((4096, 448), bf16),
            pltpu.VMEM((4096, 448), bf16),
            pltpu.VMEM((448, 4096), bf16),
            pltpu.VMEM((4, 4, 128, 128), bf16),
            pltpu.VMEM((4, 4, 128, 128), bf16),
            pltpu.VMEM((4, 4, 128, 128), f32),
            pltpu.VMEM((16, 128, 128), bf16),
            pltpu.VMEM((16, 128, 128), bf16),
            pltpu.VMEM((16, 2, 128, 128), bf16),
            pltpu.VMEM((128, 448), bf16),
            pltpu.VMEM((4, 64, 1024), bf16),
            pltpu.VMEM((4, 64, 1024), bf16),
            pltpu.VMEM((64, 4096), f32),
            pltpu.VMEM((16, 4, 4096), bf16),
            pltpu.VMEM((16, 4, 4096), bf16),
            pltpu.VMEM((8, 4096), f32),
            dma((4,)), dma((4,)), dma((4,)), dma((16,)), dma((16,)), dma((16,)), dma((16,)),
            dma((16,)), dma((16,)), dma((4,)), dma((4,)), dma((16,)), dma((16,)),
        ],
        compiler_params=pltpu.CompilerParams(
            collective_id=0, has_side_effects=True, vmem_limit_bytes=60 * 1024 * 1024
        ),
    )(attn, hidden, gain, w_out, w_gate, w_up, w_down)


CHUNKS = 8
CROWS = 256 // CHUNKS
LOG_ROWS = 32


def head_kernel(
    meta, hid_ref, again_ref, tok_ref, wq_hbm, pool_hbm, res_hbm, attn_ref, cache_hbm,
    wq, kept, qs_send, qs_recv, qfull, qflat, fsk, fsv, scores, probs, pvacc, accs, stats, msend, mrecv, *rest,
):
    f32, bf16, i32 = jnp.float32, jnp.bfloat16, jnp.int32
    nc = CHUNKS
    pool, xs, xr, zs, zr = (rest[i * nc : (i + 1) * nc] for i in range(5))
    (ld_sem, pool_sem, kept_sem, out_sem, q_ss, q_rs, a_ss, a_rs, x_ss, x_rs, z_ss, z_rs, s_ss, s_rs,
     m_ss, m_rs) = rest[5 * nc :]
    grp, kv, tp = lax.axis_index("grp"), lax.axis_index("kv"), lax.axis_index("tp")
    x, y = kv // 4, lax.rem(kv, 4)

    def dev(k):
        return (grp, peer_of(x, y, k), tp)

    def zdev(dz):
        return (lax.rem(grp + dz, 4), kv, tp)

    def remote(src, dst, send, recv, device):
        copy = pltpu.make_async_remote_copy(
            src_ref=src, dst_ref=dst, send_sem=send, recv_sem=recv, device_id=device,
            device_id_type=MESH,
        )
        copy.start()
        return copy

    wq_load = pltpu.make_async_copy(wq_hbm, wq, ld_sem.at[0])
    wq_load.start()
    pool_loads = []
    for c in range(nc):
        load = pltpu.make_async_copy(pool_hbm.at[:, pl.ds(c * CROWS, CROWS), :], pool[c], pool_sem.at[c])
        load.start()
        pool_loads.append(load)
    kept_load = pltpu.make_async_copy(res_hbm, kept, kept_sem.at[0])
    kept_load.start()

    barrier = pltpu.get_barrier_semaphore()
    for k in range(1, 16):
        pl.semaphore_signal(barrier, inc=1, device_id=dev(k), device_id_type=MESH)
    for dz in range(1, 4):
        pl.semaphore_signal(barrier, inc=1, device_id=zdev(dz), device_id_type=MESH)

    feats = hid_ref[...].astype(f32)
    normed = (feats * again_ref[...]).astype(bf16)
    squares = jnp.sum(feats * feats, axis=1, keepdims=True)
    wq_load.wait()
    for h in range(4):
        part = jnp.dot(normed, wq[:, h * 512 : h * 512 + 512], preferred_element_type=f32)
        qs_send[:, :, h * 512 : h * 512 + 512] = part.reshape(16, 8, 512)
    qs_send[:, :, 2048:2176] = jnp.broadcast_to(squares, (128, 128)).reshape(16, 8, 128)
    pl.semaphore_wait(barrier, 18)

    q_copies = {}
    for k in ORDER[::-1]:
        q_copies[k] = remote(qs_send.at[peer_of(x, y, k)], qs_recv.at[k], q_ss.at[k], q_rs.at[k], dev(k))

    x_copies = {}
    z_copies = {}
    out_copies = []

    def xy_start(c):
        pool_loads[c].wait()
        xr[c][kv] = pool[c][meta[kv]]
        for k in range(1, 16):
            xs[c][k - 1] = pool[c][meta[peer_of(x, y, k)]]
        for k in ORDER[::-1]:
            x_copies[c, k] = remote(
                xs[c].at[k - 1], xr[c].at[kv], x_ss.at[c, k], x_rs.at[c, k], dev(k)
            )

    def z_start(c):
        for k in ORDER:
            x_copies[c, k].wait_recv()
        for dz in range(4):
            g = lax.rem(grp + dz, 4)
            for r in range(4):
                page = xr[c][meta[16 + g * 4 + r]]
                if dz == 0:
                    zr[c][grp, r] = page
                else:
                    zs[c][dz - 1, r] = page
        for dz in (2, 1, 3):
            z_copies[c, dz] = remote(
                zs[c].at[dz - 1], zr[c].at[grp], z_ss.at[c, dz], z_rs.at[c, dz], zdev(dz)
            )

    def finish(c):
        for dz in (1, 3, 2):
            z_copies[c, dz].wait_recv()
        final, half = (fsk, 0) if c < nc // 2 else (fsv, 1)
        row = (c % (nc // 2)) * CROWS
        for i in range(16):
            where = meta[32 + i]
            final[i, row : row + CROWS, :] = zr[c][where // 4, lax.rem(where, 4)]
        copy = pltpu.make_async_copy(
            final.at[:, pl.ds(row, CROWS), :], cache_hbm.at[:, half, pl.ds(row, CROWS), :], out_sem.at[c]
        )
        copy.start()
        out_copies.append(copy)

    head_of = lax.broadcasted_iota(i32, (16, 512), 0) // 4
    block_of = lax.broadcasted_iota(i32, (16, 512), 1) // 128
    diag = head_of == block_of
    lanes = lax.broadcasted_iota(i32, (16, 128), 1)

    def page_scores(p, keys, slot, filled):
        q = qfull[slot]
        wide = jnp.where(diag, jnp.concatenate([q, q, q, q], axis=1), 0.0)
        high = wide.astype(bf16)
        left = wide - high.astype(f32)
        mid = left.astype(bf16)
        low = (left - mid.astype(f32)).astype(bf16)
        rows = jnp.concatenate([high, mid, low], axis=0)
        s = lax.dot_general(rows, keys, (((1,), (1,)), ((), ())), preferred_element_type=f32)
        s = s[:16] + s[16:32] + s[32:]
        s = jnp.where(lanes < filled, s, neg_fill)
        scores[p] = s
        top = jnp.max(s, axis=1, keepdims=True)
        total = jnp.sum(jnp.where(lanes < filled, jnp.exp(s - top), 0.0), axis=1, keepdims=True)
        return top, total

    def weighted(p, values, lo, hi):
        w = probs[p][:, lo:hi]
        high = w.astype(bf16)
        low = (w - high.astype(f32)).astype(bf16)
        out = jnp.dot(jnp.concatenate([high, low], axis=0), values, preferred_element_type=f32)
        return out[:16] + out[16:]

    def place(p, acc):
        for h in range(16):
            accs[h, p : p + 1, :] = acc[h : h + 1, (h // 4) * 128 : (h // 4) * 128 + 128]

    table = jnp.zeros((128, 128), f32)
    row128 = lax.broadcasted_iota(i32, (128, 128), 0)
    col128 = lax.broadcasted_iota(i32, (128, 128), 1)

    def note(table, p, top, total):
        both = jnp.concatenate([top, total, jnp.zeros((96, 1), f32)], axis=0)
        return jnp.where(col128 == p, both, table)

    def query_done():
        total = qs_send[kv]
        for k in ORDER:
            q_copies[k].wait_recv()
            total = total + qs_recv[k]
        scale = lax.rsqrt(total[:, 2048:2049] / D + norm_eps)
        q8 = total[:, :2048] * scale * HEAD_DIM ** (-0.5)
        qflat[...] = q8
        for h in range(16):
            qfull[pl.ds(pl.multiple_of(kv * 8, 8), 8), h, :] = q8[:, h * 128 : h * 128 + 128]
        mine = qfull.at[pl.ds(pl.multiple_of(kv * 8, 8), 8)]
        return {k: remote(mine, mine, a_ss.at[k], a_rs.at[k], dev(k)) for k in ORDER[::-1]}

    xy_start(0)
    xy_start(1)
    a_copies = query_done()
    xy_start(2)
    z_start(0)
    xy_start(3)
    z_start(1)
    finish(0)
    for k in ORDER:
        a_copies[k].wait_recv()
    kept_load.wait()
    for p in range(8):
        table = note(table, p, *page_scores(p, kept[p, 0], meta[48 + p], meta[56 + p]))
    xy_start(4)
    z_start(2)
    finish(1)
    xy_start(5)
    z_start(3)
    finish(2)
    xy_start(6)
    z_start(4)
    finish(3)
    for p in range(16):
        table = note(table, 8 + p, *page_scores(8 + p, fsk[p], meta[64 + p], meta[80 + p]))
    own = tok_ref[pl.ds(pl.multiple_of(kv * 8, 8), 8), :].astype(f32)
    lane8 = lax.broadcasted_iota(i32, (8, 128), 1)
    own_rows = jnp.where((lane8 >= 16) & (lane8 < 32), 1.0, 0.0).astype(f32)
    for h in range(16):
        s = jnp.sum(
            qflat[:, h * 128 : h * 128 + 128] * own[:, (h // 4) * 128 : (h // 4) * 128 + 128],
            axis=1, keepdims=True,
        )
        own_rows = jnp.where(lane8 == h, s, own_rows)
    slots = jnp.zeros((32, 1), i32)
    row32 = lax.broadcasted_iota(i32, (32, 1), 0)
    for p in range(8):
        slots = jnp.where(row32 == p, meta[48 + p], slots)
    for p in range(16):
        slots = jnp.where(row32 == 8 + p, meta[64 + p], slots)
    slots = jnp.where(row32 >= 24, kv * 8 + row32 - 24, slots)
    lane32 = lax.broadcasted_iota(i32, (32, 128), 1)
    mine = jnp.concatenate([table.T[:24], own_rows], axis=0)
    mine = jnp.where(lane32 == 32, slots.astype(f32), mine)
    stats[kv] = mine
    s_copies = {
        k: remote(stats.at[kv], stats.at[kv], s_ss.at[k], s_rs.at[k], dev(k)) for k in ORDER[::-1]
    }
    xy_start(7)
    z_start(5)
    finish(4)
    for k in ORDER:
        s_copies[k].wait_recv()
    every = stats[...].reshape(512, 128)
    every_slot = every[:, 32:33].astype(i32)
    sums = pltpu.roll(every, 112, 1)
    lane512 = lax.broadcasted_iota(i32, (512, 128), 1)
    result = jnp.zeros((128, 128), f32)
    for p in range(32):
        slot = meta[48 + p] if p < 8 else (meta[64 + p - 8] if p < 24 else kv * 8 + p - 24)
        same = (every_slot == slot) & (lane512 < 16)
        top = jnp.max(jnp.where(same, every, neg_fill), axis=0, keepdims=True)
        total = jnp.sum(jnp.where(same, jnp.exp(every - top) * sums, 0.0), axis=0, keepdims=True)
        line = jnp.where(lane8[:1] < 16, top, pltpu.roll(1.0 / jnp.where(lane8[:1] < 16, total, 1.0), 16, 1))
        result = jnp.where(row128 == p, line, result)
    turned = result.T
    for p in range(24):
        probs[p] = jnp.exp(scores[p] - turned[:16, p : p + 1]) * turned[16:32, p : p + 1]
    for p in range(8):
        place(p, weighted(p, kept[p, 1], 0, 128))
    own_weight = jnp.exp(own_rows - result[24:32]) * pltpu.roll(result[24:32], 112, 1)
    for h in range(16):
        g = 512 + (h // 4) * 128
        accs[h, 24:32, :] = own_weight[:, h : h + 1] * own[:, g : g + 128]
    member = jnp.where(every_slot == lane512, 1.0, 0.0).astype(f32)
    member = jnp.concatenate([member[128 * i : 128 * i + 128].T for i in range(4)], axis=1).astype(bf16)

    def gather_values(c):
        row = (c % (nc // 2)) * CROWS
        for p in range(16):
            part = weighted(8 + p, fsv[p, row : row + CROWS, :], row, row + CROWS)
            if row == 0:
                pvacc[p] = part
            else:
                pvacc[p] = pvacc[p] + part

    gather_values(4)
    z_start(6)
    finish(5)
    gather_values(5)
    z_start(7)
    finish(6)
    gather_values(6)
    finish(7)
    for p in range(16):
        row = 3 * CROWS
        place(8 + p, pvacc[p] + weighted(8 + p, fsv[p, row : row + CROWS, :], row, row + CROWS))

    tiles = [accs[h] for h in range(16)]
    group = lane32 // 8
    for bit in (1, 2, 4, 8):
        upper = (group & bit) != 0
        for h in range(16):
            if h & bit == 0:
                a, b = tiles[h], tiles[h + bit]
                tiles[h] = jnp.where(upper, pltpu.roll(b, 8 * bit, 1), a)
                tiles[h + bit] = jnp.where(upper, b, pltpu.roll(a, 128 - 8 * bit, 1))
    for j in range(16):
        msend[j] = tiles[j].astype(bf16)
    m_copies = {}
    for k in ORDER[::-1]:
        m_copies[k] = remote(msend.at[peer_of(x, y, k)], mrecv.at[kv], m_ss.at[k], m_rs.at[k], dev(k))
    mrecv[kv] = msend[kv]
    for k in ORDER:
        m_copies[k].wait_recv()
    attn_ref[...] = jnp.dot(
        member, mrecv[...].reshape(512, 128), preferred_element_type=f32
    ).astype(bf16)

    for copies in (q_copies, a_copies, x_copies, z_copies, s_copies, m_copies):
        for copy in copies.values():
            copy.wait_send()
    for copy in out_copies:
        copy.wait()


def head(meta, hidden, gain, token_kv, w_query, pool, resident):
    bf16, f32 = jnp.bfloat16, jnp.float32
    vmem = pl.BlockSpec(memory_space=pltpu.VMEM)
    hbm = pl.BlockSpec(memory_space=pl.ANY)
    dma = pltpu.SemaphoreType.DMA
    nc = CHUNKS
    chunk = lambda *lead: [pltpu.VMEM((*lead, CROWS, 512), bf16)] * nc
    return pl.pallas_call(
        head_kernel,
        name="head",
        out_shape=(
            jax.ShapeDtypeStruct((128, 128), bf16),
            jax.ShapeDtypeStruct((16, 2, 128, 512), bf16),
        ),
        in_specs=[pl.BlockSpec(memory_space=pltpu.SMEM), vmem, vmem, vmem, hbm, hbm, hbm],
        out_specs=(vmem, hbm),
        scratch_shapes=[
            pltpu.VMEM((256, 2048), bf16),
            pltpu.VMEM((8, 2, 128, 512), bf16),
            pltpu.VMEM((16, 8, 2176), f32),
            pltpu.VMEM((16, 8, 2176), f32),
            pltpu.VMEM((128, 16, 128), f32),
            pltpu.VMEM((8, 2048), f32),
            pltpu.VMEM((16, 128, 512), bf16),
            pltpu.VMEM((16, 128, 512), bf16),
            pltpu.VMEM((24, 16, 128), f32),
            pltpu.VMEM((24, 16, 128), f32),
            pltpu.VMEM((16, 16, 512), f32),
            pltpu.VMEM((16, 32, 128), f32),
            pltpu.VMEM((16, 32, 128), f32),
            pltpu.VMEM((16, 32, 128), bf16),
            pltpu.VMEM((16, 32, 128), bf16),
            *chunk(16), *chunk(15), *chunk(16), *chunk(3, 4), *chunk(4, 4),
            dma((1,)), dma((nc,)), dma((1,)), dma((nc,)),
            dma((16,)), dma((16,)), dma((16,)), dma((16,)),
            dma((nc, 16)), dma((nc, 16)), dma((nc, 4)), dma((nc, 4)),
            dma((16,)), dma((16,)), dma((16,)), dma((16,)),
        ],
        compiler_params=pltpu.CompilerParams(
            collective_id=1, has_side_effects=True, vmem_limit_bytes=60 * 1024 * 1024
        ),
    )(meta, hidden, gain, token_kv, w_query, pool, resident)


def routing(new_owner, new_local, resident_slot, resident_len, new_slot, new_len):
    i32 = jnp.int32
    grp, kv = lax.axis_index("grp"), lax.axis_index("kv")
    owners = new_owner.reshape(4, 16, 16)
    places = new_local.reshape(4, 16, 16)
    mine = (owners == grp * 16 + kv).astype(i32)
    pick = jnp.sum(mine * places, axis=(0, 2))
    column = lax.dynamic_index_in_dim(owners, kv, 1, keepdims=False)
    from_grp = column // 16
    earlier = jnp.arange(16)[None, :] < jnp.arange(16)[:, None]
    same = (from_grp[:, :, None] == from_grp[:, None, :]) & earlier[None]
    rank = jnp.sum(same.astype(i32), axis=2)
    hit = (from_grp == grp)[:, None, :] & (rank[:, None, :] == jnp.arange(4)[None, :, None])
    onward = jnp.sum(jnp.where(hit, (column % 16)[:, None, :], 0), axis=2).reshape(16)
    final = lax.dynamic_index_in_dim(from_grp * 4 + rank, grp, 0, keepdims=False)
    return jnp.concatenate(
        [pick, onward, final, resident_slot[0], resident_len[0], new_slot[0], new_len[0]]
    ).astype(i32)


def per_device(
    hidden_states,
    attn_gain,
    mlp_gain,
    w_query,
    w_out,
    w_gate,
    w_up,
    w_down,
    kv_pool,
    resident_cache,
    resident_slot,
    resident_len,
    new_owner,
    new_local,
    new_slot,
    new_len,
    token_kv,
):
    meta = routing(new_owner, new_local, resident_slot, resident_len, new_slot, new_len)
    piece, new_pages = head(
        meta,
        hidden_states,
        attn_gain.reshape(1, 256),
        token_kv.reshape(128, 1024),
        w_query,
        kv_pool.reshape(16, 256, 512),
        resident_cache[0],
    )
    mixed = tail(
        piece,
        hidden_states,
        mlp_gain.reshape(16, 256),
        w_out.reshape(128, 4096),
        w_gate,
        w_up,
        w_down,
    )
    return (mixed, new_pages[None])


def solution(mesh):
    return jax.shard_map(
        per_device,
        mesh=mesh,
        in_specs=(
            P("grp", "kv"),
            P("kv"),
            P(),
            P("kv", "tp"),
            P("tp", "kv", None),
            P(None, KV_TP),
            P(None, KV_TP),
            P(KV_TP, None),
            P(GRP_KV, None, None, "tp"),
            P("grp", "kv", None, None, "tp"),
            P("grp", "kv"),
            P("grp", "kv"),
            P(),
            P(),
            P("grp", "kv"),
            P("grp", "kv"),
            P("grp", None, "tp"),
        ),
        out_specs=(P(GRP_KV_TP, None), P("grp", "kv", None, None, "tp")),
        check_vma=False,
    )
```

```python
import jax
import jax.numpy as jnp
from jax import lax
from jax.experimental import pallas as pl
from jax.experimental.pallas import tpu as pltpu
from jax.sharding import PartitionSpec as P

D = 4096
HEADS = 32
KV_HEADS = 8
HEAD_DIM = 128
KV_TP = ("kv", "tp")
GRP_KV = ("grp", "kv")
GRP_KV_TP = ("grp", "kv", "tp")


neg_fill = -1e30
norm_eps = 1e-05
MESH = pl.DeviceIdType.MESH


def peer_of(x, y, k):
    return lax.rem(x + k // 4, 4) * 4 + lax.rem(y + k % 4, 4)


def source_of(x, y, k):
    return lax.rem(x + 4 - k // 4, 4) * 4 + lax.rem(y + 4 - k % 4, 4)


ORDER = sorted(range(1, 16), key=lambda k: (min(k // 4, 4 - k // 4) + min(k % 4, 4 - k % 4), k))


def tail_kernel(
    attn_ref, hid_ref, gain_ref, wout_hbm, wg_hbm, wu_hbm, wd_hbm, out_ref,
    wout, wg, wu, wd, pair_send, pair_recv, own_part, rs_send, rs_recv, ag, hunits,
    dp_send, dp_recv, dsum, d_send, d_recv, resrow,
    w_sem, pair_ss, pair_rs, rs_ss, rs_rs, ag_ss, ag_rs, fw_ss, fw_rs, dp_ss, dp_rs, d_ss, d_rs,
):
    f32, bf16 = jnp.float32, jnp.bfloat16
    grp, kv, tp = lax.axis_index("grp"), lax.axis_index("kv"), lax.axis_index("tp")
    x, y = kv // 4, lax.rem(kv, 4)
    other = 1 - tp
    partner = (grp, kv, other)

    def dev(k):
        return (grp, peer_of(x, y, k), tp)

    loads = [
        pltpu.make_async_copy(src, dst, w_sem.at[i])
        for i, (src, dst) in enumerate([(wout_hbm, wout), (wg_hbm, wg), (wu_hbm, wu), (wd_hbm, wd)])
    ]
    for load in loads:
        load.start()

    barrier = pltpu.get_barrier_semaphore()
    pl.semaphore_signal(barrier, inc=1, device_id=partner, device_id_type=MESH)
    for k in range(1, 16):
        pl.semaphore_signal(barrier, inc=1, device_id=dev(k), device_id_type=MESH)

    rho = lax.broadcasted_iota(jnp.int32, (128, 128), 0)
    col = lax.broadcasted_iota(jnp.int32, (128, 128), 1)
    slot = (lax.rem(rho, 64) // 4) * 8 + (rho // 64) * 4 + lax.rem(rho, 4)
    perm = jnp.where(col == slot, 1.0, 0.0).astype(bf16)
    attn = jnp.dot(perm, attn_ref[...], preferred_element_type=f32).astype(bf16)
    hid = jnp.dot(
        perm, hid_ref[:, pl.ds(pl.multiple_of(tp * 128, 128), 128)], preferred_element_type=f32
    )

    loads[0].wait()
    pl.semaphore_wait(barrier, 16)

    order = ORDER[::-1] + [0]
    pair_copies = []
    for g in range(4):
        for i in range(4):
            k = order[4 * g + i]
            dest = peer_of(x, y, k)
            part = jnp.dot(
                attn, wout[:, pl.ds(pl.multiple_of(dest * 256, 256), 256)], preferred_element_type=f32
            )
            low, high = part[:, :128], part[:, 128:]
            own_part[g, i] = jnp.where(tp == 0, low, high)
            pair_send[g, i] = jnp.where(tp == 0, high, low).astype(bf16)
        copy = pltpu.make_async_remote_copy(
            src_ref=pair_send.at[g], dst_ref=pair_recv.at[g], send_sem=pair_ss.at[g],
            recv_sem=pair_rs.at[g], device_id=partner, device_id_type=MESH,
        )
        copy.start()
        pair_copies.append(copy)
    rs_copies = {}
    block = None
    for g in range(4):
        pair_copies[g].wait_recv()
        for i in range(4):
            k = order[4 * g + i]
            total = own_part[g, i] + pair_recv[g, i].astype(f32)
            if k == 0:
                block = total + hid
            else:
                rs_send[k] = total.astype(bf16)
                copy = pltpu.make_async_remote_copy(
                    src_ref=rs_send.at[k], dst_ref=rs_recv.at[k], send_sem=rs_ss.at[k],
                    recv_sem=rs_rs.at[k], device_id=dev(k), device_id_type=MESH,
                )
                copy.start()
                rs_copies[k] = copy
    for k in ORDER:
        rs_copies[k].wait_recv()
        block = block + rs_recv[k].astype(f32)
    ag[0, tp] = block.astype(bf16)

    ag_copies = {}
    fw_copies = {}

    def forward(k):
        copy = pltpu.make_async_remote_copy(
            src_ref=ag.at[k, tp], dst_ref=ag.at[k, tp], send_sem=fw_ss.at[k],
            recv_sem=fw_rs.at[k], device_id=partner, device_id_type=MESH,
        )
        copy.start()
        fw_copies[k] = copy

    for k in ORDER[::-1]:
        copy = pltpu.make_async_remote_copy(
            src_ref=ag.at[0, tp], dst_ref=ag.at[k, tp], send_sem=ag_ss.at[k],
            recv_sem=ag_rs.at[k], device_id=dev(k), device_id_type=MESH,
        )
        copy.start()
        ag_copies[k] = copy
    forward(0)
    for g in range(4):
        pair_copies[g].wait_send()
    loads[1].wait()
    loads[2].wait()
    seq = [0] + ORDER
    nt = (((1,), (1,)), ((), ()))
    gate = jnp.zeros((128, 448), f32)
    upward = jnp.zeros((128, 448), f32)
    squares = jnp.zeros((128, 128), f32)
    mine = lax.broadcasted_iota(jnp.int32, (8, 128), 0) + tp * 64 + kv * 4
    pick = jnp.where(lax.broadcasted_iota(jnp.int32, (8, 128), 1) == mine, 1.0, 0.0).astype(bf16)
    for n, k in enumerate(seq):
        if n + 1 < 16:
            ag_copies[seq[n + 1]].wait_recv()
            forward(seq[n + 1])
        fw_copies[k].wait_recv()
        src = source_of(x, y, k)
        both = jnp.concatenate([ag[k, 0], ag[k, 1]], axis=1)
        wide = both.astype(f32)
        squares = squares + wide[:, :128] * wide[:, :128] + wide[:, 128:] * wide[:, 128:]
        rows = pl.ds(pl.multiple_of(src * 256, 256), 256)
        normed = (wide * gain_ref[:, rows]).astype(bf16)
        gate = gate + lax.dot_general(normed, wg[:, rows], nt, preferred_element_type=f32)
        upward = upward + lax.dot_general(normed, wu[:, rows], nt, preferred_element_type=f32)
    scale = lax.rsqrt(jnp.sum(squares, axis=1, keepdims=True) / D + norm_eps)
    gate = gate * scale
    upward = upward * scale
    hunits[...] = (gate / (1.0 + jnp.exp(-gate)) * upward).astype(bf16)

    loads[3].wait()
    dp_copies = []
    for c in range(4):
        cols = pl.ds(c * 1024, 1024)
        part = jnp.dot(hunits[...], wd[:, cols], preferred_element_type=f32)
        first, second = part[:64], part[64:]
        dsum[:, cols] = jnp.where(tp == 0, first, second)
        dp_send[c] = jnp.where(tp == 0, second, first).astype(bf16)
        copy = pltpu.make_async_remote_copy(
            src_ref=dp_send.at[c], dst_ref=dp_recv.at[c], send_sem=dp_ss.at[c],
            recv_sem=dp_rs.at[c], device_id=partner, device_id_type=MESH,
        )
        copy.start()
        dp_copies.append(copy)
    for c in range(4):
        dp_copies[c].wait_recv()
        cols = pl.ds(c * 1024, 1024)
        dsum[:, cols] = dsum[:, cols] + dp_recv[c].astype(f32)
    for j in range(16):
        d_send[j] = dsum[4 * j : 4 * j + 4, :].astype(bf16)
    d_copies = {}
    for k in ORDER[::-1]:
        copy = pltpu.make_async_remote_copy(
            src_ref=d_send.at[peer_of(x, y, k)], dst_ref=d_recv.at[k], send_sem=d_ss.at[k],
            recv_sem=d_rs.at[k], device_id=dev(k), device_id_type=MESH,
        )
        copy.start()
        d_copies[k] = copy
    for k in range(16):
        for t in range(2):
            cols = pl.ds(pl.multiple_of((source_of(x, y, k) * 2 + t) * 128, 128), 128)
            resrow[:, cols] = jnp.dot(pick, ag[k, t], preferred_element_type=f32)
    pick64 = lax.broadcasted_iota(jnp.int32, (8, 64), 0) + kv * 4
    total = resrow[...][:4]
    lane = lax.broadcasted_iota(jnp.int32, (4, 4096), 0)
    own = jnp.zeros((4, 4096), f32)
    for j in range(16):
        own = jnp.where(kv == j, dsum[4 * j : 4 * j + 4, :], own)
    total = total + own
    for k in ORDER:
        d_copies[k].wait_recv()
        total = total + d_recv[k].astype(f32)
    out_ref[...] = total.astype(bf16)

    for k in range(1, 16):
        rs_copies[k].wait_send()
        ag_copies[k].wait_send()
        d_copies[k].wait_send()
    for k in range(16):
        fw_copies[k].wait_send()
    for c in range(4):
        dp_copies[c].wait_send()


def tail(attn, hidden, gain, w_out, w_gate, w_up, w_down):
    bf16, f32 = jnp.bfloat16, jnp.float32
    vmem = pl.BlockSpec(memory_space=pltpu.VMEM)
    hbm = pl.BlockSpec(memory_space=pl.ANY)
    dma = pltpu.SemaphoreType.DMA
    return pl.pallas_call(
        tail_kernel,
        name="tail",
        out_shape=jax.ShapeDtypeStruct((4, 4096), bf16),
        in_specs=[vmem, vmem, vmem, hbm, hbm, hbm, hbm],
        out_specs=vmem,
        scratch_shapes=[
            pltpu.VMEM((128, 4096), bf16),
            pltpu.VMEM((448, 4096), bf16),
            pltpu.VMEM((448, 4096), bf16),
            pltpu.VMEM((448, 4096), bf16),
            pltpu.VMEM((4, 4, 128, 128), bf16),
            pltpu.VMEM((4, 4, 128, 128), bf16),
            pltpu.VMEM((4, 4, 128, 128), f32),
            pltpu.VMEM((16, 128, 128), bf16),
            pltpu.VMEM((16, 128, 128), bf16),
            pltpu.VMEM((16, 2, 128, 128), bf16),
            pltpu.VMEM((128, 448), bf16),
            pltpu.VMEM((4, 64, 1024), bf16),
            pltpu.VMEM((4, 64, 1024), bf16),
            pltpu.VMEM((64, 4096), f32),
            pltpu.VMEM((16, 4, 4096), bf16),
            pltpu.VMEM((16, 4, 4096), bf16),
            pltpu.VMEM((8, 4096), f32),
            dma((4,)), dma((4,)), dma((4,)), dma((16,)), dma((16,)), dma((16,)), dma((16,)),
            dma((16,)), dma((16,)), dma((4,)), dma((4,)), dma((16,)), dma((16,)),
        ],
        compiler_params=pltpu.CompilerParams(
            collective_id=0, has_side_effects=True, vmem_limit_bytes=60 * 1024 * 1024
        ),
    )(attn, hidden, gain, w_out, w_gate, w_up, w_down)


CHUNKS = 8
CROWS = 256 // CHUNKS
LOG_ROWS = 32


def head_kernel(
    meta, hid_ref, again_ref, tok_hbm, wq_hbm, pool_hbm, res_hbm, attn_ref, cache_hbm,
    wq, tok, kept, qs_send, qs_recv, qfull, qflat, fsk, fsv, scores, probs, pvacc, accs, stats, msend, mrecv, *rest,
):
    f32, bf16, i32 = jnp.float32, jnp.bfloat16, jnp.int32
    nc = CHUNKS
    pool, xs, xr, zs, zr = (rest[i * nc : (i + 1) * nc] for i in range(5))
    (ld_sem, pool_sem, kept_sem, out_sem, q_ss, q_rs, a_ss, a_rs, x_ss, x_rs, z_ss, z_rs, s_ss, s_rs,
     m_ss, m_rs) = rest[5 * nc :]
    grp, kv, tp = lax.axis_index("grp"), lax.axis_index("kv"), lax.axis_index("tp")
    x, y = kv // 4, lax.rem(kv, 4)

    def dev(k):
        return (grp, peer_of(x, y, k), tp)

    def zdev(dz):
        return (lax.rem(grp + dz, 4), kv, tp)

    def remote(src, dst, send, recv, device):
        copy = pltpu.make_async_remote_copy(
            src_ref=src, dst_ref=dst, send_sem=send, recv_sem=recv, device_id=device,
            device_id_type=MESH,
        )
        copy.start()
        return copy

    wq_load = pltpu.make_async_copy(wq_hbm, wq, ld_sem.at[0])
    wq_load.start()
    pool_loads = []
    for c in range(nc):
        load = pltpu.make_async_copy(pool_hbm.at[:, pl.ds(c * CROWS, CROWS), :], pool[c], pool_sem.at[c])
        load.start()
        pool_loads.append(load)
    kept_load = pltpu.make_async_copy(res_hbm, kept, kept_sem.at[0])
    kept_load.start()
    tok_load = pltpu.make_async_copy(
        tok_hbm.at[pl.ds(pl.multiple_of(kv * 8, 8), 8)], tok, ld_sem.at[1]
    )
    tok_load.start()

    barrier = pltpu.get_barrier_semaphore()
    for k in range(1, 16):
        pl.semaphore_signal(barrier, inc=1, device_id=dev(k), device_id_type=MESH)
    for dz in range(1, 4):
        pl.semaphore_signal(barrier, inc=1, device_id=zdev(dz), device_id_type=MESH)

    feats = hid_ref[...].astype(f32)
    normed = (feats * again_ref[...]).astype(bf16)
    squares = jnp.sum(feats * feats, axis=1, keepdims=True)
    wq_load.wait()
    for h in range(4):
        part = jnp.dot(normed, wq[:, h * 512 : h * 512 + 512], preferred_element_type=f32)
        qs_send[:, :, h * 512 : h * 512 + 512] = part.reshape(16, 8, 512)
    qs_send[:, :, 2048:2176] = jnp.broadcast_to(squares, (128, 128)).reshape(16, 8, 128)
    pl.semaphore_wait(barrier, 18)

    q_copies = {}
    for k in ORDER[::-1]:
        q_copies[k] = remote(qs_send.at[peer_of(x, y, k)], qs_recv.at[k], q_ss.at[k], q_rs.at[k], dev(k))

    x_copies = {}
    z_copies = {}
    out_copies = []

    def xy_start(c):
        pool_loads[c].wait()
        xr[c][kv] = pool[c][meta[kv]]
        for k in range(1, 16):
            xs[c][k - 1] = pool[c][meta[peer_of(x, y, k)]]
        for k in ORDER[::-1]:
            x_copies[c, k] = remote(
                xs[c].at[k - 1], xr[c].at[kv], x_ss.at[c, k], x_rs.at[c, k], dev(k)
            )

    def z_start(c):
        for k in ORDER:
            x_copies[c, k].wait_recv()
        for dz in range(4):
            g = lax.rem(grp + dz, 4)
            for r in range(4):
                page = xr[c][meta[16 + g * 4 + r]]
                if dz == 0:
                    zr[c][grp, r] = page
                else:
                    zs[c][dz - 1, r] = page
        for dz in (2, 1, 3):
            z_copies[c, dz] = remote(
                zs[c].at[dz - 1], zr[c].at[grp], z_ss.at[c, dz], z_rs.at[c, dz], zdev(dz)
            )

    def finish(c):
        for dz in (1, 3, 2):
            z_copies[c, dz].wait_recv()
        final, half = (fsk, 0) if c < nc // 2 else (fsv, 1)
        row = (c % (nc // 2)) * CROWS
        for i in range(16):
            where = meta[32 + i]
            final[i, row : row + CROWS, :] = zr[c][where // 4, lax.rem(where, 4)]
        copy = pltpu.make_async_copy(
            final.at[:, pl.ds(row, CROWS), :], cache_hbm.at[:, half, pl.ds(row, CROWS), :], out_sem.at[c]
        )
        copy.start()
        out_copies.append(copy)

    head_of = lax.broadcasted_iota(i32, (16, 512), 0) // 4
    block_of = lax.broadcasted_iota(i32, (16, 512), 1) // 128
    diag = head_of == block_of
    lanes = lax.broadcasted_iota(i32, (16, 128), 1)

    def page_scores(p, keys, slot, filled):
        q = qfull[slot]
        wide = jnp.where(diag, jnp.concatenate([q, q, q, q], axis=1), 0.0)
        high = wide.astype(bf16)
        left = wide - high.astype(f32)
        mid = left.astype(bf16)
        low = (left - mid.astype(f32)).astype(bf16)
        rows = jnp.concatenate([high, mid, low], axis=0)
        s = lax.dot_general(rows, keys, (((1,), (1,)), ((), ())), preferred_element_type=f32)
        s = s[:16] + s[16:32] + s[32:]
        s = jnp.where(lanes < filled, s, neg_fill)
        scores[p] = s
        top = jnp.max(s, axis=1, keepdims=True)
        total = jnp.sum(jnp.where(lanes < filled, jnp.exp(s - top), 0.0), axis=1, keepdims=True)
        return top, total

    def weighted(p, values, lo, hi):
        w = probs[p][:, lo:hi]
        high = w.astype(bf16)
        low = (w - high.astype(f32)).astype(bf16)
        out = jnp.dot(jnp.concatenate([high, low], axis=0), values, preferred_element_type=f32)
        return out[:16] + out[16:]

    def place(p, acc):
        for h in range(16):
            accs[h, p : p + 1, :] = acc[h : h + 1, (h // 4) * 128 : (h // 4) * 128 + 128]

    table = jnp.zeros((128, 128), f32)
    row128 = lax.broadcasted_iota(i32, (128, 128), 0)
    col128 = lax.broadcasted_iota(i32, (128, 128), 1)

    def note(table, p, top, total):
        both = jnp.concatenate([top, total, jnp.zeros((96, 1), f32)], axis=0)
        return jnp.where(col128 == p, both, table)

    def query_done():
        total = qs_send[kv]
        for k in ORDER:
            q_copies[k].wait_recv()
            total = total + qs_recv[k]
        scale = lax.rsqrt(total[:, 2048:2049] / D + norm_eps)
        q8 = total[:, :2048] * scale * HEAD_DIM ** (-0.5)
        qflat[...] = q8
        for h in range(16):
            qfull[pl.ds(pl.multiple_of(kv * 8, 8), 8), h, :] = q8[:, h * 128 : h * 128 + 128]
        mine = qfull.at[pl.ds(pl.multiple_of(kv * 8, 8), 8)]
        return {k: remote(mine, mine, a_ss.at[k], a_rs.at[k], dev(k)) for k in ORDER[::-1]}

    xy_start(0)
    xy_start(1)
    a_copies = query_done()
    xy_start(2)
    z_start(0)
    xy_start(3)
    z_start(1)
    finish(0)
    for k in ORDER:
        a_copies[k].wait_recv()
    kept_load.wait()
    for p in range(8):
        table = note(table, p, *page_scores(p, kept[p, 0], meta[48 + p], meta[56 + p]))
    xy_start(4)
    z_start(2)
    finish(1)
    xy_start(5)
    z_start(3)
    finish(2)
    xy_start(6)
    z_start(4)
    finish(3)
    for p in range(16):
        table = note(table, 8 + p, *page_scores(8 + p, fsk[p], meta[64 + p], meta[80 + p]))
    tok_load.wait()
    own_key, own_value = tok[:, 0, :].astype(f32), tok[:, 1, :].astype(f32)
    lane8 = lax.broadcasted_iota(i32, (8, 128), 1)
    own_rows = jnp.where((lane8 >= 16) & (lane8 < 32), 1.0, 0.0).astype(f32)
    for h in range(16):
        s = jnp.sum(
            qflat[:, h * 128 : h * 128 + 128] * own_key[:, (h // 4) * 128 : (h // 4) * 128 + 128],
            axis=1, keepdims=True,
        )
        own_rows = jnp.where(lane8 == h, s, own_rows)
    slots = jnp.zeros((32, 1), i32)
    row32 = lax.broadcasted_iota(i32, (32, 1), 0)
    for p in range(8):
        slots = jnp.where(row32 == p, meta[48 + p], slots)
    for p in range(16):
        slots = jnp.where(row32 == 8 + p, meta[64 + p], slots)
    slots = jnp.where(row32 >= 24, kv * 8 + row32 - 24, slots)
    lane32 = lax.broadcasted_iota(i32, (32, 128), 1)
    mine = jnp.concatenate([table.T[:24], own_rows], axis=0)
    mine = jnp.where(lane32 == 32, slots.astype(f32), mine)
    stats[kv] = mine
    s_copies = {
        k: remote(stats.at[kv], stats.at[kv], s_ss.at[k], s_rs.at[k], dev(k)) for k in ORDER[::-1]
    }
    xy_start(7)
    z_start(5)
    finish(4)
    for k in ORDER:
        s_copies[k].wait_recv()
    every = stats[...].reshape(512, 128)
    every_slot = every[:, 32:33].astype(i32)
    sums = pltpu.roll(every, 112, 1)
    lane512 = lax.broadcasted_iota(i32, (512, 128), 1)
    result = jnp.zeros((128, 128), f32)
    for p in range(32):
        slot = meta[48 + p] if p < 8 else (meta[64 + p - 8] if p < 24 else kv * 8 + p - 24)
        same = (every_slot == slot) & (lane512 < 16)
        top = jnp.max(jnp.where(same, every, neg_fill), axis=0, keepdims=True)
        total = jnp.sum(jnp.where(same, jnp.exp(every - top) * sums, 0.0), axis=0, keepdims=True)
        line = jnp.where(lane8[:1] < 16, top, pltpu.roll(1.0 / jnp.where(lane8[:1] < 16, total, 1.0), 16, 1))
        result = jnp.where(row128 == p, line, result)
    turned = result.T
    for p in range(24):
        probs[p] = jnp.exp(scores[p] - turned[:16, p : p + 1]) * turned[16:32, p : p + 1]
    for p in range(8):
        place(p, weighted(p, kept[p, 1], 0, 128))
    own_weight = jnp.exp(own_rows - result[24:32]) * pltpu.roll(result[24:32], 112, 1)
    for h in range(16):
        g = (h // 4) * 128
        accs[h, 24:32, :] = own_weight[:, h : h + 1] * own_value[:, g : g + 128]
    member = jnp.where(every_slot == lane512, 1.0, 0.0).astype(f32)
    member = jnp.concatenate([member[128 * i : 128 * i + 128].T for i in range(4)], axis=1).astype(bf16)

    def gather_values(c):
        row = (c % (nc // 2)) * CROWS
        for p in range(16):
            part = weighted(8 + p, fsv[p, row : row + CROWS, :], row, row + CROWS)
            if row == 0:
                pvacc[p] = part
            else:
                pvacc[p] = pvacc[p] + part

    gather_values(4)
    z_start(6)
    finish(5)
    gather_values(5)
    z_start(7)
    finish(6)
    gather_values(6)
    finish(7)
    for p in range(16):
        row = 3 * CROWS
        place(8 + p, pvacc[p] + weighted(8 + p, fsv[p, row : row + CROWS, :], row, row + CROWS))

    tiles = [accs[h] for h in range(16)]
    group = lane32 // 8
    for bit in (1, 2, 4, 8):
        upper = (group & bit) != 0
        for h in range(16):
            if h & bit == 0:
                a, b = tiles[h], tiles[h + bit]
                tiles[h] = jnp.where(upper, pltpu.roll(b, 8 * bit, 1), a)
                tiles[h + bit] = jnp.where(upper, b, pltpu.roll(a, 128 - 8 * bit, 1))
    for j in range(16):
        msend[j] = tiles[j].astype(bf16)
    m_copies = {}
    for k in ORDER[::-1]:
        m_copies[k] = remote(msend.at[peer_of(x, y, k)], mrecv.at[kv], m_ss.at[k], m_rs.at[k], dev(k))
    mrecv[kv] = msend[kv]
    for k in ORDER:
        m_copies[k].wait_recv()
    attn_ref[...] = jnp.dot(
        member, mrecv[...].reshape(512, 128), preferred_element_type=f32
    ).astype(bf16)

    for copies in (q_copies, a_copies, x_copies, z_copies, s_copies, m_copies):
        for copy in copies.values():
            copy.wait_send()
    for copy in out_copies:
        copy.wait()


def head(meta, hidden, gain, token_kv, w_query, pool, resident):
    bf16, f32 = jnp.bfloat16, jnp.float32
    vmem = pl.BlockSpec(memory_space=pltpu.VMEM)
    hbm = pl.BlockSpec(memory_space=pl.ANY)
    dma = pltpu.SemaphoreType.DMA
    nc = CHUNKS
    chunk = lambda *lead: [pltpu.VMEM((*lead, CROWS, 512), bf16)] * nc
    return pl.pallas_call(
        head_kernel,
        name="head",
        out_shape=(
            jax.ShapeDtypeStruct((128, 128), bf16),
            jax.ShapeDtypeStruct((16, 2, 128, 512), bf16),
        ),
        in_specs=[pl.BlockSpec(memory_space=pltpu.SMEM), vmem, vmem, hbm, hbm, hbm, hbm],
        out_specs=(vmem, hbm),
        scratch_shapes=[
            pltpu.VMEM((256, 2048), bf16),
            pltpu.VMEM((8, 2, 512), bf16),
            pltpu.VMEM((8, 2, 128, 512), bf16),
            pltpu.VMEM((16, 8, 2176), f32),
            pltpu.VMEM((16, 8, 2176), f32),
            pltpu.VMEM((128, 16, 128), f32),
            pltpu.VMEM((8, 2048), f32),
            pltpu.VMEM((16, 128, 512), bf16),
            pltpu.VMEM((16, 128, 512), bf16),
            pltpu.VMEM((24, 16, 128), f32),
            pltpu.VMEM((24, 16, 128), f32),
            pltpu.VMEM((16, 16, 512), f32),
            pltpu.VMEM((16, 32, 128), f32),
            pltpu.VMEM((16, 32, 128), f32),
            pltpu.VMEM((16, 32, 128), bf16),
            pltpu.VMEM((16, 32, 128), bf16),
            *chunk(16), *chunk(15), *chunk(16), *chunk(3, 4), *chunk(4, 4),
            dma((2,)), dma((nc,)), dma((1,)), dma((nc,)),
            dma((16,)), dma((16,)), dma((16,)), dma((16,)),
            dma((nc, 16)), dma((nc, 16)), dma((nc, 4)), dma((nc, 4)),
            dma((16,)), dma((16,)), dma((16,)), dma((16,)),
        ],
        compiler_params=pltpu.CompilerParams(
            collective_id=1, has_side_effects=True, vmem_limit_bytes=60 * 1024 * 1024
        ),
    )(meta, hidden, gain, token_kv, w_query, pool, resident)


def routing(new_owner, new_local, resident_slot, resident_len, new_slot, new_len):
    i32 = jnp.int32
    grp, kv = lax.axis_index("grp"), lax.axis_index("kv")
    owners = new_owner.reshape(4, 16, 16)
    places = new_local.reshape(4, 16, 16)
    mine = (owners == grp * 16 + kv).astype(i32)
    pick = jnp.sum(mine * places, axis=(0, 2))
    column = lax.dynamic_index_in_dim(owners, kv, 1, keepdims=False)
    from_grp = column // 16
    earlier = jnp.arange(16)[None, :] < jnp.arange(16)[:, None]
    same = (from_grp[:, :, None] == from_grp[:, None, :]) & earlier[None]
    rank = jnp.sum(same.astype(i32), axis=2)
    hit = (from_grp == grp)[:, None, :] & (rank[:, None, :] == jnp.arange(4)[None, :, None])
    onward = jnp.sum(jnp.where(hit, (column % 16)[:, None, :], 0), axis=2).reshape(16)
    final = lax.dynamic_index_in_dim(from_grp * 4 + rank, grp, 0, keepdims=False)
    return jnp.concatenate(
        [pick, onward, final, resident_slot[0], resident_len[0], new_slot[0], new_len[0]]
    ).astype(i32)


def per_device(
    hidden_states,
    attn_gain,
    mlp_gain,
    w_query,
    w_out,
    w_gate,
    w_up,
    w_down,
    kv_pool,
    resident_cache,
    resident_slot,
    resident_len,
    new_owner,
    new_local,
    new_slot,
    new_len,
    token_kv,
):
    meta = routing(new_owner, new_local, resident_slot, resident_len, new_slot, new_len)
    piece, new_pages = head(
        meta,
        hidden_states,
        attn_gain.reshape(1, 256),
        token_kv,
        w_query,
        kv_pool.reshape(16, 256, 512),
        resident_cache[0],
    )
    mixed = tail(
        piece,
        hidden_states,
        mlp_gain.reshape(1, 4096),
        w_out.reshape(128, 4096),
        w_gate.T,
        w_up.T,
        w_down,
    )
    return (mixed, new_pages[None])


def solution(mesh):
    return jax.shard_map(
        per_device,
        mesh=mesh,
        in_specs=(
            P("grp", "kv"),
            P("kv"),
            P(),
            P("kv", "tp"),
            P("tp", "kv", None),
            P(None, KV_TP),
            P(None, KV_TP),
            P(KV_TP, None),
            P(GRP_KV, None, None, "tp"),
            P("grp", "kv", None, None, "tp"),
            P("grp", "kv"),
            P("grp", "kv"),
            P(),
            P(),
            P("grp", "kv"),
            P("grp", "kv"),
            P("grp", None, "tp"),
        ),
        out_specs=(P(GRP_KV_TP, None), P("grp", "kv", None, None, "tp")),
        check_vma=False,
    )
```

```python
import jax
import jax.numpy as jnp
from jax import lax
from jax.experimental import pallas as pl
from jax.experimental.pallas import tpu as pltpu
from jax.sharding import PartitionSpec as P

D = 4096
HEADS = 32
KV_HEADS = 8
HEAD_DIM = 128
KV_TP = ("kv", "tp")
GRP_KV = ("grp", "kv")
GRP_KV_TP = ("grp", "kv", "tp")


neg_fill = -1e30
norm_eps = 1e-05
MESH = pl.DeviceIdType.MESH


def peer_of(x, y, k):
    return lax.rem(x + k // 4, 4) * 4 + lax.rem(y + k % 4, 4)


def source_of(x, y, k):
    return lax.rem(x + 4 - k // 4, 4) * 4 + lax.rem(y + 4 - k % 4, 4)


ORDER = sorted(range(1, 16), key=lambda k: (min(k // 4, 4 - k // 4) + min(k % 4, 4 - k % 4), k))


CHUNKS = 8
CROWS = 256 // CHUNKS


def step_kernel(
    meta, hid_ref, again_ref, gain_ref, tok_hbm, wq_hbm, pool_hbm, res_hbm, wout_hbm, wg_hbm, wu_hbm, wd_hbm,
    out_ref, cache_hbm,
    wq, tok, kept, qs_send, qs_recv, qfull, qflat, fsk, fsv, scores, probs, pvacc, accs, stats, msend, mrecv,
    wout, wg, wu, wd, pair_send, pair_recv, own_part, rs_send, rs_recv, ag, hunits,
    dp_send, dp_recv, dsum, d_send, d_recv, resrow, *rest,
):
    f32, bf16, i32 = jnp.float32, jnp.bfloat16, jnp.int32
    nc = CHUNKS
    pool, xs, xr, zs, zr = (rest[i * nc : (i + 1) * nc] for i in range(5))
    (ld_sem, pool_sem, kept_sem, out_sem, q_ss, q_rs, a_ss, a_rs, x_ss, x_rs, z_ss, z_rs, s_ss, s_rs,
     m_ss, m_rs, w_sem, pair_ss, pair_rs, rs_ss, rs_rs, ag_ss, ag_rs, fw_ss, fw_rs, dp_ss, dp_rs, d_ss,
     d_rs) = rest[5 * nc :]
    grp, kv, tp = lax.axis_index("grp"), lax.axis_index("kv"), lax.axis_index("tp")
    x, y = kv // 4, lax.rem(kv, 4)
    other = 1 - tp
    partner = (grp, kv, other)

    def dev(k):
        return (grp, peer_of(x, y, k), tp)

    def zdev(dz):
        return (lax.rem(grp + dz, 4), kv, tp)

    def remote(src, dst, send, recv, device):
        copy = pltpu.make_async_remote_copy(
            src_ref=src, dst_ref=dst, send_sem=send, recv_sem=recv, device_id=device,
            device_id_type=MESH,
        )
        copy.start()
        return copy

    wq_load = pltpu.make_async_copy(wq_hbm, wq, ld_sem.at[0])
    wq_load.start()
    pool_loads = []
    for c in range(nc):
        load = pltpu.make_async_copy(pool_hbm.at[:, pl.ds(c * CROWS, CROWS), :], pool[c], pool_sem.at[c])
        load.start()
        pool_loads.append(load)
    kept_load = pltpu.make_async_copy(res_hbm, kept, kept_sem.at[0])
    kept_load.start()
    tok_load = pltpu.make_async_copy(
        tok_hbm.at[pl.ds(pl.multiple_of(kv * 8, 8), 8)], tok, ld_sem.at[1]
    )
    tok_load.start()

    loads = [
        pltpu.make_async_copy(src, dst, w_sem.at[i])
        for i, (src, dst) in enumerate([(wout_hbm, wout), (wg_hbm, wg), (wu_hbm, wu), (wd_hbm, wd)])
    ]
    for load in loads:
        load.start()

    barrier = pltpu.get_barrier_semaphore()
    pl.semaphore_signal(barrier, inc=1, device_id=partner, device_id_type=MESH)
    for k in range(1, 16):
        pl.semaphore_signal(barrier, inc=1, device_id=dev(k), device_id_type=MESH)
    for dz in range(1, 4):
        pl.semaphore_signal(barrier, inc=1, device_id=zdev(dz), device_id_type=MESH)

    feats = hid_ref[...].astype(f32)
    normed = (feats * again_ref[...]).astype(bf16)
    squares = jnp.sum(feats * feats, axis=1, keepdims=True)
    wq_load.wait()
    for h in range(4):
        part = jnp.dot(normed, wq[:, h * 512 : h * 512 + 512], preferred_element_type=f32)
        qs_send[:, :, h * 512 : h * 512 + 512] = part.reshape(16, 8, 512)
    qs_send[:, :, 2048:2176] = jnp.broadcast_to(squares, (128, 128)).reshape(16, 8, 128)
    pl.semaphore_wait(barrier, 19)

    q_copies = {}
    for k in ORDER[::-1]:
        q_copies[k] = remote(qs_send.at[peer_of(x, y, k)], qs_recv.at[k], q_ss.at[k], q_rs.at[k], dev(k))

    x_copies = {}
    z_copies = {}
    out_copies = []

    def xy_start(c):
        pool_loads[c].wait()
        xr[c][kv] = pool[c][meta[kv]]
        for k in range(1, 16):
            xs[c][k - 1] = pool[c][meta[peer_of(x, y, k)]]
        for k in ORDER[::-1]:
            x_copies[c, k] = remote(
                xs[c].at[k - 1], xr[c].at[kv], x_ss.at[c, k], x_rs.at[c, k], dev(k)
            )

    def z_start(c):
        for k in ORDER:
            x_copies[c, k].wait_recv()
        for dz in range(4):
            g = lax.rem(grp + dz, 4)
            for r in range(4):
                page = xr[c][meta[16 + g * 4 + r]]
                if dz == 0:
                    zr[c][grp, r] = page
                else:
                    zs[c][dz - 1, r] = page
        for dz in (2, 1, 3):
            z_copies[c, dz] = remote(
                zs[c].at[dz - 1], zr[c].at[grp], z_ss.at[c, dz], z_rs.at[c, dz], zdev(dz)
            )

    def finish(c):
        for dz in (1, 3, 2):
            z_copies[c, dz].wait_recv()
        final, half = (fsk, 0) if c < nc // 2 else (fsv, 1)
        row = (c % (nc // 2)) * CROWS
        for i in range(16):
            where = meta[32 + i]
            final[i, row : row + CROWS, :] = zr[c][where // 4, lax.rem(where, 4)]
        copy = pltpu.make_async_copy(
            final.at[:, pl.ds(row, CROWS), :], cache_hbm.at[:, half, pl.ds(row, CROWS), :], out_sem.at[c]
        )
        copy.start()
        out_copies.append(copy)

    head_of = lax.broadcasted_iota(i32, (16, 512), 0) // 4
    block_of = lax.broadcasted_iota(i32, (16, 512), 1) // 128
    diag = head_of == block_of
    lanes = lax.broadcasted_iota(i32, (16, 128), 1)

    def page_scores(p, keys, slot, filled):
        q = qfull[slot]
        wide = jnp.where(diag, jnp.concatenate([q, q, q, q], axis=1), 0.0)
        high = wide.astype(bf16)
        left = wide - high.astype(f32)
        mid = left.astype(bf16)
        low = (left - mid.astype(f32)).astype(bf16)
        rows = jnp.concatenate([high, mid, low], axis=0)
        s = lax.dot_general(rows, keys, (((1,), (1,)), ((), ())), preferred_element_type=f32)
        s = s[:16] + s[16:32] + s[32:]
        s = jnp.where(lanes < filled, s, neg_fill)
        scores[p] = s
        top = jnp.max(s, axis=1, keepdims=True)
        total = jnp.sum(jnp.where(lanes < filled, jnp.exp(s - top), 0.0), axis=1, keepdims=True)
        return top, total

    def weighted(p, values, lo, hi):
        w = probs[p][:, lo:hi]
        high = w.astype(bf16)
        low = (w - high.astype(f32)).astype(bf16)
        out = jnp.dot(jnp.concatenate([high, low], axis=0), values, preferred_element_type=f32)
        return out[:16] + out[16:]

    def place(p, acc):
        for h in range(16):
            accs[h, p : p + 1, :] = acc[h : h + 1, (h // 4) * 128 : (h // 4) * 128 + 128]

    lane32 = lax.broadcasted_iota(i32, (32, 128), 1)

    def note(table, p, top, total):
        return jnp.where(lane32 == p, jnp.concatenate([top, total], axis=0), table)

    def query_done():
        total = qs_send[kv]
        for k in ORDER:
            q_copies[k].wait_recv()
            total = total + qs_recv[k]
        scale = lax.rsqrt(total[:, 2048:2049] / D + norm_eps)
        q8 = total[:, :2048] * scale * HEAD_DIM ** (-0.5)
        qflat[...] = q8
        for h in range(16):
            qfull[pl.ds(pl.multiple_of(kv * 8, 8), 8), h, :] = q8[:, h * 128 : h * 128 + 128]
        mine = qfull.at[pl.ds(pl.multiple_of(kv * 8, 8), 8)]
        return {k: remote(mine, mine, a_ss.at[k], a_rs.at[k], dev(k)) for k in ORDER[::-1]}

    for c in range(3):
        xy_start(c)
    a_copies = query_done()
    xy_start(3)
    z_start(0)
    xy_start(4)
    z_start(1)
    finish(0)
    xy_start(5)
    z_start(2)
    finish(1)
    xy_start(6)
    z_start(3)
    finish(2)
    xy_start(7)
    tok_load.wait()
    own_key, own_value = tok[:, 0, :].astype(f32), tok[:, 1, :].astype(f32)
    lane8 = lax.broadcasted_iota(i32, (8, 128), 1)
    own_rows = jnp.zeros((8, 128), f32)
    for h in range(16):
        s = jnp.sum(
            qflat[:, h * 128 : h * 128 + 128] * own_key[:, (h // 4) * 128 : (h // 4) * 128 + 128],
            axis=1, keepdims=True,
        )
        own_rows = jnp.where(lane8 == h, s, own_rows)
    own_tops = jnp.concatenate([jnp.zeros((24, 128), f32), own_rows, jnp.zeros((96, 128), f32)], axis=0).T[:16]
    slot_row = jnp.zeros((8, 128), i32)
    for p in range(24):
        slot_row = jnp.where(lane8 == p, meta[48 + p] if p < 8 else meta[56 + p], slot_row)
    slot_row = jnp.where(lane8 >= 24, kv * 8 + lane8 - 24, slot_row)
    for k in ORDER:
        a_copies[k].wait_recv()
    kept_load.wait()
    table = jnp.zeros((32, 128), f32)
    for p in range(8):
        table = note(table, p, *page_scores(p, kept[p, 0], meta[48 + p], meta[56 + p]))
    z_start(4)
    finish(3)
    for p in range(16):
        table = note(table, 8 + p, *page_scores(8 + p, fsk[p], meta[64 + p], meta[80 + p]))
    own_lane = lanes >= 24
    mine = jnp.concatenate(
        [
            jnp.where(own_lane, own_tops, table[:16]),
            jnp.where(own_lane, 1.0, table[16:]),
            slot_row.astype(f32),
        ],
        axis=0,
    )
    mine = jnp.where(lax.broadcasted_iota(i32, (40, 128), 1) < 32, mine, 0.0)
    turned = [mine] + [pltpu.roll(mine, 32 * q, 1) for q in range(1, 4)]
    for q in range(1, 4):
        mine = jnp.where(y == q, turned[q], mine)
    stats[kv] = mine
    s_copies = {
        k: remote(stats.at[kv], stats.at[kv], s_ss.at[k], s_rs.at[k], dev(k)) for k in ORDER[::-1]
    }
    z_start(5)
    finish(4)
    for k in ORDER:
        s_copies[k].wait_recv()
    every = jnp.concatenate(
        [stats[4 * i] + stats[4 * i + 1] + stats[4 * i + 2] + stats[4 * i + 3] for i in range(4)], axis=1
    )
    tops, sums, every_slot = every[:16], every[16:32], every[32:33].astype(i32)
    own_w = jnp.zeros((16, 128), f32)
    for p in range(32):
        slot = meta[48 + p] if p < 8 else (meta[56 + p] if p < 24 else kv * 8 + p - 24)
        same = jnp.broadcast_to(every_slot == slot, (16, 512))
        top = jnp.max(jnp.where(same, tops, neg_fill), axis=1, keepdims=True)
        total = jnp.sum(jnp.where(same, jnp.exp(tops - top) * sums, 0.0), axis=1, keepdims=True)
        if p < 24:
            probs[p] = jnp.exp(scores[p] - top) * (1.0 / total)
        else:
            own_w = jnp.where(lanes == p, jnp.exp(own_tops - top) * (1.0 / total), own_w)
    own_weight = jnp.concatenate([own_w, jnp.zeros((112, 128), f32)], axis=0).T[24:32]
    for h in range(16):
        g = (h // 4) * 128
        accs[h, 24:32, :] = own_weight[:, h : h + 1] * own_value[:, g : g + 128]
    rho = lax.broadcasted_iota(i32, (128, 512), 0)
    member = (lax.rem(rho, 64) // 4) * 8 + (rho // 64) * 4 + lax.rem(rho, 4) == every_slot
    member = jnp.where(member, 1.0, 0.0).astype(bf16)
    z_start(6)
    finish(5)
    for p in range(8):
        place(p, weighted(p, kept[p, 1], 0, 128))

    def gather_values(c):
        row = (c % (nc // 2)) * CROWS
        for p in range(16):
            part = weighted(8 + p, fsv[p, row : row + CROWS, :], row, row + CROWS)
            if row == 0:
                pvacc[p] = part
            else:
                pvacc[p] = pvacc[p] + part

    gather_values(4)
    gather_values(5)
    z_start(7)
    finish(6)
    gather_values(6)
    finish(7)
    for p in range(16):
        row = 3 * CROWS
        place(8 + p, pvacc[p] + weighted(8 + p, fsv[p, row : row + CROWS, :], row, row + CROWS))

    tiles = [accs[h] for h in range(16)]
    group = lane32 // 8
    for bit in (1, 2, 4, 8):
        upper = (group & bit) != 0
        for h in range(16):
            if h & bit == 0:
                a, b = tiles[h], tiles[h + bit]
                tiles[h] = jnp.where(upper, pltpu.roll(b, 8 * bit, 1), a)
                tiles[h + bit] = jnp.where(upper, b, pltpu.roll(a, 128 - 8 * bit, 1))
    for j in range(16):
        msend[j] = tiles[j].astype(bf16)
    m_copies = {}
    for k in ORDER[::-1]:
        m_copies[k] = remote(msend.at[peer_of(x, y, k)], mrecv.at[kv], m_ss.at[k], m_rs.at[k], dev(k))
    mrecv[kv] = msend[kv]
    for k in ORDER:
        m_copies[k].wait_recv()
    attn = jnp.dot(
        member, mrecv[...].reshape(512, 128), preferred_element_type=f32
    ).astype(bf16)

    rho = lax.broadcasted_iota(jnp.int32, (128, 128), 0)
    col = lax.broadcasted_iota(jnp.int32, (128, 128), 1)
    slot = (lax.rem(rho, 64) // 4) * 8 + (rho // 64) * 4 + lax.rem(rho, 4)
    perm = jnp.where(col == slot, 1.0, 0.0).astype(bf16)
    hid = jnp.dot(
        perm, hid_ref[:, pl.ds(pl.multiple_of(tp * 128, 128), 128)], preferred_element_type=f32
    )

    loads[0].wait()

    order = ORDER[::-1] + [0]
    pair_copies = []
    for g in range(4):
        for i in range(4):
            k = order[4 * g + i]
            dest = peer_of(x, y, k)
            part = jnp.dot(
                attn, wout[:, pl.ds(pl.multiple_of(dest * 256, 256), 256)], preferred_element_type=f32
            )
            low, high = part[:, :128], part[:, 128:]
            own_part[g, i] = jnp.where(tp == 0, low, high)
            pair_send[g, i] = jnp.where(tp == 0, high, low).astype(bf16)
        copy = pltpu.make_async_remote_copy(
            src_ref=pair_send.at[g], dst_ref=pair_recv.at[g], send_sem=pair_ss.at[g],
            recv_sem=pair_rs.at[g], device_id=partner, device_id_type=MESH,
        )
        copy.start()
        pair_copies.append(copy)
    rs_copies = {}
    block = None
    for g in range(4):
        pair_copies[g].wait_recv()
        for i in range(4):
            k = order[4 * g + i]
            total = own_part[g, i] + pair_recv[g, i].astype(f32)
            if k == 0:
                block = total + hid
            else:
                rs_send[k] = total.astype(bf16)
                copy = pltpu.make_async_remote_copy(
                    src_ref=rs_send.at[k], dst_ref=rs_recv.at[k], send_sem=rs_ss.at[k],
                    recv_sem=rs_rs.at[k], device_id=dev(k), device_id_type=MESH,
                )
                copy.start()
                rs_copies[k] = copy
    for k in ORDER:
        rs_copies[k].wait_recv()
        block = block + rs_recv[k].astype(f32)
    ag[0, tp] = block.astype(bf16)

    ag_copies = {}
    fw_copies = {}

    def forward(k):
        copy = pltpu.make_async_remote_copy(
            src_ref=ag.at[k, tp], dst_ref=ag.at[k, tp], send_sem=fw_ss.at[k],
            recv_sem=fw_rs.at[k], device_id=partner, device_id_type=MESH,
        )
        copy.start()
        fw_copies[k] = copy

    for k in ORDER[::-1]:
        copy = pltpu.make_async_remote_copy(
            src_ref=ag.at[0, tp], dst_ref=ag.at[k, tp], send_sem=ag_ss.at[k],
            recv_sem=ag_rs.at[k], device_id=dev(k), device_id_type=MESH,
        )
        copy.start()
        ag_copies[k] = copy
    forward(0)
    for g in range(4):
        pair_copies[g].wait_send()
    loads[1].wait()
    loads[2].wait()
    seq = [0] + ORDER
    nt = (((1,), (1,)), ((), ()))
    gate = jnp.zeros((128, 448), f32)
    upward = jnp.zeros((128, 448), f32)
    squares = jnp.zeros((128, 128), f32)
    mine = lax.broadcasted_iota(jnp.int32, (8, 128), 0) + tp * 64 + kv * 4
    pick = jnp.where(lax.broadcasted_iota(jnp.int32, (8, 128), 1) == mine, 1.0, 0.0).astype(bf16)
    for n, k in enumerate(seq):
        if n + 1 < 16:
            ag_copies[seq[n + 1]].wait_recv()
            forward(seq[n + 1])
        fw_copies[k].wait_recv()
        src = source_of(x, y, k)
        both = jnp.concatenate([ag[k, 0], ag[k, 1]], axis=1)
        wide = both.astype(f32)
        squares = squares + wide[:, :128] * wide[:, :128] + wide[:, 128:] * wide[:, 128:]
        rows = pl.ds(pl.multiple_of(src * 256, 256), 256)
        normed = (wide * gain_ref[:, rows]).astype(bf16)
        gate = gate + lax.dot_general(normed, wg[:, rows], nt, preferred_element_type=f32)
        upward = upward + lax.dot_general(normed, wu[:, rows], nt, preferred_element_type=f32)
    scale = lax.rsqrt(jnp.sum(squares, axis=1, keepdims=True) / D + norm_eps)
    gate = gate * scale
    upward = upward * scale
    hunits[...] = (gate / (1.0 + jnp.exp(-gate)) * upward).astype(bf16)

    loads[3].wait()
    dp_copies = []
    for c in range(4):
        cols = pl.ds(c * 1024, 1024)
        part = jnp.dot(hunits[...], wd[:, cols], preferred_element_type=f32)
        first, second = part[:64], part[64:]
        dsum[:, cols] = jnp.where(tp == 0, first, second)
        dp_send[c] = jnp.where(tp == 0, second, first).astype(bf16)
        copy = pltpu.make_async_remote_copy(
            src_ref=dp_send.at[c], dst_ref=dp_recv.at[c], send_sem=dp_ss.at[c],
            recv_sem=dp_rs.at[c], device_id=partner, device_id_type=MESH,
        )
        copy.start()
        dp_copies.append(copy)
    for c in range(4):
        dp_copies[c].wait_recv()
        cols = pl.ds(c * 1024, 1024)
        dsum[:, cols] = dsum[:, cols] + dp_recv[c].astype(f32)
    for j in range(16):
        d_send[j] = dsum[4 * j : 4 * j + 4, :].astype(bf16)
    d_copies = {}
    for k in ORDER[::-1]:
        copy = pltpu.make_async_remote_copy(
            src_ref=d_send.at[peer_of(x, y, k)], dst_ref=d_recv.at[k], send_sem=d_ss.at[k],
            recv_sem=d_rs.at[k], device_id=dev(k), device_id_type=MESH,
        )
        copy.start()
        d_copies[k] = copy
    for k in range(16):
        for t in range(2):
            cols = pl.ds(pl.multiple_of((source_of(x, y, k) * 2 + t) * 128, 128), 128)
            resrow[:, cols] = jnp.dot(pick, ag[k, t], preferred_element_type=f32)
    pick64 = lax.broadcasted_iota(jnp.int32, (8, 64), 0) + kv * 4
    total = resrow[...][:4]
    lane = lax.broadcasted_iota(jnp.int32, (4, 4096), 0)
    own = jnp.zeros((4, 4096), f32)
    for j in range(16):
        own = jnp.where(kv == j, dsum[4 * j : 4 * j + 4, :], own)
    total = total + own
    for k in ORDER:
        d_copies[k].wait_recv()
        total = total + d_recv[k].astype(f32)
    out_ref[...] = total.astype(bf16)

    for k in range(1, 16):
        rs_copies[k].wait_send()
        ag_copies[k].wait_send()
        d_copies[k].wait_send()
    for k in range(16):
        fw_copies[k].wait_send()
    for c in range(4):
        dp_copies[c].wait_send()
    for copies in (q_copies, a_copies, x_copies, z_copies, s_copies, m_copies):
        for copy in copies.values():
            copy.wait_send()
    for copy in out_copies:
        copy.wait()


def step(meta, hidden, again, gain, token_kv, w_query, pool, resident, w_out, w_gate, w_up, w_down):
    bf16, f32 = jnp.bfloat16, jnp.float32
    vmem = pl.BlockSpec(memory_space=pltpu.VMEM)
    hbm = pl.BlockSpec(memory_space=pl.ANY)
    dma = pltpu.SemaphoreType.DMA
    nc = CHUNKS

    def chunk(*lead):
        return [pltpu.VMEM((*lead, CROWS, 512), bf16)] * nc

    return pl.pallas_call(
        step_kernel,
        name="step",
        out_shape=(
            jax.ShapeDtypeStruct((4, 4096), bf16),
            jax.ShapeDtypeStruct((16, 2, 128, 512), bf16),
        ),
        in_specs=[pl.BlockSpec(memory_space=pltpu.SMEM), vmem, vmem, vmem] + [hbm] * 8,
        out_specs=(vmem, hbm),
        scratch_shapes=[
            pltpu.VMEM((256, 2048), bf16),
            pltpu.VMEM((8, 2, 512), bf16),
            pltpu.VMEM((8, 2, 128, 512), bf16),
            pltpu.VMEM((16, 8, 2176), f32),
            pltpu.VMEM((16, 8, 2176), f32),
            pltpu.VMEM((128, 16, 128), f32),
            pltpu.VMEM((8, 2048), f32),
            pltpu.VMEM((16, 128, 512), bf16),
            pltpu.VMEM((16, 128, 512), bf16),
            pltpu.VMEM((24, 16, 128), f32),
            pltpu.VMEM((24, 16, 128), f32),
            pltpu.VMEM((16, 16, 512), f32),
            pltpu.VMEM((16, 32, 128), f32),
            pltpu.VMEM((16, 40, 128), f32),
            pltpu.VMEM((16, 32, 128), bf16),
            pltpu.VMEM((16, 32, 128), bf16),
            pltpu.VMEM((128, 4096), bf16),
            pltpu.VMEM((448, 4096), bf16),
            pltpu.VMEM((448, 4096), bf16),
            pltpu.VMEM((448, 4096), bf16),
            pltpu.VMEM((4, 4, 128, 128), bf16),
            pltpu.VMEM((4, 4, 128, 128), bf16),
            pltpu.VMEM((4, 4, 128, 128), f32),
            pltpu.VMEM((16, 128, 128), bf16),
            pltpu.VMEM((16, 128, 128), bf16),
            pltpu.VMEM((16, 2, 128, 128), bf16),
            pltpu.VMEM((128, 448), bf16),
            pltpu.VMEM((4, 64, 1024), bf16),
            pltpu.VMEM((4, 64, 1024), bf16),
            pltpu.VMEM((64, 4096), f32),
            pltpu.VMEM((16, 4, 4096), bf16),
            pltpu.VMEM((16, 4, 4096), bf16),
            pltpu.VMEM((8, 4096), f32),
            *chunk(16), *chunk(15), *chunk(16), *chunk(3, 4), *chunk(4, 4),
            dma((2,)), dma((nc,)), dma((1,)), dma((nc,)),
            dma((16,)), dma((16,)), dma((16,)), dma((16,)),
            dma((nc, 16)), dma((nc, 16)), dma((nc, 4)), dma((nc, 4)),
            dma((16,)), dma((16,)), dma((16,)), dma((16,)),
            dma((4,)), dma((4,)), dma((4,)), dma((16,)), dma((16,)), dma((16,)), dma((16,)),
            dma((16,)), dma((16,)), dma((4,)), dma((4,)), dma((16,)), dma((16,)),
        ],
        compiler_params=pltpu.CompilerParams(
            collective_id=0, has_side_effects=True, vmem_limit_bytes=62 * 1024 * 1024
        ),
    )(meta, hidden, again, gain, token_kv, w_query, pool, resident, w_out, w_gate, w_up, w_down)


def routing(new_owner, new_local, resident_slot, resident_len, new_slot, new_len):
    i32 = jnp.int32
    grp, kv = lax.axis_index("grp"), lax.axis_index("kv")
    mine = jnp.where(new_owner == grp * 16 + kv, new_local, 0)
    pick = jnp.sum(jnp.sum(mine, axis=0).reshape(16, 16), axis=1)
    column = lax.dynamic_slice(new_owner, (0, kv * 16), (4, 16))
    from_grp = column // 16
    earlier = jnp.arange(16)[None, :] < jnp.arange(16)[:, None]
    same = (from_grp[:, :, None] == from_grp[:, None, :]) & earlier[None]
    rank = jnp.sum(same.astype(i32), axis=2)
    hit = (from_grp == grp)[:, None, :] & (rank[:, None, :] == jnp.arange(4)[None, :, None])
    onward = jnp.sum(jnp.where(hit, (column % 16)[:, None, :], 0), axis=2).reshape(16)
    final = lax.dynamic_index_in_dim(from_grp * 4 + rank, grp, 0, keepdims=False)
    return jnp.concatenate(
        [pick, onward, final, resident_slot[0], resident_len[0], new_slot[0], new_len[0]]
    ).astype(i32)


def per_device(
    hidden_states,
    attn_gain,
    mlp_gain,
    w_query,
    w_out,
    w_gate,
    w_up,
    w_down,
    kv_pool,
    resident_cache,
    resident_slot,
    resident_len,
    new_owner,
    new_local,
    new_slot,
    new_len,
    token_kv,
):
    meta = routing(new_owner, new_local, resident_slot, resident_len, new_slot, new_len)
    mixed, new_pages = step(
        meta,
        hidden_states,
        attn_gain.reshape(1, 256),
        mlp_gain.reshape(1, 4096),
        token_kv,
        w_query,
        kv_pool.reshape(16, 256, 512),
        resident_cache[0],
        w_out.reshape(128, 4096),
        w_gate.T,
        w_up.T,
        w_down,
    )
    return (mixed, new_pages[None])


def solution(mesh):
    return jax.shard_map(
        per_device,
        mesh=mesh,
        in_specs=(
            P("grp", "kv"),
            P("kv"),
            P(),
            P("kv", "tp"),
            P("tp", "kv", None),
            P(None, KV_TP),
            P(None, KV_TP),
            P(KV_TP, None),
            P(GRP_KV, None, None, "tp"),
            P("grp", "kv", None, None, "tp"),
            P("grp", "kv"),
            P("grp", "kv"),
            P(),
            P(),
            P("grp", "kv"),
            P("grp", "kv"),
            P("grp", None, "tp"),
        ),
        out_specs=(P(GRP_KV_TP, None), P("grp", "kv", None, None, "tp")),
        check_vma=False,
    )
```

```python
import jax
import jax.numpy as jnp
from jax import lax
from jax.experimental import pallas as pl
from jax.experimental.pallas import tpu as pltpu
from jax.sharding import PartitionSpec as P

D = 4096
HEADS = 32
KV_HEADS = 8
HEAD_DIM = 128
KV_TP = ("kv", "tp")
GRP_KV = ("grp", "kv")
GRP_KV_TP = ("grp", "kv", "tp")


neg_fill = -1e30
norm_eps = 1e-05
MESH = pl.DeviceIdType.MESH


def peer_of(x, y, k):
    return lax.rem(x + k // 4, 4) * 4 + lax.rem(y + k % 4, 4)


def source_of(x, y, k):
    return lax.rem(x + 4 - k // 4, 4) * 4 + lax.rem(y + 4 - k % 4, 4)


ORDER = sorted(range(1, 16), key=lambda k: (min(k // 4, 4 - k // 4) + min(k % 4, 4 - k % 4), k))


CHUNKS = 8
CROWS = 256 // CHUNKS


def step_kernel(
    meta, hid_ref, again_ref, gain_ref, tok_hbm, wq_hbm, pool_hbm, res_hbm, wout_hbm, wg_hbm, wu_hbm, wd_hbm,
    out_ref, cache_hbm,
    wq, tok, kept, qs_send, qs_recv, qfull, qflat, fsk, fsv, scores, probs, pvacc, accs, stats, msend, mrecv,
    wout, wg, wu, wd, pair_send, pair_recv, own_part, rs_send, rs_recv, ag, hunits,
    dp_send, dp_recv, dsum, d_send, d_recv, resrow, *rest,
):
    f32, bf16, i32 = jnp.float32, jnp.bfloat16, jnp.int32
    nc = CHUNKS
    pool, xs, xr, zs, zr = (rest[i * nc : (i + 1) * nc] for i in range(5))
    (ld_sem, pool_sem, kept_sem, out_sem, q_ss, q_rs, a_ss, a_rs, x_ss, x_rs, z_ss, z_rs, s_ss, s_rs,
     m_ss, m_rs, w_sem, pair_ss, pair_rs, rs_ss, rs_rs, ag_ss, ag_rs, fw_ss, fw_rs, dp_ss, dp_rs, d_ss,
     d_rs) = rest[5 * nc :]
    grp, kv, tp = lax.axis_index("grp"), lax.axis_index("kv"), lax.axis_index("tp")
    x, y = kv // 4, lax.rem(kv, 4)
    other = 1 - tp
    partner = (grp, kv, other)

    def dev(k):
        return (grp, peer_of(x, y, k), tp)

    def zdev(dz):
        return (lax.rem(grp + dz, 4), kv, tp)

    def remote(src, dst, send, recv, device):
        copy = pltpu.make_async_remote_copy(
            src_ref=src, dst_ref=dst, send_sem=send, recv_sem=recv, device_id=device,
            device_id_type=MESH,
        )
        copy.start()
        return copy

    def settle(ref, sem):
        pltpu.make_async_copy(ref, ref, sem).wait()

    wq_load = pltpu.make_async_copy(wq_hbm, wq, ld_sem.at[0])
    wq_load.start()
    pool_loads = []
    for c in range(nc):
        load = pltpu.make_async_copy(pool_hbm.at[:, pl.ds(c * CROWS, CROWS), :], pool[c], pool_sem.at[c])
        load.start()
        pool_loads.append(load)
    kept_load = pltpu.make_async_copy(res_hbm, kept, kept_sem.at[0])
    kept_load.start()
    tok_load = pltpu.make_async_copy(
        tok_hbm.at[pl.ds(pl.multiple_of(kv * 8, 8), 8)], tok, ld_sem.at[1]
    )
    tok_load.start()

    loads = [
        pltpu.make_async_copy(src, dst, w_sem.at[i])
        for i, (src, dst) in enumerate([(wout_hbm, wout), (wg_hbm, wg), (wu_hbm, wu), (wd_hbm, wd)])
    ]
    for load in loads:
        load.start()

    barrier = pltpu.get_barrier_semaphore()
    pl.semaphore_signal(barrier, inc=1, device_id=partner, device_id_type=MESH)
    for k in range(1, 16):
        pl.semaphore_signal(barrier, inc=1, device_id=dev(k), device_id_type=MESH)
    for dz in range(1, 4):
        pl.semaphore_signal(barrier, inc=1, device_id=zdev(dz), device_id_type=MESH)

    feats = hid_ref[...].astype(f32)
    normed = (feats * again_ref[...]).astype(bf16)
    squares = jnp.sum(feats * feats, axis=1, keepdims=True)
    wq_load.wait()
    for h in range(4):
        part = jnp.dot(normed, wq[:, h * 512 : h * 512 + 512], preferred_element_type=f32)
        qs_send[:, :, h * 512 : h * 512 + 512] = part.reshape(16, 8, 512)
    qs_send[:, :, 2048:2176] = jnp.broadcast_to(squares, (128, 128)).reshape(16, 8, 128)
    pl.semaphore_wait(barrier, 19)

    for k in ORDER[::-1]:
        remote(qs_send.at[peer_of(x, y, k)], qs_recv.at[k], q_ss.at[0], q_rs.at[0], dev(k))

    def xy_start(c):
        pool_loads[c].wait()
        xr[c][kv] = pool[c][meta[kv]]
        for k in range(1, 16):
            xs[c][k - 1] = pool[c][meta[peer_of(x, y, k)]]
        for k in ORDER[::-1]:
            remote(xs[c].at[k - 1], xr[c].at[kv], x_ss.at[c], x_rs.at[c], dev(k))

    def z_start(c):
        settle(xs[c], x_rs.at[c])
        for dz in range(4):
            g = lax.rem(grp + dz, 4)
            for r in range(4):
                page = xr[c][meta[16 + g * 4 + r]]
                if dz == 0:
                    zr[c][grp, r] = page
                else:
                    zs[c][dz - 1, r] = page
        for dz in (2, 1, 3):
            remote(zs[c].at[dz - 1], zr[c].at[grp], z_ss.at[c], z_rs.at[c], zdev(dz))

    def finish(c):
        settle(zs[c], z_rs.at[c])
        final, half = (fsk, 0) if c < nc // 2 else (fsv, 1)
        row = (c % (nc // 2)) * CROWS
        for i in range(16):
            where = meta[32 + i]
            final[i, row : row + CROWS, :] = zr[c][where // 4, lax.rem(where, 4)]
        pltpu.make_async_copy(
            final.at[:, pl.ds(row, CROWS), :], cache_hbm.at[:, half, pl.ds(row, CROWS), :], out_sem.at[half]
        ).start()

    head_of = lax.broadcasted_iota(i32, (16, 512), 0) // 4
    block_of = lax.broadcasted_iota(i32, (16, 512), 1) // 128
    diag = head_of == block_of
    lanes = lax.broadcasted_iota(i32, (16, 128), 1)

    def page_scores(p, keys, slot, filled):
        q = qfull[slot]
        wide = jnp.where(diag, jnp.concatenate([q, q, q, q], axis=1), 0.0)
        high = wide.astype(bf16)
        left = wide - high.astype(f32)
        mid = left.astype(bf16)
        low = (left - mid.astype(f32)).astype(bf16)
        rows = jnp.concatenate([high, mid, low], axis=0)
        s = lax.dot_general(rows, keys, (((1,), (1,)), ((), ())), preferred_element_type=f32)
        s = s[:16] + s[16:32] + s[32:]
        s = jnp.where(lanes < filled, s, neg_fill)
        scores[p] = s
        top = jnp.max(s, axis=1, keepdims=True)
        total = jnp.sum(jnp.where(lanes < filled, jnp.exp(s - top), 0.0), axis=1, keepdims=True)
        return top, total

    def weighted(p, values, lo, hi):
        w = probs[p][:, lo:hi]
        high = w.astype(bf16)
        low = (w - high.astype(f32)).astype(bf16)
        out = jnp.dot(jnp.concatenate([high, low], axis=0), values, preferred_element_type=f32)
        return out[:16] + out[16:]

    def place(p, acc):
        for h in range(16):
            accs[h, p : p + 1, :] = acc[h : h + 1, (h // 4) * 128 : (h // 4) * 128 + 128]

    lane32 = lax.broadcasted_iota(i32, (32, 128), 1)

    def note(table, p, top, total):
        return jnp.where(lane32 == p, jnp.concatenate([top, total], axis=0), table)

    def query_done():
        total = qs_send[kv]
        settle(qs_recv.at[pl.ds(1, 15)], q_rs.at[0])
        for k in range(1, 16):
            total = total + qs_recv[k]
        scale = lax.rsqrt(total[:, 2048:2049] / D + norm_eps)
        q8 = total[:, :2048] * scale * HEAD_DIM ** (-0.5)
        qflat[...] = q8
        for h in range(16):
            qfull[pl.ds(pl.multiple_of(kv * 8, 8), 8), h, :] = q8[:, h * 128 : h * 128 + 128]
        mine = qfull.at[pl.ds(pl.multiple_of(kv * 8, 8), 8)]
        for k in ORDER[::-1]:
            remote(mine, mine, a_ss.at[0], a_rs.at[0], dev(k))

    for c in range(3):
        xy_start(c)
    query_done()
    xy_start(3)
    z_start(0)
    xy_start(4)
    z_start(1)
    finish(0)
    xy_start(5)
    z_start(2)
    finish(1)
    xy_start(6)
    z_start(3)
    finish(2)
    xy_start(7)
    tok_load.wait()
    own_key, own_value = tok[:, 0, :].astype(f32), tok[:, 1, :].astype(f32)
    lane8 = lax.broadcasted_iota(i32, (8, 128), 1)
    own_rows = jnp.zeros((8, 128), f32)
    for h in range(16):
        s = jnp.sum(
            qflat[:, h * 128 : h * 128 + 128] * own_key[:, (h // 4) * 128 : (h // 4) * 128 + 128],
            axis=1, keepdims=True,
        )
        own_rows = jnp.where(lane8 == h, s, own_rows)
    own_tops = jnp.concatenate([jnp.zeros((24, 128), f32), own_rows, jnp.zeros((96, 128), f32)], axis=0).T[:16]
    slot_row = jnp.zeros((8, 128), i32)
    for p in range(24):
        slot_row = jnp.where(lane8 == p, meta[48 + p] if p < 8 else meta[56 + p], slot_row)
    slot_row = jnp.where(lane8 >= 24, kv * 8 + lane8 - 24, slot_row)
    settle(qfull.at[pl.ds(0, 120)], a_rs.at[0])
    kept_load.wait()
    table = jnp.zeros((32, 128), f32)
    for p in range(8):
        table = note(table, p, *page_scores(p, kept[p, 0], meta[48 + p], meta[56 + p]))
    z_start(4)
    finish(3)
    for p in range(16):
        table = note(table, 8 + p, *page_scores(8 + p, fsk[p], meta[64 + p], meta[80 + p]))
    own_lane = lanes >= 24
    mine = jnp.concatenate(
        [
            jnp.where(own_lane, own_tops, table[:16]),
            jnp.where(own_lane, 1.0, table[16:]),
            slot_row.astype(f32),
        ],
        axis=0,
    )
    mine = jnp.where(lax.broadcasted_iota(i32, (40, 128), 1) < 32, mine, 0.0)
    turned = [mine] + [pltpu.roll(mine, 32 * q, 1) for q in range(1, 4)]
    for q in range(1, 4):
        mine = jnp.where(y == q, turned[q], mine)
    stats[kv] = mine
    for k in ORDER[::-1]:
        remote(stats.at[kv], stats.at[kv], s_ss.at[0], s_rs.at[0], dev(k))
    z_start(5)
    finish(4)
    z_start(6)
    finish(5)
    z_start(7)
    settle(stats.at[pl.ds(0, 15)], s_rs.at[0])
    every = jnp.concatenate(
        [stats[4 * i] + stats[4 * i + 1] + stats[4 * i + 2] + stats[4 * i + 3] for i in range(4)], axis=1
    )
    tops, sums, every_slot = every[:16], every[16:32], every[32:33].astype(i32)
    own_w = jnp.zeros((16, 128), f32)
    for p in range(32):
        slot = meta[48 + p] if p < 8 else (meta[56 + p] if p < 24 else kv * 8 + p - 24)
        same = jnp.broadcast_to(every_slot == slot, (16, 512))
        top = jnp.max(jnp.where(same, tops, neg_fill), axis=1, keepdims=True)
        total = jnp.sum(jnp.where(same, jnp.exp(tops - top) * sums, 0.0), axis=1, keepdims=True)
        if p < 24:
            probs[p] = jnp.exp(scores[p] - top) * (1.0 / total)
        else:
            own_w = jnp.where(lanes == p, jnp.exp(own_tops - top) * (1.0 / total), own_w)
    own_weight = jnp.concatenate([own_w, jnp.zeros((112, 128), f32)], axis=0).T[24:32]
    for h in range(16):
        g = (h // 4) * 128
        accs[h, 24:32, :] = own_weight[:, h : h + 1] * own_value[:, g : g + 128]
    rho = lax.broadcasted_iota(i32, (128, 512), 0)
    member = (lax.rem(rho, 64) // 4) * 8 + (rho // 64) * 4 + lax.rem(rho, 4) == every_slot
    member = jnp.where(member, 1.0, 0.0).astype(bf16)
    for p in range(8):
        place(p, weighted(p, kept[p, 1], 0, 128))

    def gather_values(c):
        row = (c % (nc // 2)) * CROWS
        for p in range(16):
            part = weighted(8 + p, fsv[p, row : row + CROWS, :], row, row + CROWS)
            if row == 0:
                pvacc[p] = part
            else:
                pvacc[p] = pvacc[p] + part

    gather_values(4)
    gather_values(5)
    finish(6)
    gather_values(6)
    finish(7)
    for p in range(16):
        row = 3 * CROWS
        place(8 + p, pvacc[p] + weighted(8 + p, fsv[p, row : row + CROWS, :], row, row + CROWS))

    tiles = [accs[h] for h in range(16)]
    group = lane32 // 8
    for bit in (1, 2, 4, 8):
        upper = (group & bit) != 0
        for h in range(16):
            if h & bit == 0:
                a, b = tiles[h], tiles[h + bit]
                tiles[h] = jnp.where(upper, pltpu.roll(b, 8 * bit, 1), a)
                tiles[h + bit] = jnp.where(upper, b, pltpu.roll(a, 128 - 8 * bit, 1))
    for j in range(16):
        msend[j] = tiles[j].astype(bf16)
    for k in ORDER[::-1]:
        remote(msend.at[peer_of(x, y, k)], mrecv.at[kv], m_ss.at[0], m_rs.at[0], dev(k))
    mrecv[kv] = msend[kv]
    settle(msend.at[pl.ds(0, 15)], m_rs.at[0])
    attn = jnp.dot(
        member, mrecv[...].reshape(512, 128), preferred_element_type=f32
    ).astype(bf16)

    rho = lax.broadcasted_iota(jnp.int32, (128, 128), 0)
    col = lax.broadcasted_iota(jnp.int32, (128, 128), 1)
    slot = (lax.rem(rho, 64) // 4) * 8 + (rho // 64) * 4 + lax.rem(rho, 4)
    perm = jnp.where(col == slot, 1.0, 0.0).astype(bf16)
    hid = jnp.dot(
        perm, hid_ref[:, pl.ds(pl.multiple_of(tp * 128, 128), 128)], preferred_element_type=f32
    )

    loads[0].wait()

    order = ORDER[::-1] + [0]
    for g in range(4):
        for i in range(4):
            k = order[4 * g + i]
            dest = peer_of(x, y, k)
            part = jnp.dot(
                attn, wout[:, pl.ds(pl.multiple_of(dest * 256, 256), 256)], preferred_element_type=f32
            )
            low, high = part[:, :128], part[:, 128:]
            own_part[g, i] = jnp.where(tp == 0, low, high)
            pair_send[g, i] = jnp.where(tp == 0, high, low).astype(bf16)
        remote(pair_send.at[g], pair_recv.at[g], pair_ss.at[0], pair_rs.at[g], partner)
    block = None
    for g in range(4):
        settle(pair_recv.at[g], pair_rs.at[g])
        for i in range(4):
            k = order[4 * g + i]
            total = own_part[g, i] + pair_recv[g, i].astype(f32)
            if k == 0:
                block = total + hid
            else:
                rs_send[k] = total.astype(bf16)
                remote(rs_send.at[k], rs_recv.at[k], rs_ss.at[0], rs_rs.at[0], dev(k))
    settle(rs_recv.at[pl.ds(1, 15)], rs_rs.at[0])
    for k in ORDER:
        block = block + rs_recv[k].astype(f32)
    ag[0, tp] = block.astype(bf16)

    def forward(k):
        remote(ag.at[k, tp], ag.at[k, tp], fw_ss.at[0], fw_rs.at[k], partner)

    forward(0)
    for k in ORDER:
        remote(ag.at[0, tp], ag.at[k, tp], ag_ss.at[0], ag_rs.at[k], dev(k))
    loads[1].wait()
    loads[2].wait()
    seq = [0] + ORDER
    nt = (((1,), (1,)), ((), ()))
    gate = jnp.zeros((128, 448), f32)
    upward = jnp.zeros((128, 448), f32)
    squares = jnp.zeros((128, 128), f32)
    mine = lax.broadcasted_iota(jnp.int32, (8, 128), 0) + tp * 64 + kv * 4
    pick = jnp.where(lax.broadcasted_iota(jnp.int32, (8, 128), 1) == mine, 1.0, 0.0).astype(bf16)
    for n, k in enumerate(seq):
        for later in seq[n + 1 : n + 7] if n == 0 else seq[n + 6 : n + 7]:
            settle(ag.at[later, tp], ag_rs.at[later])
            forward(later)
        settle(ag.at[k, other], fw_rs.at[k])
        src = source_of(x, y, k)
        both = jnp.concatenate([ag[k, 0], ag[k, 1]], axis=1)
        wide = both.astype(f32)
        squares = squares + wide[:, :128] * wide[:, :128] + wide[:, 128:] * wide[:, 128:]
        rows = pl.ds(pl.multiple_of(src * 256, 256), 256)
        normed = (wide * gain_ref[:, rows]).astype(bf16)
        gate = gate + lax.dot_general(normed, wg[:, rows], nt, preferred_element_type=f32)
        upward = upward + lax.dot_general(normed, wu[:, rows], nt, preferred_element_type=f32)
    scale = lax.rsqrt(jnp.sum(squares, axis=1, keepdims=True) / D + norm_eps)
    gate = gate * scale
    upward = upward * scale
    hunits[...] = (gate / (1.0 + jnp.exp(-gate)) * upward).astype(bf16)

    loads[3].wait()
    for c in range(4):
        cols = pl.ds(c * 1024, 1024)
        part = jnp.dot(hunits[...], wd[:, cols], preferred_element_type=f32)
        first, second = part[:64], part[64:]
        dsum[:, cols] = jnp.where(tp == 0, first, second)
        dp_send[c] = jnp.where(tp == 0, second, first).astype(bf16)
        remote(dp_send.at[c], dp_recv.at[c], dp_ss.at[0], dp_rs.at[c], partner)
    for c in range(4):
        settle(dp_recv.at[c], dp_rs.at[c])
        cols = pl.ds(c * 1024, 1024)
        dsum[:, cols] = dsum[:, cols] + dp_recv[c].astype(f32)
    for j in range(16):
        d_send[j] = dsum[4 * j : 4 * j + 4, :].astype(bf16)
    for k in ORDER[::-1]:
        remote(d_send.at[peer_of(x, y, k)], d_recv.at[k], d_ss.at[0], d_rs.at[0], dev(k))
    for c in range(nc):
        settle(xs[c], x_ss.at[c])
        settle(zs[c], z_ss.at[c])
    settle(qs_send.at[pl.ds(0, 15)], q_ss.at[0])
    settle(qfull.at[pl.ds(0, 120)], a_ss.at[0])
    settle(stats.at[pl.ds(0, 15)], s_ss.at[0])
    settle(msend.at[pl.ds(0, 15)], m_ss.at[0])
    settle(pair_send, pair_ss.at[0])
    settle(rs_send.at[pl.ds(1, 15)], rs_ss.at[0])
    settle(rs_send.at[pl.ds(1, 15)], ag_ss.at[0])
    settle(rs_send, fw_ss.at[0])
    settle(dp_send, dp_ss.at[0])
    settle(fsk, out_sem.at[0])
    settle(fsv, out_sem.at[1])
    for k in range(16):
        for t in range(2):
            cols = pl.ds(pl.multiple_of((source_of(x, y, k) * 2 + t) * 128, 128), 128)
            resrow[:, cols] = jnp.dot(pick, ag[k, t], preferred_element_type=f32)
    total = resrow[...][:4]
    own = jnp.zeros((4, 4096), f32)
    for j in range(16):
        own = jnp.where(kv == j, dsum[4 * j : 4 * j + 4, :], own)
    total = total + own
    settle(d_recv.at[pl.ds(1, 15)], d_rs.at[0])
    for k in ORDER:
        total = total + d_recv[k].astype(f32)
    out_ref[...] = total.astype(bf16)
    settle(d_send.at[pl.ds(0, 15)], d_ss.at[0])


def step(meta, hidden, again, gain, token_kv, w_query, pool, resident, w_out, w_gate, w_up, w_down):
    bf16, f32 = jnp.bfloat16, jnp.float32
    vmem = pl.BlockSpec(memory_space=pltpu.VMEM)
    hbm = pl.BlockSpec(memory_space=pl.ANY)
    dma = pltpu.SemaphoreType.DMA
    nc = CHUNKS

    def chunk(*lead):
        return [pltpu.VMEM((*lead, CROWS, 512), bf16)] * nc

    return pl.pallas_call(
        step_kernel,
        name="step",
        out_shape=(
            jax.ShapeDtypeStruct((4, 4096), bf16),
            jax.ShapeDtypeStruct((16, 2, 128, 512), bf16),
        ),
        in_specs=[pl.BlockSpec(memory_space=pltpu.SMEM), vmem, vmem, vmem] + [hbm] * 8,
        out_specs=(vmem, hbm),
        scratch_shapes=[
            pltpu.VMEM((256, 2048), bf16),
            pltpu.VMEM((8, 2, 512), bf16),
            pltpu.VMEM((8, 2, 128, 512), bf16),
            pltpu.VMEM((16, 8, 2176), f32),
            pltpu.VMEM((16, 8, 2176), f32),
            pltpu.VMEM((128, 16, 128), f32),
            pltpu.VMEM((8, 2048), f32),
            pltpu.VMEM((16, 128, 512), bf16),
            pltpu.VMEM((16, 128, 512), bf16),
            pltpu.VMEM((24, 16, 128), f32),
            pltpu.VMEM((24, 16, 128), f32),
            pltpu.VMEM((16, 16, 512), f32),
            pltpu.VMEM((16, 32, 128), f32),
            pltpu.VMEM((16, 40, 128), f32),
            pltpu.VMEM((16, 32, 128), bf16),
            pltpu.VMEM((16, 32, 128), bf16),
            pltpu.VMEM((128, 4096), bf16),
            pltpu.VMEM((448, 4096), bf16),
            pltpu.VMEM((448, 4096), bf16),
            pltpu.VMEM((448, 4096), bf16),
            pltpu.VMEM((4, 4, 128, 128), bf16),
            pltpu.VMEM((4, 4, 128, 128), bf16),
            pltpu.VMEM((4, 4, 128, 128), f32),
            pltpu.VMEM((16, 128, 128), bf16),
            pltpu.VMEM((16, 128, 128), bf16),
            pltpu.VMEM((16, 2, 128, 128), bf16),
            pltpu.VMEM((128, 448), bf16),
            pltpu.VMEM((4, 64, 1024), bf16),
            pltpu.VMEM((4, 64, 1024), bf16),
            pltpu.VMEM((64, 4096), f32),
            pltpu.VMEM((16, 4, 4096), bf16),
            pltpu.VMEM((16, 4, 4096), bf16),
            pltpu.VMEM((8, 4096), f32),
            *chunk(16), *chunk(15), *chunk(16), *chunk(3, 4), *chunk(4, 4),
            dma((2,)), dma((nc,)), dma((1,)), dma((2,)),
            dma((1,)), dma((1,)), dma((1,)), dma((1,)),
            dma((nc,)), dma((nc,)), dma((nc,)), dma((nc,)),
            dma((1,)), dma((1,)), dma((1,)), dma((1,)),
            dma((4,)), dma((1,)), dma((4,)), dma((1,)), dma((1,)), dma((1,)), dma((16,)),
            dma((1,)), dma((16,)), dma((1,)), dma((4,)), dma((1,)), dma((1,)),
        ],
        compiler_params=pltpu.CompilerParams(
            collective_id=0, has_side_effects=True, vmem_limit_bytes=62 * 1024 * 1024
        ),
    )(meta, hidden, again, gain, token_kv, w_query, pool, resident, w_out, w_gate, w_up, w_down)


def routing(new_owner, new_local, resident_slot, resident_len, new_slot, new_len):
    i32 = jnp.int32
    grp, kv = lax.axis_index("grp"), lax.axis_index("kv")
    mine = jnp.where(new_owner == grp * 16 + kv, new_local, 0)
    pick = jnp.sum(jnp.sum(mine, axis=0).reshape(16, 16), axis=1)
    column = lax.dynamic_slice(new_owner, (0, kv * 16), (4, 16))
    from_grp = column // 16
    earlier = jnp.arange(16)[None, :] < jnp.arange(16)[:, None]
    same = (from_grp[:, :, None] == from_grp[:, None, :]) & earlier[None]
    rank = jnp.sum(same.astype(i32), axis=2)
    hit = (from_grp == grp)[:, None, :] & (rank[:, None, :] == jnp.arange(4)[None, :, None])
    onward = jnp.sum(jnp.where(hit, (column % 16)[:, None, :], 0), axis=2).reshape(16)
    final = lax.dynamic_index_in_dim(from_grp * 4 + rank, grp, 0, keepdims=False)
    return jnp.concatenate(
        [pick, onward, final, resident_slot[0], resident_len[0], new_slot[0], new_len[0]]
    ).astype(i32)


def per_device(
    hidden_states,
    attn_gain,
    mlp_gain,
    w_query,
    w_out,
    w_gate,
    w_up,
    w_down,
    kv_pool,
    resident_cache,
    resident_slot,
    resident_len,
    new_owner,
    new_local,
    new_slot,
    new_len,
    token_kv,
):
    meta = routing(new_owner, new_local, resident_slot, resident_len, new_slot, new_len)
    mixed, new_pages = step(
        meta,
        hidden_states,
        attn_gain.reshape(1, 256),
        mlp_gain.reshape(1, 4096),
        token_kv,
        w_query,
        kv_pool.reshape(16, 256, 512),
        resident_cache[0],
        w_out.reshape(128, 4096),
        w_gate.T,
        w_up.T,
        w_down,
    )
    return (mixed, new_pages[None])


def solution(mesh):
    return jax.shard_map(
        per_device,
        mesh=mesh,
        in_specs=(
            P("grp", "kv"),
            P("kv"),
            P(),
            P("kv", "tp"),
            P("tp", "kv", None),
            P(None, KV_TP),
            P(None, KV_TP),
            P(KV_TP, None),
            P(GRP_KV, None, None, "tp"),
            P("grp", "kv", None, None, "tp"),
            P("grp", "kv"),
            P("grp", "kv"),
            P(),
            P(),
            P("grp", "kv"),
            P("grp", "kv"),
            P("grp", None, "tp"),
        ),
        out_specs=(P(GRP_KV_TP, None), P("grp", "kv", None, None, "tp")),
        check_vma=False,
    )
```

```python
import jax
import jax.numpy as jnp
from jax import lax
from jax.experimental import pallas as pl
from jax.experimental.pallas import tpu as pltpu
from jax.sharding import PartitionSpec as P

D = 4096
HEADS = 32
KV_HEADS = 8
HEAD_DIM = 128
KV_TP = ("kv", "tp")
GRP_KV = ("grp", "kv")
GRP_KV_TP = ("grp", "kv", "tp")


neg_fill = -1e30
norm_eps = 1e-05
MESH = pl.DeviceIdType.MESH


def peer_of(x, y, k):
    return lax.rem(x + k // 4, 4) * 4 + lax.rem(y + k % 4, 4)


def source_of(x, y, k):
    return lax.rem(x + 4 - k // 4, 4) * 4 + lax.rem(y + 4 - k % 4, 4)


ORDER = sorted(range(1, 16), key=lambda k: (min(k // 4, 4 - k // 4) + min(k % 4, 4 - k % 4), k))


PIECES = [(0, 0, 32), (0, 32, 32), (0, 64, 32), (0, 96, 32), (1, 0, 32), (1, 32, 32), (1, 64, 32), (1, 96, 16), (1, 112, 16)]


def step_kernel(
    meta, hid_ref, again_ref, gain_ref, tok_hbm, wq_hbm, pool_hbm, res_hbm, wout_hbm, wg_hbm, wu_hbm, wd_hbm,
    out_ref, cache_hbm,
    wq, tok, kept, qa1s, qa1r, qa2s, qa2r, qb1s, qb1r, qb2s, qb2r, qfa, qfb, qflat, fsk, fsv, scores, probs, pvacc, accs, stats, msend, mrecv,
    wout, wg, wu, wd, pair_send, pair_recv, own_part, rs_send, rs_recv, ag, hunits,
    dp_send, dp_recv, dsum, d_send, d_recv, resrow, *rest,
):
    f32, bf16, i32 = jnp.float32, jnp.bfloat16, jnp.int32
    nc = len(PIECES)
    pool, xs, xr, zs, zr = (rest[i * nc : (i + 1) * nc] for i in range(5))
    (ld_sem, pool_sem, kept_sem, out_sem, q_ss, q_rs, a_ss, a_rs, x_ss, x_rs, z_ss, z_rs, s_ss, s_rs,
     m_ss, m_rs, w_sem, pair_ss, pair_rs, rs_ss, rs_rs, ag_ss, ag_rs, fw_ss, fw_rs, dp_ss, dp_rs, d_ss,
     d_rs) = rest[5 * nc :]
    grp, kv, tp = lax.axis_index("grp"), lax.axis_index("kv"), lax.axis_index("tp")
    x, y = kv // 4, lax.rem(kv, 4)
    other = 1 - tp
    partner = (grp, kv, other)

    def dev(k):
        return (grp, peer_of(x, y, k), tp)

    def zdev(dz):
        return (lax.rem(grp + dz, 4), kv, tp)

    def remote(src, dst, send, recv, device):
        copy = pltpu.make_async_remote_copy(
            src_ref=src, dst_ref=dst, send_sem=send, recv_sem=recv, device_id=device,
            device_id_type=MESH,
        )
        copy.start()
        return copy

    def settle(ref, sem):
        pltpu.make_async_copy(ref, ref, sem).wait()

    wq_load = pltpu.make_async_copy(wq_hbm, wq, ld_sem.at[0])
    wq_load.start()
    pool_loads = []
    for c in range(nc):
        load = pltpu.make_async_copy(pool_hbm.at[:, pl.ds(PIECES[c][0] * 128 + PIECES[c][1], PIECES[c][2]), :], pool[c], pool_sem.at[c])
        load.start()
        pool_loads.append(load)
    kept_load = pltpu.make_async_copy(res_hbm, kept, kept_sem.at[0])
    kept_load.start()
    tok_load = pltpu.make_async_copy(
        tok_hbm.at[pl.ds(pl.multiple_of(kv * 8, 8), 8)], tok, ld_sem.at[1]
    )
    tok_load.start()

    loads = [
        pltpu.make_async_copy(src, dst, w_sem.at[i])
        for i, (src, dst) in enumerate([(wout_hbm, wout), (wg_hbm, wg), (wu_hbm, wu), (wd_hbm, wd)])
    ]
    for load in loads:
        load.start()

    barrier = pltpu.get_barrier_semaphore()
    pl.semaphore_signal(barrier, inc=1, device_id=partner, device_id_type=MESH)
    for k in range(1, 16):
        pl.semaphore_signal(barrier, inc=1, device_id=dev(k), device_id_type=MESH)
    for dz in range(1, 4):
        pl.semaphore_signal(barrier, inc=1, device_id=zdev(dz), device_id_type=MESH)

    feats = hid_ref[...].astype(f32)
    normed = (feats * again_ref[...]).astype(bf16)
    squares = jnp.sum(feats * feats, axis=1, keepdims=True)
    wq_load.wait()
    for h in range(2):
        part = jnp.dot(normed, wq[:, h * 512 : h * 512 + 512], preferred_element_type=f32)
        qa1s[:, :, h * 512 : h * 512 + 512] = part.reshape(4, 32, 512)
    qa1s[:, :, 1024:1152] = jnp.broadcast_to(squares, (128, 128)).reshape(4, 32, 128)
    for h in range(2):
        part = jnp.dot(normed, wq[:, 1024 + h * 512 : 1536 + h * 512], preferred_element_type=f32)
        for i in range(16):
            qb1s[i % 4, i // 4, :, h * 512 : h * 512 + 512] = part[8 * i : 8 * i + 8]
    pl.semaphore_wait(barrier, 19)

    for step in (2, 1, 3):
        remote(qa1s.at[lax.rem(x + step, 4)], qa1r.at[step], q_ss.at[0], q_rs.at[0], dev(4 * step))
        remote(qb1s.at[lax.rem(y + step, 4)], qb1r.at[step], q_ss.at[1], q_rs.at[1], dev(step))

    def xy_start(c):
        pool_loads[c].wait()
        xr[c][kv] = pool[c][meta[kv]]
        for k in range(1, 16):
            xs[c][k - 1] = pool[c][meta[peer_of(x, y, k)]]
        for k in ORDER[::-1]:
            remote(xs[c].at[k - 1], xr[c].at[kv], x_ss.at[c], x_rs.at[c], dev(k))

    def z_start(c):
        settle(xs[c], x_rs.at[c])
        for dz in range(4):
            g = lax.rem(grp + dz, 4)
            for r in range(4):
                page = xr[c][meta[16 + g * 4 + r]]
                if dz == 0:
                    zr[c][grp, r] = page
                else:
                    zs[c][dz - 1, r] = page
        for dz in (2, 1, 3):
            remote(zs[c].at[dz - 1], zr[c].at[grp], z_ss.at[c], z_rs.at[c], zdev(dz))

    def finish(c):
        settle(zs[c], z_rs.at[c])
        half, row, tokens = PIECES[c]
        final = (fsk, fsv)[half]
        for i in range(16):
            where = meta[32 + i]
            final[i, row : row + tokens, :] = zr[c][where // 4, lax.rem(where, 4)]
        pltpu.make_async_copy(
            final.at[:, pl.ds(row, tokens), :], cache_hbm.at[:, half, pl.ds(row, tokens), :], out_sem.at[half]
        ).start()

    head_of = lax.broadcasted_iota(i32, (16, 512), 0) // 4
    block_of = lax.broadcasted_iota(i32, (16, 512), 1) // 128
    diag = head_of == block_of
    lanes = lax.broadcasted_iota(i32, (16, 128), 1)

    def page_scores(p, keys, slot, filled):
        place_x, place_y, place_s = slot // 32, lax.rem(slot // 8, 4), lax.rem(slot, 8)
        q = jnp.concatenate([qfa[place_x, place_y, place_s], qfb[place_x, place_y, place_s]], axis=0)
        wide = jnp.where(diag, jnp.concatenate([q, q, q, q], axis=1), 0.0)
        high = wide.astype(bf16)
        left = wide - high.astype(f32)
        mid = left.astype(bf16)
        low = (left - mid.astype(f32)).astype(bf16)
        rows = jnp.concatenate([high, mid, low], axis=0)
        s = lax.dot_general(rows, keys, (((1,), (1,)), ((), ())), preferred_element_type=f32)
        s = s[:16] + s[16:32] + s[32:]
        s = jnp.where(lanes < filled, s, neg_fill)
        scores[p] = s
        top = jnp.max(s, axis=1, keepdims=True)
        total = jnp.sum(jnp.where(lanes < filled, jnp.exp(s - top), 0.0), axis=1, keepdims=True)
        return top, total

    def weighted(p, values, lo, hi):
        w = probs[p][:, lo:hi]
        high = w.astype(bf16)
        low = (w - high.astype(f32)).astype(bf16)
        out = jnp.dot(jnp.concatenate([high, low], axis=0), values, preferred_element_type=f32)
        return out[:16] + out[16:]

    def place(p, acc):
        for h in range(16):
            accs[h, p : p + 1, :] = acc[h : h + 1, (h // 4) * 128 : (h // 4) * 128 + 128]

    lane32 = lax.broadcasted_iota(i32, (32, 128), 1)

    def note(table, p, top, total):
        return jnp.where(lane32 == p, jnp.concatenate([top, total], axis=0), table)

    def query_second():
        settle(qa1r.at[pl.ds(1, 3)], q_rs.at[0])
        qa2s[...] = (qa1s[x] + qa1r[1] + qa1r[2] + qa1r[3]).reshape(4, 8, 1152)
        settle(qb1r.at[pl.ds(1, 3)], q_rs.at[1])
        qb2s[...] = qb1s[y] + qb1r[1] + qb1r[2] + qb1r[3]
        for step in (2, 1, 3):
            remote(qa2s.at[lax.rem(y + step, 4)], qa2r.at[step], q_ss.at[2], q_rs.at[2], dev(step))
            remote(qb2s.at[lax.rem(x + step, 4)], qb2r.at[step], q_ss.at[3], q_rs.at[3], dev(4 * step))

    def query_done():
        settle(qa2r.at[pl.ds(1, 3)], q_rs.at[2])
        first = qa2s[y] + qa2r[1] + qa2r[2] + qa2r[3]
        settle(qb2r.at[pl.ds(1, 3)], q_rs.at[3])
        second = qb2s[x] + qb2r[1] + qb2r[2] + qb2r[3]
        scale = lax.rsqrt(first[:, 1024:1025] / D + norm_eps)
        q8 = jnp.concatenate([first[:, :1024], second], axis=1) * scale * HEAD_DIM ** (-0.5)
        qflat[...] = q8
        for h in range(8):
            qfa[x, y, :, h, :] = q8[:, h * 128 : h * 128 + 128]
            qfb[x, y, :, h, :] = q8[:, 1024 + h * 128 : 1152 + h * 128]
        for step in (2, 1, 3):
            remote(qfa.at[x, y], qfa.at[x, y], a_ss.at[0], a_rs.at[0], dev(4 * step))
            remote(qfb.at[x, y], qfb.at[x, y], a_ss.at[1], a_rs.at[1], dev(step))

    def query_spread():
        settle(qfa.at[pl.ds(0, 3), 0], a_rs.at[0])
        settle(qfb.at[pl.ds(0, 3), 0], a_rs.at[1])
        for step in (2, 1, 3):
            remote(qfa.at[:, y], qfa.at[:, y], a_ss.at[2], a_rs.at[2], dev(step))
            remote(qfb.at[x], qfb.at[x], a_ss.at[3], a_rs.at[3], dev(4 * step))

    xy_start(0)
    query_second()
    xy_start(1)
    xy_start(2)
    z_start(0)
    query_done()
    xy_start(3)
    z_start(1)
    finish(0)
    query_spread()
    xy_start(4)
    z_start(2)
    finish(1)
    xy_start(5)
    z_start(3)
    finish(2)
    xy_start(6)
    tok_load.wait()
    own_key, own_value = tok[:, 0, :].astype(f32), tok[:, 1, :].astype(f32)
    lane8 = lax.broadcasted_iota(i32, (8, 128), 1)
    own_rows = jnp.zeros((8, 128), f32)
    for h in range(16):
        s = jnp.sum(
            qflat[:, h * 128 : h * 128 + 128] * own_key[:, (h // 4) * 128 : (h // 4) * 128 + 128],
            axis=1, keepdims=True,
        )
        own_rows = jnp.where(lane8 == h, s, own_rows)
    own_tops = jnp.concatenate([jnp.zeros((24, 128), f32), own_rows, jnp.zeros((96, 128), f32)], axis=0).T[:16]
    slot_row = jnp.zeros((8, 128), i32)
    for p in range(24):
        slot_row = jnp.where(lane8 == p, meta[48 + p] if p < 8 else meta[56 + p], slot_row)
    slot_row = jnp.where(lane8 >= 24, kv * 8 + lane8 - 24, slot_row)
    settle(qfa.at[:, pl.ds(0, 3)], a_rs.at[2])
    settle(qfb.at[pl.ds(0, 3)], a_rs.at[3])
    kept_load.wait()
    table = jnp.zeros((32, 128), f32)
    for p in range(8):
        table = note(table, p, *page_scores(p, kept[p, 0], meta[48 + p], meta[56 + p]))
    z_start(4)
    finish(3)
    xy_start(7)
    xy_start(8)
    for p in range(16):
        table = note(table, 8 + p, *page_scores(8 + p, fsk[p], meta[64 + p], meta[80 + p]))
    own_lane = lanes >= 24
    mine = jnp.concatenate(
        [
            jnp.where(own_lane, own_tops, table[:16]),
            jnp.where(own_lane, 1.0, table[16:]),
            slot_row.astype(f32),
        ],
        axis=0,
    )
    mine = jnp.where(lax.broadcasted_iota(i32, (40, 128), 1) < 32, mine, 0.0)
    turned = [mine] + [pltpu.roll(mine, 32 * q, 1) for q in range(1, 4)]
    for q in range(1, 4):
        mine = jnp.where(y == q, turned[q], mine)
    stats[kv] = mine
    for k in ORDER[::-1]:
        remote(stats.at[kv], stats.at[kv], s_ss.at[0], s_rs.at[0], dev(k))
    z_start(5)
    finish(4)
    z_start(6)
    finish(5)
    z_start(7)
    z_start(8)
    settle(stats.at[pl.ds(0, 15)], s_rs.at[0])
    every = jnp.concatenate(
        [stats[4 * i] + stats[4 * i + 1] + stats[4 * i + 2] + stats[4 * i + 3] for i in range(4)], axis=1
    )
    tops, sums, every_slot = every[:16], every[16:32], every[32:33].astype(i32)
    own_w = jnp.zeros((16, 128), f32)
    for p in range(32):
        slot = meta[48 + p] if p < 8 else (meta[56 + p] if p < 24 else kv * 8 + p - 24)
        same = jnp.broadcast_to(every_slot == slot, (16, 512))
        top = jnp.max(jnp.where(same, tops, neg_fill), axis=1, keepdims=True)
        total = jnp.sum(jnp.where(same, jnp.exp(tops - top) * sums, 0.0), axis=1, keepdims=True)
        if p < 24:
            probs[p] = jnp.exp(scores[p] - top) * (1.0 / total)
        else:
            own_w = jnp.where(lanes == p, jnp.exp(own_tops - top) * (1.0 / total), own_w)
    own_weight = jnp.concatenate([own_w, jnp.zeros((112, 128), f32)], axis=0).T[24:32]
    for h in range(16):
        g = (h // 4) * 128
        accs[h, 24:32, :] = own_weight[:, h : h + 1] * own_value[:, g : g + 128]
    rho = lax.broadcasted_iota(i32, (128, 512), 0)
    member = (lax.rem(rho, 64) // 4) * 8 + (rho // 64) * 4 + lax.rem(rho, 4) == every_slot
    member = jnp.where(member, 1.0, 0.0).astype(bf16)
    for p in range(8):
        place(p, weighted(p, kept[p, 1], 0, 128))

    def gather_values(c):
        _, row, tokens = PIECES[c]
        for p in range(16):
            part = weighted(8 + p, fsv[p, row : row + tokens, :], row, row + tokens)
            if row == 0:
                pvacc[p] = part
            else:
                pvacc[p] = pvacc[p] + part

    gather_values(4)
    gather_values(5)
    finish(6)
    gather_values(6)
    finish(7)
    gather_values(7)
    finish(8)
    _, row, tokens = PIECES[8]
    for p in range(16):
        place(8 + p, pvacc[p] + weighted(8 + p, fsv[p, row : row + tokens, :], row, row + tokens))

    tiles = [accs[h] for h in range(16)]
    group = lane32 // 8
    for bit in (1, 2, 4, 8):
        upper = (group & bit) != 0
        for h in range(16):
            if h & bit == 0:
                a, b = tiles[h], tiles[h + bit]
                tiles[h] = jnp.where(upper, pltpu.roll(b, 8 * bit, 1), a)
                tiles[h + bit] = jnp.where(upper, b, pltpu.roll(a, 128 - 8 * bit, 1))
    for j in range(16):
        msend[j] = tiles[j].astype(bf16)
    for k in ORDER[::-1]:
        remote(msend.at[peer_of(x, y, k)], mrecv.at[kv], m_ss.at[0], m_rs.at[0], dev(k))
    mrecv[kv] = msend[kv]
    settle(msend.at[pl.ds(0, 15)], m_rs.at[0])
    attn = jnp.dot(
        member, mrecv[...].reshape(512, 128), preferred_element_type=f32
    ).astype(bf16)

    rho = lax.broadcasted_iota(jnp.int32, (128, 128), 0)
    col = lax.broadcasted_iota(jnp.int32, (128, 128), 1)
    slot = (lax.rem(rho, 64) // 4) * 8 + (rho // 64) * 4 + lax.rem(rho, 4)
    perm = jnp.where(col == slot, 1.0, 0.0).astype(bf16)
    hid = jnp.dot(
        perm, hid_ref[:, pl.ds(pl.multiple_of(tp * 128, 128), 128)], preferred_element_type=f32
    )

    loads[0].wait()

    order = ORDER[::-1] + [0]
    for g in range(4):
        for i in range(4):
            k = order[4 * g + i]
            dest = peer_of(x, y, k)
            part = jnp.dot(
                attn, wout[:, pl.ds(pl.multiple_of(dest * 256, 256), 256)], preferred_element_type=f32
            )
            low, high = part[:, :128], part[:, 128:]
            own_part[g, i] = jnp.where(tp == 0, low, high)
            pair_send[g, i] = jnp.where(tp == 0, high, low).astype(bf16)
        remote(pair_send.at[g], pair_recv.at[g], pair_ss.at[0], pair_rs.at[g], partner)
    block = None
    for g in range(4):
        settle(pair_recv.at[g], pair_rs.at[g])
        for i in range(4):
            k = order[4 * g + i]
            total = own_part[g, i] + pair_recv[g, i].astype(f32)
            if k == 0:
                block = total + hid
            else:
                rs_send[k] = total.astype(bf16)
                remote(rs_send.at[k], rs_recv.at[k], rs_ss.at[0], rs_rs.at[0], dev(k))
    settle(rs_recv.at[pl.ds(1, 15)], rs_rs.at[0])
    for k in ORDER:
        block = block + rs_recv[k].astype(f32)
    ag[0, tp] = block.astype(bf16)

    def forward(k):
        remote(ag.at[k, tp], ag.at[k, tp], fw_ss.at[0], fw_rs.at[k], partner)

    forward(0)
    for k in ORDER:
        remote(ag.at[0, tp], ag.at[k, tp], ag_ss.at[0], ag_rs.at[k], dev(k))
    loads[1].wait()
    loads[2].wait()
    seq = [0] + ORDER
    nt = (((1,), (1,)), ((), ()))
    gate = jnp.zeros((128, 448), f32)
    upward = jnp.zeros((128, 448), f32)
    squares = jnp.zeros((128, 128), f32)
    mine = lax.broadcasted_iota(jnp.int32, (8, 128), 0) + tp * 64 + kv * 4
    pick = jnp.where(lax.broadcasted_iota(jnp.int32, (8, 128), 1) == mine, 1.0, 0.0).astype(bf16)
    for n, k in enumerate(seq):
        for later in seq[n + 1 : n + 7] if n == 0 else seq[n + 6 : n + 7]:
            settle(ag.at[later, tp], ag_rs.at[later])
            forward(later)
        settle(ag.at[k, other], fw_rs.at[k])
        src = source_of(x, y, k)
        both = jnp.concatenate([ag[k, 0], ag[k, 1]], axis=1)
        wide = both.astype(f32)
        squares = squares + wide[:, :128] * wide[:, :128] + wide[:, 128:] * wide[:, 128:]
        rows = pl.ds(pl.multiple_of(src * 256, 256), 256)
        normed = (wide * gain_ref[:, rows]).astype(bf16)
        gate = gate + lax.dot_general(normed, wg[:, rows], nt, preferred_element_type=f32)
        upward = upward + lax.dot_general(normed, wu[:, rows], nt, preferred_element_type=f32)
    scale = lax.rsqrt(jnp.sum(squares, axis=1, keepdims=True) / D + norm_eps)
    gate = gate * scale
    upward = upward * scale
    hunits[...] = (gate / (1.0 + jnp.exp(-gate)) * upward).astype(bf16)

    loads[3].wait()
    for c in range(4):
        cols = pl.ds(c * 1024, 1024)
        part = jnp.dot(hunits[...], wd[:, cols], preferred_element_type=f32)
        first, second = part[:64], part[64:]
        dsum[:, cols] = jnp.where(tp == 0, first, second)
        dp_send[c] = jnp.where(tp == 0, second, first).astype(bf16)
        remote(dp_send.at[c], dp_recv.at[c], dp_ss.at[0], dp_rs.at[c], partner)
    for c in range(4):
        settle(dp_recv.at[c], dp_rs.at[c])
        cols = pl.ds(c * 1024, 1024)
        dsum[:, cols] = dsum[:, cols] + dp_recv[c].astype(f32)
    for j in range(16):
        d_send[j] = dsum[4 * j : 4 * j + 4, :].astype(bf16)
    for k in ORDER[::-1]:
        remote(d_send.at[peer_of(x, y, k)], d_recv.at[k], d_ss.at[0], d_rs.at[0], dev(k))
    for c in range(nc):
        settle(xs[c], x_ss.at[c])
        settle(zs[c], z_ss.at[c])
    settle(qa1s.at[pl.ds(0, 3)], q_ss.at[0])
    settle(qb1s.at[pl.ds(0, 3)], q_ss.at[1])
    settle(qa2s.at[pl.ds(0, 3)], q_ss.at[2])
    settle(qb2s.at[pl.ds(0, 3)], q_ss.at[3])
    settle(qfa.at[pl.ds(0, 3), 0], a_ss.at[0])
    settle(qfb.at[pl.ds(0, 3), 0], a_ss.at[1])
    settle(qfa.at[:, pl.ds(0, 3)], a_ss.at[2])
    settle(qfb.at[pl.ds(0, 3)], a_ss.at[3])
    settle(stats.at[pl.ds(0, 15)], s_ss.at[0])
    settle(msend.at[pl.ds(0, 15)], m_ss.at[0])
    settle(pair_send, pair_ss.at[0])
    settle(rs_send.at[pl.ds(1, 15)], rs_ss.at[0])
    settle(rs_send.at[pl.ds(1, 15)], ag_ss.at[0])
    settle(rs_send, fw_ss.at[0])
    settle(dp_send, dp_ss.at[0])
    settle(fsk, out_sem.at[0])
    settle(fsv, out_sem.at[1])
    for k in range(16):
        for t in range(2):
            cols = pl.ds(pl.multiple_of((source_of(x, y, k) * 2 + t) * 128, 128), 128)
            resrow[:, cols] = jnp.dot(pick, ag[k, t], preferred_element_type=f32)
    total = resrow[...][:4]
    own = jnp.zeros((4, 4096), f32)
    for j in range(16):
        own = jnp.where(kv == j, dsum[4 * j : 4 * j + 4, :], own)
    total = total + own
    settle(d_recv.at[pl.ds(1, 15)], d_rs.at[0])
    for k in ORDER:
        total = total + d_recv[k].astype(f32)
    out_ref[...] = total.astype(bf16)
    settle(d_send.at[pl.ds(0, 15)], d_ss.at[0])


def step(meta, hidden, again, gain, token_kv, w_query, pool, resident, w_out, w_gate, w_up, w_down):
    bf16, f32 = jnp.bfloat16, jnp.float32
    vmem = pl.BlockSpec(memory_space=pltpu.VMEM)
    hbm = pl.BlockSpec(memory_space=pl.ANY)
    dma = pltpu.SemaphoreType.DMA
    nc = len(PIECES)

    def chunk(*lead):
        return [pltpu.VMEM((*lead, tokens, 512), bf16) for _, _, tokens in PIECES]

    return pl.pallas_call(
        step_kernel,
        name="step",
        out_shape=(
            jax.ShapeDtypeStruct((4, 4096), bf16),
            jax.ShapeDtypeStruct((16, 2, 128, 512), bf16),
        ),
        in_specs=[pl.BlockSpec(memory_space=pltpu.SMEM), vmem, vmem, vmem] + [hbm] * 8,
        out_specs=(vmem, hbm),
        scratch_shapes=[
            pltpu.VMEM((256, 2048), bf16),
            pltpu.VMEM((8, 2, 512), bf16),
            pltpu.VMEM((8, 2, 128, 512), bf16),
            pltpu.VMEM((4, 32, 1152), f32),
            pltpu.VMEM((4, 32, 1152), f32),
            pltpu.VMEM((4, 8, 1152), f32),
            pltpu.VMEM((4, 8, 1152), f32),
            pltpu.VMEM((4, 4, 8, 1024), f32),
            pltpu.VMEM((4, 4, 8, 1024), f32),
            pltpu.VMEM((4, 8, 1024), f32),
            pltpu.VMEM((4, 8, 1024), f32),
            pltpu.VMEM((4, 4, 8, 8, 128), f32),
            pltpu.VMEM((4, 4, 8, 8, 128), f32),
            pltpu.VMEM((8, 2048), f32),
            pltpu.VMEM((16, 128, 512), bf16),
            pltpu.VMEM((16, 128, 512), bf16),
            pltpu.VMEM((24, 16, 128), f32),
            pltpu.VMEM((24, 16, 128), f32),
            pltpu.VMEM((16, 16, 512), f32),
            pltpu.VMEM((16, 32, 128), f32),
            pltpu.VMEM((16, 40, 128), f32),
            pltpu.VMEM((16, 32, 128), bf16),
            pltpu.VMEM((16, 32, 128), bf16),
            pltpu.VMEM((128, 4096), bf16),
            pltpu.VMEM((448, 4096), bf16),
            pltpu.VMEM((448, 4096), bf16),
            pltpu.VMEM((448, 4096), bf16),
            pltpu.VMEM((4, 4, 128, 128), bf16),
            pltpu.VMEM((4, 4, 128, 128), bf16),
            pltpu.VMEM((4, 4, 128, 128), f32),
            pltpu.VMEM((16, 128, 128), bf16),
            pltpu.VMEM((16, 128, 128), bf16),
            pltpu.VMEM((16, 2, 128, 128), bf16),
            pltpu.VMEM((128, 448), bf16),
            pltpu.VMEM((4, 64, 1024), bf16),
            pltpu.VMEM((4, 64, 1024), bf16),
            pltpu.VMEM((64, 4096), f32),
            pltpu.VMEM((16, 4, 4096), bf16),
            pltpu.VMEM((16, 4, 4096), bf16),
            pltpu.VMEM((8, 4096), f32),
            *chunk(16), *chunk(15), *chunk(16), *chunk(3, 4), *chunk(4, 4),
            dma((2,)), dma((nc,)), dma((1,)), dma((2,)),
            dma((4,)), dma((4,)), dma((4,)), dma((4,)),
            dma((nc,)), dma((nc,)), dma((nc,)), dma((nc,)),
            dma((1,)), dma((1,)), dma((1,)), dma((1,)),
            dma((4,)), dma((1,)), dma((4,)), dma((1,)), dma((1,)), dma((1,)), dma((16,)),
            dma((1,)), dma((16,)), dma((1,)), dma((4,)), dma((1,)), dma((1,)),
        ],
        compiler_params=pltpu.CompilerParams(
            collective_id=0, has_side_effects=True, vmem_limit_bytes=62 * 1024 * 1024
        ),
    )(meta, hidden, again, gain, token_kv, w_query, pool, resident, w_out, w_gate, w_up, w_down)


def routing(new_owner, new_local, resident_slot, resident_len, new_slot, new_len):
    i32 = jnp.int32
    grp, kv = lax.axis_index("grp"), lax.axis_index("kv")
    mine = jnp.where(new_owner == grp * 16 + kv, new_local, 0)
    pick = jnp.sum(jnp.sum(mine, axis=0).reshape(16, 16), axis=1)
    column = lax.dynamic_slice(new_owner, (0, kv * 16), (4, 16))
    from_grp = column // 16
    earlier = jnp.arange(16)[None, :] < jnp.arange(16)[:, None]
    same = (from_grp[:, :, None] == from_grp[:, None, :]) & earlier[None]
    rank = jnp.sum(same.astype(i32), axis=2)
    hit = (from_grp == grp)[:, None, :] & (rank[:, None, :] == jnp.arange(4)[None, :, None])
    onward = jnp.sum(jnp.where(hit, (column % 16)[:, None, :], 0), axis=2).reshape(16)
    final = lax.dynamic_index_in_dim(from_grp * 4 + rank, grp, 0, keepdims=False)
    return jnp.concatenate(
        [pick, onward, final, resident_slot[0], resident_len[0], new_slot[0], new_len[0]]
    ).astype(i32)


def per_device(
    hidden_states,
    attn_gain,
    mlp_gain,
    w_query,
    w_out,
    w_gate,
    w_up,
    w_down,
    kv_pool,
    resident_cache,
    resident_slot,
    resident_len,
    new_owner,
    new_local,
    new_slot,
    new_len,
    token_kv,
):
    meta = routing(new_owner, new_local, resident_slot, resident_len, new_slot, new_len)
    mixed, new_pages = step(
        meta,
        hidden_states,
        attn_gain.reshape(1, 256),
        mlp_gain.reshape(1, 4096),
        token_kv,
        w_query,
        kv_pool.reshape(16, 256, 512),
        resident_cache[0],
        w_out.reshape(128, 4096),
        w_gate.T,
        w_up.T,
        w_down,
    )
    return (mixed, new_pages[None])


def solution(mesh):
    return jax.shard_map(
        per_device,
        mesh=mesh,
        in_specs=(
            P("grp", "kv"),
            P("kv"),
            P(),
            P("kv", "tp"),
            P("tp", "kv", None),
            P(None, KV_TP),
            P(None, KV_TP),
            P(KV_TP, None),
            P(GRP_KV, None, None, "tp"),
            P("grp", "kv", None, None, "tp"),
            P("grp", "kv"),
            P("grp", "kv"),
            P(),
            P(),
            P("grp", "kv"),
            P("grp", "kv"),
            P("grp", None, "tp"),
        ),
        out_specs=(P(GRP_KV_TP, None), P("grp", "kv", None, None, "tp")),
        check_vma=False,
    )
```

```python
import jax
import jax.numpy as jnp
from jax import lax
from jax.experimental import pallas as pl
from jax.experimental.pallas import tpu as pltpu
from jax.sharding import PartitionSpec as P

D = 4096
HEADS = 32
KV_HEADS = 8
HEAD_DIM = 128
KV_TP = ("kv", "tp")
GRP_KV = ("grp", "kv")
GRP_KV_TP = ("grp", "kv", "tp")


neg_fill = -1e30
norm_eps = 1e-05
MESH = pl.DeviceIdType.MESH


def peer_of(x, y, k):
    return lax.rem(x + k // 4, 4) * 4 + lax.rem(y + k % 4, 4)


def source_of(x, y, k):
    return lax.rem(x + 4 - k // 4, 4) * 4 + lax.rem(y + 4 - k % 4, 4)


ORDER = sorted(range(1, 16), key=lambda k: (min(k // 4, 4 - k // 4) + min(k % 4, 4 - k % 4), k))


PIECES = [(0, 0, 32), (0, 32, 32), (0, 64, 32), (0, 96, 32), (1, 0, 32), (1, 32, 32), (1, 64, 32), (1, 96, 16), (1, 112, 16)]


def step_kernel(
    res_slot, res_len, arr_slot, arr_len, own_ref, loc_ref, hid_ref, again_ref, gain_ref, tok_hbm, wq_hbm, pool_hbm, res_hbm, wout_hbm, wg_hbm, wu_hbm, wd_hbm,
    out_ref, cache_hbm,
    wq, tok, kept, qa1s, qa1r, qa2s, qa2r, qb1s, qb1r, qb2s, qb2r, qfa, qfb, qflat, fsk, fsv, scores, probs, pvacc, accs, stats, msend, mrecv,
    wout, wg, wu, wd, pair_send, pair_recv, own_part, rs_send, rs_recv, ag, hunits,
    dp_send, dp_recv, dsum, d_send, d_recv, resrow, picks, *rest,
):
    f32, bf16, i32 = jnp.float32, jnp.bfloat16, jnp.int32
    nc = len(PIECES)
    pool, xs, xr, zs, zr = (rest[i * nc : (i + 1) * nc] for i in range(5))
    (ld_sem, pool_sem, kept_sem, out_sem, q_ss, q_rs, a_ss, a_rs, x_ss, x_rs, z_ss, z_rs, s_ss, s_rs,
     m_ss, m_rs, w_sem, pair_ss, pair_rs, rs_ss, rs_rs, ag_ss, ag_rs, fw_ss, fw_rs, dp_ss, dp_rs, d_ss,
     d_rs) = rest[5 * nc :]
    grp, kv, tp = lax.axis_index("grp"), lax.axis_index("kv"), lax.axis_index("tp")
    x, y = kv // 4, lax.rem(kv, 4)
    other = 1 - tp
    partner = (grp, kv, other)

    def dev(k):
        return (grp, peer_of(x, y, k), tp)

    def zdev(dz):
        return (lax.rem(grp + dz, 4), kv, tp)

    def remote(src, dst, send, recv, device):
        copy = pltpu.make_async_remote_copy(
            src_ref=src, dst_ref=dst, send_sem=send, recv_sem=recv, device_id=device,
            device_id_type=MESH,
        )
        copy.start()
        return copy

    def settle(ref, sem):
        pltpu.make_async_copy(ref, ref, sem).wait()

    wq_load = pltpu.make_async_copy(wq_hbm, wq, ld_sem.at[0])
    wq_load.start()
    pool_loads = []
    for c in range(nc):
        load = pltpu.make_async_copy(pool_hbm.at[:, pl.ds(PIECES[c][0] * 128 + PIECES[c][1], PIECES[c][2]), :], pool[c], pool_sem.at[c])
        load.start()
        pool_loads.append(load)
    kept_load = pltpu.make_async_copy(res_hbm, kept, kept_sem.at[0])
    kept_load.start()
    tok_load = pltpu.make_async_copy(
        tok_hbm.at[pl.ds(pl.multiple_of(kv * 8, 8), 8)], tok, ld_sem.at[1]
    )
    tok_load.start()

    loads = [
        pltpu.make_async_copy(src, dst, w_sem.at[i])
        for i, (src, dst) in enumerate([(wout_hbm, wout), (wg_hbm, wg), (wu_hbm, wu), (wd_hbm, wd)])
    ]
    for load in loads:
        load.start()

    barrier = pltpu.get_barrier_semaphore()
    pl.semaphore_signal(barrier, inc=1, device_id=partner, device_id_type=MESH)
    for k in range(1, 16):
        pl.semaphore_signal(barrier, inc=1, device_id=dev(k), device_id_type=MESH)
    for dz in range(1, 4):
        pl.semaphore_signal(barrier, inc=1, device_id=zdev(dz), device_id_type=MESH)

    feats = hid_ref[...].astype(f32)
    normed = (feats * again_ref[...]).astype(bf16)
    squares = jnp.sum(feats * feats, axis=1, keepdims=True)
    wq_load.wait()
    for h in range(2):
        part = jnp.dot(normed, wq[:, h * 512 : h * 512 + 512], preferred_element_type=f32)
        qa1s[:, :, h * 512 : h * 512 + 512] = part.reshape(4, 32, 512)
    qa1s[:, :, 1024:1152] = jnp.broadcast_to(squares, (128, 128)).reshape(4, 32, 128)
    for h in range(2):
        part = jnp.dot(normed, wq[:, 1024 + h * 512 : 1536 + h * 512], preferred_element_type=f32)
        for i in range(16):
            qb1s[i % 4, i // 4, :, h * 512 : h * 512 + 512] = part[8 * i : 8 * i + 8]
    pl.semaphore_wait(barrier, 19)

    for step in (2, 1, 3):
        remote(qa1s.at[lax.rem(x + step, 4)], qa1r.at[step], q_ss.at[0], q_rs.at[0], dev(4 * step))
        remote(qb1s.at[lax.rem(y + step, 4)], qb1r.at[step], q_ss.at[1], q_rs.at[1], dev(step))

    owners = own_ref[...]
    spot = lax.broadcasted_iota(i32, (4, 256), 1)
    group_row = lax.broadcasted_iota(i32, (4, 256), 0)
    mine = jnp.where(owners == grp * 16 + kv, loc_ref[...], 0)
    pick = [jnp.sum(jnp.where(spot // 16 == j, mine, 0)) for j in range(16)]
    from_grp = owners // 16
    rank = jnp.zeros((4, 256), i32)
    for back in range(1, 16):
        earlier = pltpu.roll(from_grp, back, 1) == from_grp
        rank = rank + jnp.where(earlier & (lax.rem(spot, 16) >= back), 1, 0)
    here = spot // 16 == kv
    leaving = here & (from_grp == grp)
    sender = lax.rem(owners, 16)
    onward = [
        [jnp.sum(jnp.where(leaving & (group_row == g) & (rank == r), sender, 0)) for r in range(4)]
        for g in range(4)
    ]
    landed = jnp.where(here & (group_row == grp), from_grp * 4 + rank, 0)
    landing = [jnp.sum(jnp.where(lax.rem(spot, 16) == i, landed, 0)) for i in range(16)]
    del mine
    for j in range(16):
        picks[j] = pick[j]
        picks[32 + j] = landing[j]
    for g in range(4):
        for r in range(4):
            picks[16 + 4 * g + r] = onward[g][r]

    def xy_start(c):
        pool_loads[c].wait()
        xr[c][kv] = pool[c][picks[kv]]
        for k in range(1, 16):
            xs[c][k - 1] = pool[c][picks[peer_of(x, y, k)]]
        for k in ORDER[::-1]:
            remote(xs[c].at[k - 1], xr[c].at[kv], x_ss.at[c], x_rs.at[c], dev(k))

    def z_start(c):
        settle(xs[c], x_rs.at[c])
        for dz in range(4):
            g = lax.rem(grp + dz, 4)
            for r in range(4):
                page = xr[c][picks[16 + g * 4 + r]]
                if dz == 0:
                    zr[c][grp, r] = page
                else:
                    zs[c][dz - 1, r] = page
        for dz in (2, 1, 3):
            remote(zs[c].at[dz - 1], zr[c].at[grp], z_ss.at[c], z_rs.at[c], zdev(dz))

    def finish(c):
        settle(zs[c], z_rs.at[c])
        half, row, tokens = PIECES[c]
        final = (fsk, fsv)[half]
        for i in range(16):
            where = picks[32 + i]
            final[i, row : row + tokens, :] = zr[c][where // 4, lax.rem(where, 4)]
        pltpu.make_async_copy(
            final.at[:, pl.ds(row, tokens), :], cache_hbm.at[:, half, pl.ds(row, tokens), :], out_sem.at[half]
        ).start()

    head_of = lax.broadcasted_iota(i32, (16, 512), 0) // 4
    block_of = lax.broadcasted_iota(i32, (16, 512), 1) // 128
    diag = head_of == block_of
    lanes = lax.broadcasted_iota(i32, (16, 128), 1)

    def page_scores(p, keys, slot, filled):
        place_x, place_y, place_s = slot // 32, lax.rem(slot // 8, 4), lax.rem(slot, 8)
        q = jnp.concatenate([qfa[place_x, place_y, place_s], qfb[place_x, place_y, place_s]], axis=0)
        wide = jnp.where(diag, jnp.concatenate([q, q, q, q], axis=1), 0.0)
        high = wide.astype(bf16)
        left = wide - high.astype(f32)
        mid = left.astype(bf16)
        low = (left - mid.astype(f32)).astype(bf16)
        rows = jnp.concatenate([high, mid, low], axis=0)
        s = lax.dot_general(rows, keys, (((1,), (1,)), ((), ())), preferred_element_type=f32)
        s = s[:16] + s[16:32] + s[32:]
        s = jnp.where(lanes < filled, s, neg_fill)
        scores[p] = s
        top = jnp.max(s, axis=1, keepdims=True)
        total = jnp.sum(jnp.where(lanes < filled, jnp.exp(s - top), 0.0), axis=1, keepdims=True)
        return top, total

    def weighted(p, values, lo, hi):
        w = probs[p][:, lo:hi]
        high = w.astype(bf16)
        low = (w - high.astype(f32)).astype(bf16)
        out = jnp.dot(jnp.concatenate([high, low], axis=0), values, preferred_element_type=f32)
        return out[:16] + out[16:]

    def place(p, acc):
        for h in range(16):
            accs[h, p : p + 1, :] = acc[h : h + 1, (h // 4) * 128 : (h // 4) * 128 + 128]

    lane32 = lax.broadcasted_iota(i32, (32, 128), 1)

    def note(table, p, top, total):
        return jnp.where(lane32 == p, jnp.concatenate([top, total], axis=0), table)

    def query_second():
        settle(qa1r.at[pl.ds(1, 3)], q_rs.at[0])
        qa2s[...] = (qa1s[x] + qa1r[1] + qa1r[2] + qa1r[3]).reshape(4, 8, 1152)
        settle(qb1r.at[pl.ds(1, 3)], q_rs.at[1])
        qb2s[...] = qb1s[y] + qb1r[1] + qb1r[2] + qb1r[3]
        for step in (2, 1, 3):
            remote(qa2s.at[lax.rem(y + step, 4)], qa2r.at[step], q_ss.at[2], q_rs.at[2], dev(step))
            remote(qb2s.at[lax.rem(x + step, 4)], qb2r.at[step], q_ss.at[3], q_rs.at[3], dev(4 * step))

    def query_done():
        settle(qa2r.at[pl.ds(1, 3)], q_rs.at[2])
        first = qa2s[y] + qa2r[1] + qa2r[2] + qa2r[3]
        settle(qb2r.at[pl.ds(1, 3)], q_rs.at[3])
        second = qb2s[x] + qb2r[1] + qb2r[2] + qb2r[3]
        scale = lax.rsqrt(first[:, 1024:1025] / D + norm_eps)
        q8 = jnp.concatenate([first[:, :1024], second], axis=1) * scale * HEAD_DIM ** (-0.5)
        qflat[...] = q8
        for h in range(8):
            qfa[x, y, :, h, :] = q8[:, h * 128 : h * 128 + 128]
            qfb[x, y, :, h, :] = q8[:, 1024 + h * 128 : 1152 + h * 128]
        for step in (2, 1, 3):
            remote(qfa.at[x, y], qfa.at[x, y], a_ss.at[0], a_rs.at[0], dev(4 * step))
            remote(qfb.at[x, y], qfb.at[x, y], a_ss.at[1], a_rs.at[1], dev(step))

    def query_spread():
        settle(qfa.at[pl.ds(0, 3), 0], a_rs.at[0])
        settle(qfb.at[pl.ds(0, 3), 0], a_rs.at[1])
        for step in (2, 1, 3):
            remote(qfa.at[:, y], qfa.at[:, y], a_ss.at[2], a_rs.at[2], dev(step))
            remote(qfb.at[x], qfb.at[x], a_ss.at[3], a_rs.at[3], dev(4 * step))

    xy_start(0)
    query_second()
    xy_start(1)
    xy_start(2)
    z_start(0)
    query_done()
    xy_start(3)
    z_start(1)
    finish(0)
    query_spread()
    xy_start(4)
    z_start(2)
    finish(1)
    xy_start(5)
    z_start(3)
    finish(2)
    xy_start(6)
    tok_load.wait()
    own_key, own_value = tok[:, 0, :].astype(f32), tok[:, 1, :].astype(f32)
    lane8 = lax.broadcasted_iota(i32, (8, 128), 1)
    own_rows = jnp.zeros((8, 128), f32)
    for h in range(16):
        s = jnp.sum(
            qflat[:, h * 128 : h * 128 + 128] * own_key[:, (h // 4) * 128 : (h // 4) * 128 + 128],
            axis=1, keepdims=True,
        )
        own_rows = jnp.where(lane8 == h, s, own_rows)
    own_tops = jnp.concatenate([jnp.zeros((24, 128), f32), own_rows, jnp.zeros((96, 128), f32)], axis=0).T[:16]
    slot_row = jnp.zeros((8, 128), i32)
    for p in range(24):
        slot_row = jnp.where(lane8 == p, res_slot[0, p] if p < 8 else arr_slot[0, p - 8], slot_row)
    slot_row = jnp.where(lane8 >= 24, kv * 8 + lane8 - 24, slot_row)
    settle(qfa.at[:, pl.ds(0, 3)], a_rs.at[2])
    settle(qfb.at[pl.ds(0, 3)], a_rs.at[3])
    kept_load.wait()
    table = jnp.zeros((32, 128), f32)
    for p in range(8):
        table = note(table, p, *page_scores(p, kept[p, 0], res_slot[0, p], res_len[0, p]))
    z_start(4)
    finish(3)
    xy_start(7)
    xy_start(8)
    for p in range(16):
        table = note(table, 8 + p, *page_scores(8 + p, fsk[p], arr_slot[0, p], arr_len[0, p]))
    own_lane = lanes >= 24
    mine = jnp.concatenate(
        [
            jnp.where(own_lane, own_tops, table[:16]),
            jnp.where(own_lane, 1.0, table[16:]),
            slot_row.astype(f32),
        ],
        axis=0,
    )
    mine = jnp.where(lax.broadcasted_iota(i32, (40, 128), 1) < 32, mine, 0.0)
    turned = [mine] + [pltpu.roll(mine, 32 * q, 1) for q in range(1, 4)]
    for q in range(1, 4):
        mine = jnp.where(y == q, turned[q], mine)
    stats[kv] = mine
    for k in ORDER[::-1]:
        remote(stats.at[kv], stats.at[kv], s_ss.at[0], s_rs.at[0], dev(k))
    z_start(5)
    finish(4)
    z_start(6)
    finish(5)
    z_start(7)
    z_start(8)
    settle(stats.at[pl.ds(0, 15)], s_rs.at[0])
    every = jnp.concatenate(
        [stats[4 * i] + stats[4 * i + 1] + stats[4 * i + 2] + stats[4 * i + 3] for i in range(4)], axis=1
    )
    tops, sums, every_slot = every[:16], every[16:32], every[32:33].astype(i32)
    own_w = jnp.zeros((16, 128), f32)
    for p in range(32):
        slot = res_slot[0, p] if p < 8 else (arr_slot[0, p - 8] if p < 24 else kv * 8 + p - 24)
        same = jnp.broadcast_to(every_slot == slot, (16, 512))
        top = jnp.max(jnp.where(same, tops, neg_fill), axis=1, keepdims=True)
        total = jnp.sum(jnp.where(same, jnp.exp(tops - top) * sums, 0.0), axis=1, keepdims=True)
        if p < 24:
            probs[p] = jnp.exp(scores[p] - top) * (1.0 / total)
        else:
            own_w = jnp.where(lanes == p, jnp.exp(own_tops - top) * (1.0 / total), own_w)
    own_weight = jnp.concatenate([own_w, jnp.zeros((112, 128), f32)], axis=0).T[24:32]
    for h in range(16):
        g = (h // 4) * 128
        accs[h, 24:32, :] = own_weight[:, h : h + 1] * own_value[:, g : g + 128]
    rho = lax.broadcasted_iota(i32, (128, 512), 0)
    member = (lax.rem(rho, 64) // 4) * 8 + (rho // 64) * 4 + lax.rem(rho, 4) == every_slot
    member = jnp.where(member, 1.0, 0.0).astype(bf16)
    for p in range(8):
        place(p, weighted(p, kept[p, 1], 0, 128))

    def gather_values(c):
        _, row, tokens = PIECES[c]
        for p in range(16):
            part = weighted(8 + p, fsv[p, row : row + tokens, :], row, row + tokens)
            if row == 0:
                pvacc[p] = part
            else:
                pvacc[p] = pvacc[p] + part

    gather_values(4)
    gather_values(5)
    finish(6)
    gather_values(6)
    finish(7)
    gather_values(7)
    finish(8)
    _, row, tokens = PIECES[8]
    for p in range(16):
        place(8 + p, pvacc[p] + weighted(8 + p, fsv[p, row : row + tokens, :], row, row + tokens))

    tiles = [accs[h] for h in range(16)]
    group = lane32 // 8
    for bit in (1, 2, 4, 8):
        upper = (group & bit) != 0
        for h in range(16):
            if h & bit == 0:
                a, b = tiles[h], tiles[h + bit]
                tiles[h] = jnp.where(upper, pltpu.roll(b, 8 * bit, 1), a)
                tiles[h + bit] = jnp.where(upper, b, pltpu.roll(a, 128 - 8 * bit, 1))
    for j in range(16):
        msend[j] = tiles[j].astype(bf16)
    for k in ORDER[::-1]:
        remote(msend.at[peer_of(x, y, k)], mrecv.at[kv], m_ss.at[0], m_rs.at[0], dev(k))
    mrecv[kv] = msend[kv]
    settle(msend.at[pl.ds(0, 15)], m_rs.at[0])
    attn = jnp.dot(
        member, mrecv[...].reshape(512, 128), preferred_element_type=f32
    ).astype(bf16)

    rho = lax.broadcasted_iota(jnp.int32, (128, 128), 0)
    col = lax.broadcasted_iota(jnp.int32, (128, 128), 1)
    slot = (lax.rem(rho, 64) // 4) * 8 + (rho // 64) * 4 + lax.rem(rho, 4)
    perm = jnp.where(col == slot, 1.0, 0.0).astype(bf16)
    hid = jnp.dot(
        perm, hid_ref[:, pl.ds(pl.multiple_of(tp * 128, 128), 128)], preferred_element_type=f32
    )

    loads[0].wait()

    order = ORDER[::-1] + [0]
    for g in range(4):
        for i in range(4):
            k = order[4 * g + i]
            dest = peer_of(x, y, k)
            part = jnp.dot(
                attn, wout[:, pl.ds(pl.multiple_of(dest * 256, 256), 256)], preferred_element_type=f32
            )
            low, high = part[:, :128], part[:, 128:]
            own_part[g, i] = jnp.where(tp == 0, low, high)
            pair_send[g, i] = jnp.where(tp == 0, high, low).astype(bf16)
        remote(pair_send.at[g], pair_recv.at[g], pair_ss.at[0], pair_rs.at[g], partner)
    block = None
    for g in range(4):
        settle(pair_recv.at[g], pair_rs.at[g])
        for i in range(4):
            k = order[4 * g + i]
            total = own_part[g, i] + pair_recv[g, i].astype(f32)
            if k == 0:
                block = total + hid
            else:
                rs_send[k] = total.astype(bf16)
                remote(rs_send.at[k], rs_recv.at[k], rs_ss.at[0], rs_rs.at[0], dev(k))
    settle(rs_recv.at[pl.ds(1, 15)], rs_rs.at[0])
    for k in ORDER:
        block = block + rs_recv[k].astype(f32)
    ag[0, tp] = block.astype(bf16)

    def forward(k):
        remote(ag.at[k, tp], ag.at[k, tp], fw_ss.at[0], fw_rs.at[k], partner)

    forward(0)
    for k in ORDER:
        remote(ag.at[0, tp], ag.at[k, tp], ag_ss.at[0], ag_rs.at[k], dev(k))
    loads[1].wait()
    loads[2].wait()
    seq = [0] + ORDER
    nt = (((1,), (1,)), ((), ()))
    gate = jnp.zeros((128, 448), f32)
    upward = jnp.zeros((128, 448), f32)
    squares = jnp.zeros((128, 128), f32)
    mine = lax.broadcasted_iota(jnp.int32, (8, 128), 0) + tp * 64 + kv * 4
    pick = jnp.where(lax.broadcasted_iota(jnp.int32, (8, 128), 1) == mine, 1.0, 0.0).astype(bf16)
    for n, k in enumerate(seq):
        for later in seq[n + 1 : n + 7] if n == 0 else seq[n + 6 : n + 7]:
            settle(ag.at[later, tp], ag_rs.at[later])
            forward(later)
        settle(ag.at[k, other], fw_rs.at[k])
        src = source_of(x, y, k)
        both = jnp.concatenate([ag[k, 0], ag[k, 1]], axis=1)
        wide = both.astype(f32)
        squares = squares + wide[:, :128] * wide[:, :128] + wide[:, 128:] * wide[:, 128:]
        rows = pl.ds(pl.multiple_of(src * 256, 256), 256)
        normed = (wide * gain_ref[:, rows]).astype(bf16)
        gate = gate + lax.dot_general(normed, wg[:, rows], nt, preferred_element_type=f32)
        upward = upward + lax.dot_general(normed, wu[:, rows], nt, preferred_element_type=f32)
    scale = lax.rsqrt(jnp.sum(squares, axis=1, keepdims=True) / D + norm_eps)
    gate = gate * scale
    upward = upward * scale
    hunits[...] = (gate / (1.0 + jnp.exp(-gate)) * upward).astype(bf16)

    loads[3].wait()
    for c in range(4):
        cols = pl.ds(c * 1024, 1024)
        part = jnp.dot(hunits[...], wd[:, cols], preferred_element_type=f32)
        first, second = part[:64], part[64:]
        dsum[:, cols] = jnp.where(tp == 0, first, second)
        dp_send[c] = jnp.where(tp == 0, second, first).astype(bf16)
        remote(dp_send.at[c], dp_recv.at[c], dp_ss.at[0], dp_rs.at[c], partner)
    for c in range(4):
        settle(dp_recv.at[c], dp_rs.at[c])
        cols = pl.ds(c * 1024, 1024)
        dsum[:, cols] = dsum[:, cols] + dp_recv[c].astype(f32)
    for j in range(16):
        d_send[j] = dsum[4 * j : 4 * j + 4, :].astype(bf16)
    for k in ORDER[::-1]:
        remote(d_send.at[peer_of(x, y, k)], d_recv.at[k], d_ss.at[0], d_rs.at[0], dev(k))
    for c in range(nc):
        settle(xs[c], x_ss.at[c])
        settle(zs[c], z_ss.at[c])
    settle(qa1s.at[pl.ds(0, 3)], q_ss.at[0])
    settle(qb1s.at[pl.ds(0, 3)], q_ss.at[1])
    settle(qa2s.at[pl.ds(0, 3)], q_ss.at[2])
    settle(qb2s.at[pl.ds(0, 3)], q_ss.at[3])
    settle(qfa.at[pl.ds(0, 3), 0], a_ss.at[0])
    settle(qfb.at[pl.ds(0, 3), 0], a_ss.at[1])
    settle(qfa.at[:, pl.ds(0, 3)], a_ss.at[2])
    settle(qfb.at[pl.ds(0, 3)], a_ss.at[3])
    settle(stats.at[pl.ds(0, 15)], s_ss.at[0])
    settle(msend.at[pl.ds(0, 15)], m_ss.at[0])
    settle(pair_send, pair_ss.at[0])
    settle(rs_send.at[pl.ds(1, 15)], rs_ss.at[0])
    settle(rs_send.at[pl.ds(1, 15)], ag_ss.at[0])
    settle(rs_send, fw_ss.at[0])
    settle(dp_send, dp_ss.at[0])
    settle(fsk, out_sem.at[0])
    settle(fsv, out_sem.at[1])
    for k in range(16):
        for t in range(2):
            cols = pl.ds(pl.multiple_of((source_of(x, y, k) * 2 + t) * 128, 128), 128)
            resrow[:, cols] = jnp.dot(pick, ag[k, t], preferred_element_type=f32)
    total = resrow[...][:4]
    own = jnp.zeros((4, 4096), f32)
    for j in range(16):
        own = jnp.where(kv == j, dsum[4 * j : 4 * j + 4, :], own)
    total = total + own
    settle(d_recv.at[pl.ds(1, 15)], d_rs.at[0])
    for k in ORDER:
        total = total + d_recv[k].astype(f32)
    out_ref[...] = total.astype(bf16)
    settle(d_send.at[pl.ds(0, 15)], d_ss.at[0])


def step(*operands):
    bf16, f32 = jnp.bfloat16, jnp.float32
    smem = pl.BlockSpec(memory_space=pltpu.SMEM)
    vmem = pl.BlockSpec(memory_space=pltpu.VMEM)
    hbm = pl.BlockSpec(memory_space=pl.ANY)
    dma = pltpu.SemaphoreType.DMA
    nc = len(PIECES)

    def chunk(*lead):
        return [pltpu.VMEM((*lead, tokens, 512), bf16) for _, _, tokens in PIECES]

    return pl.pallas_call(
        step_kernel,
        name="step",
        out_shape=(
            jax.ShapeDtypeStruct((4, 4096), bf16),
            jax.ShapeDtypeStruct((16, 2, 128, 512), bf16),
        ),
        in_specs=[smem] * 4 + [vmem] * 5 + [hbm] * 8,
        out_specs=(vmem, hbm),
        scratch_shapes=[
            pltpu.VMEM((256, 2048), bf16),
            pltpu.VMEM((8, 2, 512), bf16),
            pltpu.VMEM((8, 2, 128, 512), bf16),
            pltpu.VMEM((4, 32, 1152), f32),
            pltpu.VMEM((4, 32, 1152), f32),
            pltpu.VMEM((4, 8, 1152), f32),
            pltpu.VMEM((4, 8, 1152), f32),
            pltpu.VMEM((4, 4, 8, 1024), f32),
            pltpu.VMEM((4, 4, 8, 1024), f32),
            pltpu.VMEM((4, 8, 1024), f32),
            pltpu.VMEM((4, 8, 1024), f32),
            pltpu.VMEM((4, 4, 8, 8, 128), f32),
            pltpu.VMEM((4, 4, 8, 8, 128), f32),
            pltpu.VMEM((8, 2048), f32),
            pltpu.VMEM((16, 128, 512), bf16),
            pltpu.VMEM((16, 128, 512), bf16),
            pltpu.VMEM((24, 16, 128), f32),
            pltpu.VMEM((24, 16, 128), f32),
            pltpu.VMEM((16, 16, 512), f32),
            pltpu.VMEM((16, 32, 128), f32),
            pltpu.VMEM((16, 40, 128), f32),
            pltpu.VMEM((16, 32, 128), bf16),
            pltpu.VMEM((16, 32, 128), bf16),
            pltpu.VMEM((128, 4096), bf16),
            pltpu.VMEM((448, 4096), bf16),
            pltpu.VMEM((448, 4096), bf16),
            pltpu.VMEM((448, 4096), bf16),
            pltpu.VMEM((4, 4, 128, 128), bf16),
            pltpu.VMEM((4, 4, 128, 128), bf16),
            pltpu.VMEM((4, 4, 128, 128), f32),
            pltpu.VMEM((16, 128, 128), bf16),
            pltpu.VMEM((16, 128, 128), bf16),
            pltpu.VMEM((16, 2, 128, 128), bf16),
            pltpu.VMEM((128, 448), bf16),
            pltpu.VMEM((4, 64, 1024), bf16),
            pltpu.VMEM((4, 64, 1024), bf16),
            pltpu.VMEM((64, 4096), f32),
            pltpu.VMEM((16, 4, 4096), bf16),
            pltpu.VMEM((16, 4, 4096), bf16),
            pltpu.VMEM((8, 4096), f32),
            pltpu.SMEM((48,), jnp.int32),
            *chunk(16), *chunk(15), *chunk(16), *chunk(3, 4), *chunk(4, 4),
            dma((2,)), dma((nc,)), dma((1,)), dma((2,)),
            dma((4,)), dma((4,)), dma((4,)), dma((4,)),
            dma((nc,)), dma((nc,)), dma((nc,)), dma((nc,)),
            dma((1,)), dma((1,)), dma((1,)), dma((1,)),
            dma((4,)), dma((1,)), dma((4,)), dma((1,)), dma((1,)), dma((1,)), dma((16,)),
            dma((1,)), dma((16,)), dma((1,)), dma((4,)), dma((1,)), dma((1,)),
        ],
        compiler_params=pltpu.CompilerParams(
            collective_id=0, has_side_effects=True, vmem_limit_bytes=62 * 1024 * 1024
        ),
    )(*operands)


def per_device(
    hidden_states,
    attn_gain,
    mlp_gain,
    w_query,
    w_out,
    w_gate,
    w_up,
    w_down,
    kv_pool,
    resident_cache,
    resident_slot,
    resident_len,
    new_owner,
    new_local,
    new_slot,
    new_len,
    token_kv,
):
    mixed, new_pages = step(
        resident_slot,
        resident_len,
        new_slot,
        new_len,
        new_owner,
        new_local,
        hidden_states,
        attn_gain.reshape(1, 256),
        mlp_gain.reshape(1, 4096),
        token_kv,
        w_query,
        kv_pool.reshape(16, 256, 512),
        resident_cache[0],
        w_out.reshape(128, 4096),
        w_gate.T,
        w_up.T,
        w_down,
    )
    return (mixed, new_pages[None])


def solution(mesh):
    return jax.shard_map(
        per_device,
        mesh=mesh,
        in_specs=(
            P("grp", "kv"),
            P("kv"),
            P(),
            P("kv", "tp"),
            P("tp", "kv", None),
            P(None, KV_TP),
            P(None, KV_TP),
            P(KV_TP, None),
            P(GRP_KV, None, None, "tp"),
            P("grp", "kv", None, None, "tp"),
            P("grp", "kv"),
            P("grp", "kv"),
            P(),
            P(),
            P("grp", "kv"),
            P("grp", "kv"),
            P("grp", None, "tp"),
        ),
        out_specs=(P(GRP_KV_TP, None), P("grp", "kv", None, None, "tp")),
        check_vma=False,
    )
```

```python
import jax
import jax.numpy as jnp
from jax import lax
from jax.experimental import pallas as pl
from jax.experimental.pallas import tpu as pltpu
from jax.sharding import PartitionSpec as P

D = 4096
HEADS = 32
KV_HEADS = 8
HEAD_DIM = 128
KV_TP = ("kv", "tp")
GRP_KV = ("grp", "kv")
GRP_KV_TP = ("grp", "kv", "tp")


neg_fill = -1e30
norm_eps = 1e-05
MESH = pl.DeviceIdType.MESH


def peer_of(x, y, k):
    return lax.rem(x + k // 4, 4) * 4 + lax.rem(y + k % 4, 4)


def source_of(x, y, k):
    return lax.rem(x + 4 - k // 4, 4) * 4 + lax.rem(y + 4 - k % 4, 4)


ORDER = sorted(range(1, 16), key=lambda k: (min(k // 4, 4 - k // 4) + min(k % 4, 4 - k % 4), k))


PIECES = [(0, 0, 32), (0, 32, 32), (0, 64, 32), (0, 96, 32), (1, 0, 32), (1, 32, 32), (1, 64, 32), (1, 96, 16), (1, 112, 16)]


def step_kernel(
    res_slot, res_len, arr_slot, arr_len, own_ref, loc_ref, hid_ref, again_ref, gain_ref, tok_hbm, wq_hbm, pool_hbm, res_hbm, wout_hbm, wg_hbm, wu_hbm, wd_hbm,
    out_ref, cache_hbm,
    wq, tok, kept, qa1s, qa1r, qa2s, qa2r, qb1s, qb1r, qb2s, qb2r, qfa, qfb, qflat, fsk, fsv, scores, probs, pvacc, accs, stats, msend, mrecv,
    wout, wpart, wg, wu, wd, rs_send, rs_recv, ag, hunits,
    dp_send, dp_recv, dsum, d_send, d_recv, resrow, picks, *rest,
):
    f32, bf16, i32 = jnp.float32, jnp.bfloat16, jnp.int32
    nc = len(PIECES)
    pool, xs, xr, zs, zr = (rest[i * nc : (i + 1) * nc] for i in range(5))
    (ld_sem, pool_sem, kept_sem, out_sem, q_ss, q_rs, a_ss, a_rs, x_ss, x_rs, z_ss, z_rs, s_ss, s_rs,
     m_ss, m_rs, w_sem, wp_ss, wp_rs, rs_ss, rs_rs, ag_ss, ag_rs, fw_ss, fw_rs, dp_ss, dp_rs, d_ss,
     d_rs) = rest[5 * nc :]
    grp, kv, tp = lax.axis_index("grp"), lax.axis_index("kv"), lax.axis_index("tp")
    x, y = kv // 4, lax.rem(kv, 4)
    other = 1 - tp
    partner = (grp, kv, other)

    def dev(k):
        return (grp, peer_of(x, y, k), tp)

    def zdev(dz):
        return (lax.rem(grp + dz, 4), kv, tp)

    def remote(src, dst, send, recv, device):
        copy = pltpu.make_async_remote_copy(
            src_ref=src, dst_ref=dst, send_sem=send, recv_sem=recv, device_id=device,
            device_id_type=MESH,
        )
        copy.start()
        return copy

    def settle(ref, sem):
        pltpu.make_async_copy(ref, ref, sem).wait()

    wq_load = pltpu.make_async_copy(wq_hbm, wq, ld_sem.at[0])
    wq_load.start()
    pool_loads = []
    for c in range(nc):
        load = pltpu.make_async_copy(pool_hbm.at[:, pl.ds(PIECES[c][0] * 128 + PIECES[c][1], PIECES[c][2]), :], pool[c], pool_sem.at[c])
        load.start()
        pool_loads.append(load)
    kept_load = pltpu.make_async_copy(res_hbm, kept, kept_sem.at[0])
    kept_load.start()
    tok_load = pltpu.make_async_copy(
        tok_hbm.at[pl.ds(pl.multiple_of(kv * 8, 8), 8)], tok, ld_sem.at[1]
    )
    tok_load.start()

    loads = [
        pltpu.make_async_copy(src, dst, w_sem.at[i])
        for i, (src, dst) in enumerate([(wout_hbm, wout), (wg_hbm, wg), (wu_hbm, wu), (wd_hbm, wd)])
    ]
    for load in loads:
        load.start()

    barrier = pltpu.get_barrier_semaphore()
    pl.semaphore_signal(barrier, inc=1, device_id=partner, device_id_type=MESH)
    for k in range(1, 16):
        pl.semaphore_signal(barrier, inc=1, device_id=dev(k), device_id_type=MESH)
        pl.semaphore_signal(
            barrier, inc=1, device_id=(grp, peer_of(x, y, k), other), device_id_type=MESH
        )
    for dz in range(1, 4):
        pl.semaphore_signal(barrier, inc=1, device_id=zdev(dz), device_id_type=MESH)

    feats = hid_ref[...].astype(f32)
    normed = (feats * again_ref[...]).astype(bf16)
    squares = jnp.sum(feats * feats, axis=1, keepdims=True)
    wq_load.wait()
    for h in range(2):
        part = jnp.dot(normed, wq[:, h * 512 : h * 512 + 512], preferred_element_type=f32)
        qa1s[:, :, h * 512 : h * 512 + 512] = part.reshape(4, 32, 512)
    qa1s[:, :, 1024:1152] = jnp.broadcast_to(squares, (128, 128)).reshape(4, 32, 128)
    for h in range(2):
        part = jnp.dot(normed, wq[:, 1024 + h * 512 : 1536 + h * 512], preferred_element_type=f32)
        for i in range(16):
            qb1s[i % 4, i // 4, :, h * 512 : h * 512 + 512] = part[8 * i : 8 * i + 8]
    pl.semaphore_wait(barrier, 34)

    for step in (2, 1, 3):
        remote(qa1s.at[lax.rem(x + step, 4)], qa1r.at[step], q_ss.at[0], q_rs.at[0], dev(4 * step))
        remote(qb1s.at[lax.rem(y + step, 4)], qb1r.at[step], q_ss.at[1], q_rs.at[1], dev(step))

    owners = own_ref[...]
    spot = lax.broadcasted_iota(i32, (4, 256), 1)
    group_row = lax.broadcasted_iota(i32, (4, 256), 0)
    mine = jnp.where(owners == grp * 16 + kv, loc_ref[...], 0)
    pick = [jnp.sum(jnp.where(spot // 16 == j, mine, 0)) for j in range(16)]
    from_grp = owners // 16
    rank = jnp.zeros((4, 256), i32)
    for back in range(1, 16):
        earlier = pltpu.roll(from_grp, back, 1) == from_grp
        rank = rank + jnp.where(earlier & (lax.rem(spot, 16) >= back), 1, 0)
    here = spot // 16 == kv
    leaving = here & (from_grp == grp)
    sender = lax.rem(owners, 16)
    onward = [
        [jnp.sum(jnp.where(leaving & (group_row == g) & (rank == r), sender, 0)) for r in range(4)]
        for g in range(4)
    ]
    landed = jnp.where(here & (group_row == grp), from_grp * 4 + rank, 0)
    landing = [jnp.sum(jnp.where(lax.rem(spot, 16) == i, landed, 0)) for i in range(16)]
    del mine
    for j in range(16):
        picks[j] = pick[j]
        picks[32 + j] = landing[j]
    for g in range(4):
        for r in range(4):
            picks[16 + 4 * g + r] = onward[g][r]

    def xy_start(c):
        pool_loads[c].wait()
        xr[c][kv] = pool[c][picks[kv]]
        for k in range(1, 16):
            xs[c][k - 1] = pool[c][picks[peer_of(x, y, k)]]
        for k in ORDER[::-1]:
            remote(xs[c].at[k - 1], xr[c].at[kv], x_ss.at[c], x_rs.at[c], dev(k))

    def z_start(c):
        settle(xs[c], x_rs.at[c])
        for dz in range(4):
            g = lax.rem(grp + dz, 4)
            for r in range(4):
                page = xr[c][picks[16 + g * 4 + r]]
                if dz == 0:
                    zr[c][grp, r] = page
                else:
                    zs[c][dz - 1, r] = page
        for dz in (2, 1, 3):
            remote(zs[c].at[dz - 1], zr[c].at[grp], z_ss.at[c], z_rs.at[c], zdev(dz))

    def finish(c):
        settle(zs[c], z_rs.at[c])
        half, row, tokens = PIECES[c]
        final = (fsk, fsv)[half]
        for i in range(16):
            where = picks[32 + i]
            final[i, row : row + tokens, :] = zr[c][where // 4, lax.rem(where, 4)]
        pltpu.make_async_copy(
            final.at[:, pl.ds(row, tokens), :], cache_hbm.at[:, half, pl.ds(row, tokens), :], out_sem.at[half]
        ).start()

    head_of = lax.broadcasted_iota(i32, (16, 512), 0) // 4
    block_of = lax.broadcasted_iota(i32, (16, 512), 1) // 128
    diag = head_of == block_of
    lanes = lax.broadcasted_iota(i32, (16, 128), 1)

    def page_scores(p, keys, slot, filled):
        place_x, place_y, place_s = slot // 32, lax.rem(slot // 8, 4), lax.rem(slot, 8)
        q = jnp.concatenate([qfa[place_x, place_y, place_s], qfb[place_x, place_y, place_s]], axis=0)
        wide = jnp.where(diag, jnp.concatenate([q, q, q, q], axis=1), 0.0)
        high = wide.astype(bf16)
        left = wide - high.astype(f32)
        mid = left.astype(bf16)
        low = (left - mid.astype(f32)).astype(bf16)
        rows = jnp.concatenate([high, mid, low], axis=0)
        s = lax.dot_general(rows, keys, (((1,), (1,)), ((), ())), preferred_element_type=f32)
        s = s[:16] + s[16:32] + s[32:]
        s = jnp.where(lanes < filled, s, neg_fill)
        scores[p] = s
        top = jnp.max(s, axis=1, keepdims=True)
        total = jnp.sum(jnp.where(lanes < filled, jnp.exp(s - top), 0.0), axis=1, keepdims=True)
        return top, total

    def weighted(p, values, lo, hi):
        w = probs[p][:, lo:hi]
        high = w.astype(bf16)
        low = (w - high.astype(f32)).astype(bf16)
        out = jnp.dot(jnp.concatenate([high, low], axis=0), values, preferred_element_type=f32)
        return out[:16] + out[16:]

    def place(p, acc):
        for h in range(16):
            accs[h, p : p + 1, :] = acc[h : h + 1, (h // 4) * 128 : (h // 4) * 128 + 128]

    lane32 = lax.broadcasted_iota(i32, (32, 128), 1)

    def note(table, p, top, total):
        return jnp.where(lane32 == p, jnp.concatenate([top, total], axis=0), table)

    def query_second():
        settle(qa1r.at[pl.ds(1, 3)], q_rs.at[0])
        qa2s[...] = (qa1s[x] + qa1r[1] + qa1r[2] + qa1r[3]).reshape(4, 8, 1152)
        settle(qb1r.at[pl.ds(1, 3)], q_rs.at[1])
        qb2s[...] = qb1s[y] + qb1r[1] + qb1r[2] + qb1r[3]
        for step in (2, 1, 3):
            remote(qa2s.at[lax.rem(y + step, 4)], qa2r.at[step], q_ss.at[2], q_rs.at[2], dev(step))
            remote(qb2s.at[lax.rem(x + step, 4)], qb2r.at[step], q_ss.at[3], q_rs.at[3], dev(4 * step))

    def query_done():
        settle(qa2r.at[pl.ds(1, 3)], q_rs.at[2])
        first = qa2s[y] + qa2r[1] + qa2r[2] + qa2r[3]
        settle(qb2r.at[pl.ds(1, 3)], q_rs.at[3])
        second = qb2s[x] + qb2r[1] + qb2r[2] + qb2r[3]
        scale = lax.rsqrt(first[:, 1024:1025] / D + norm_eps)
        q8 = jnp.concatenate([first[:, :1024], second], axis=1) * scale * HEAD_DIM ** (-0.5)
        qflat[...] = q8
        for h in range(8):
            qfa[x, y, :, h, :] = q8[:, h * 128 : h * 128 + 128]
            qfb[x, y, :, h, :] = q8[:, 1024 + h * 128 : 1152 + h * 128]
        for step in (2, 1, 3):
            remote(qfa.at[x, y], qfa.at[x, y], a_ss.at[0], a_rs.at[0], dev(4 * step))
            remote(qfb.at[x, y], qfb.at[x, y], a_ss.at[1], a_rs.at[1], dev(step))

    def query_spread():
        settle(qfa.at[pl.ds(0, 3), 0], a_rs.at[0])
        settle(qfb.at[pl.ds(0, 3), 0], a_rs.at[1])
        for step in (2, 1, 3):
            remote(qfa.at[:, y], qfa.at[:, y], a_ss.at[2], a_rs.at[2], dev(step))
            remote(qfb.at[x], qfb.at[x], a_ss.at[3], a_rs.at[3], dev(4 * step))

    xy_start(0)
    query_second()
    loads[0].wait()
    for j in range(16):
        cols = pl.ds(pl.multiple_of(j * 256 + other * 128, 128), 128)
        remote(wout.at[:, cols], wpart.at[j], wp_ss.at[0], wp_rs.at[0], partner)
    xy_start(1)
    xy_start(2)
    z_start(0)
    query_done()
    xy_start(3)
    z_start(1)
    finish(0)
    query_spread()
    xy_start(4)
    z_start(2)
    finish(1)
    xy_start(5)
    z_start(3)
    finish(2)
    xy_start(6)
    tok_load.wait()
    own_key, own_value = tok[:, 0, :].astype(f32), tok[:, 1, :].astype(f32)
    lane8 = lax.broadcasted_iota(i32, (8, 128), 1)
    own_rows = jnp.zeros((8, 128), f32)
    for h in range(16):
        s = jnp.sum(
            qflat[:, h * 128 : h * 128 + 128] * own_key[:, (h // 4) * 128 : (h // 4) * 128 + 128],
            axis=1, keepdims=True,
        )
        own_rows = jnp.where(lane8 == h, s, own_rows)
    own_tops = jnp.concatenate([jnp.zeros((24, 128), f32), own_rows, jnp.zeros((96, 128), f32)], axis=0).T[:16]
    slot_row = jnp.zeros((8, 128), i32)
    for p in range(24):
        slot_row = jnp.where(lane8 == p, res_slot[0, p] if p < 8 else arr_slot[0, p - 8], slot_row)
    slot_row = jnp.where(lane8 >= 24, kv * 8 + lane8 - 24, slot_row)
    settle(qfa.at[:, pl.ds(0, 3)], a_rs.at[2])
    settle(qfb.at[pl.ds(0, 3)], a_rs.at[3])
    kept_load.wait()
    table = jnp.zeros((32, 128), f32)
    for p in range(8):
        table = note(table, p, *page_scores(p, kept[p, 0], res_slot[0, p], res_len[0, p]))
    z_start(4)
    finish(3)
    xy_start(7)
    xy_start(8)
    for p in range(16):
        table = note(table, 8 + p, *page_scores(8 + p, fsk[p], arr_slot[0, p], arr_len[0, p]))
    own_lane = lanes >= 24
    mine = jnp.concatenate(
        [
            jnp.where(own_lane, own_tops, table[:16]),
            jnp.where(own_lane, 1.0, table[16:]),
            slot_row.astype(f32),
        ],
        axis=0,
    )
    mine = jnp.where(lax.broadcasted_iota(i32, (40, 128), 1) < 32, mine, 0.0)
    turned = [mine] + [pltpu.roll(mine, 32 * q, 1) for q in range(1, 4)]
    for q in range(1, 4):
        mine = jnp.where(y == q, turned[q], mine)
    stats[kv] = mine
    for k in ORDER[::-1]:
        remote(stats.at[kv], stats.at[kv], s_ss.at[0], s_rs.at[0], dev(k))
    z_start(5)
    finish(4)
    z_start(6)
    finish(5)
    z_start(7)
    z_start(8)
    settle(stats.at[pl.ds(0, 15)], s_rs.at[0])
    every = jnp.concatenate(
        [stats[4 * i] + stats[4 * i + 1] + stats[4 * i + 2] + stats[4 * i + 3] for i in range(4)], axis=1
    )
    tops, sums, every_slot = every[:16], every[16:32], every[32:33].astype(i32)
    own_w = jnp.zeros((16, 128), f32)
    for p in range(32):
        slot = res_slot[0, p] if p < 8 else (arr_slot[0, p - 8] if p < 24 else kv * 8 + p - 24)
        same = jnp.broadcast_to(every_slot == slot, (16, 512))
        top = jnp.max(jnp.where(same, tops, neg_fill), axis=1, keepdims=True)
        total = jnp.sum(jnp.where(same, jnp.exp(tops - top) * sums, 0.0), axis=1, keepdims=True)
        if p < 24:
            probs[p] = jnp.exp(scores[p] - top) * (1.0 / total)
        else:
            own_w = jnp.where(lanes == p, jnp.exp(own_tops - top) * (1.0 / total), own_w)
    own_weight = jnp.concatenate([own_w, jnp.zeros((112, 128), f32)], axis=0).T[24:32]
    for h in range(16):
        g = (h // 4) * 128
        accs[h, 24:32, :] = own_weight[:, h : h + 1] * own_value[:, g : g + 128]
    rho = lax.broadcasted_iota(i32, (128, 512), 0)
    member = (lax.rem(rho, 64) // 4) * 8 + (rho // 64) * 4 + lax.rem(rho, 4) == every_slot
    member = jnp.where(member, 1.0, 0.0).astype(bf16)
    for p in range(8):
        place(p, weighted(p, kept[p, 1], 0, 128))

    def gather_values(c):
        _, row, tokens = PIECES[c]
        for p in range(16):
            part = weighted(8 + p, fsv[p, row : row + tokens, :], row, row + tokens)
            if row == 0:
                pvacc[p] = part
            else:
                pvacc[p] = pvacc[p] + part

    gather_values(4)
    gather_values(5)
    finish(6)
    gather_values(6)
    finish(7)
    gather_values(7)
    finish(8)
    _, row, tokens = PIECES[8]
    for p in range(16):
        place(8 + p, pvacc[p] + weighted(8 + p, fsv[p, row : row + tokens, :], row, row + tokens))

    tiles = [accs[h] for h in range(16)]
    group = lane32 // 8
    for bit in (1, 2, 4, 8):
        upper = (group & bit) != 0
        for h in range(16):
            if h & bit == 0:
                a, b = tiles[h], tiles[h + bit]
                tiles[h] = jnp.where(upper, pltpu.roll(b, 8 * bit, 1), a)
                tiles[h + bit] = jnp.where(upper, b, pltpu.roll(a, 128 - 8 * bit, 1))
    for j in range(16):
        msend[j] = tiles[j].astype(bf16)
    for k in ORDER[::-1]:
        piece = msend.at[peer_of(x, y, k)]
        remote(piece, mrecv.at[tp, kv], m_ss.at[0], m_rs.at[0], dev(k))
        remote(piece, mrecv.at[tp, kv], m_ss.at[1], m_rs.at[1], (grp, peer_of(x, y, k), other))
    remote(msend.at[kv], mrecv.at[tp, kv], m_ss.at[1], m_rs.at[1], partner)
    mrecv[tp, kv] = msend[kv]

    rho = lax.broadcasted_iota(jnp.int32, (128, 128), 0)
    col = lax.broadcasted_iota(jnp.int32, (128, 128), 1)
    slot = (lax.rem(rho, 64) // 4) * 8 + (rho // 64) * 4 + lax.rem(rho, 4)
    perm = jnp.where(col == slot, 1.0, 0.0).astype(bf16)
    block = jnp.dot(
        perm, hid_ref[:, pl.ds(pl.multiple_of(tp * 128, 128), 128)], preferred_element_type=f32
    )
    settle(wpart, wp_rs.at[0])
    settle(msend.at[pl.ds(0, 15)], m_rs.at[0])
    near = jnp.dot(member, mrecv[tp].reshape(512, 128), preferred_element_type=f32).astype(bf16)
    settle(msend, m_rs.at[1])
    far = jnp.dot(member, mrecv[other].reshape(512, 128), preferred_element_type=f32).astype(bf16)
    for k in ORDER[::-1] + [0]:
        dest = peer_of(x, y, k)
        cols = pl.ds(pl.multiple_of(dest * 256 + tp * 128, 128), 128)
        total = jnp.dot(near, wout[:, cols], preferred_element_type=f32)
        total = total + jnp.dot(far, wpart[dest], preferred_element_type=f32)
        if k == 0:
            block = block + total
        else:
            rs_send[k] = total.astype(bf16)
            remote(rs_send.at[k], rs_recv.at[k], rs_ss.at[0], rs_rs.at[0], dev(k))
    settle(rs_recv.at[pl.ds(1, 15)], rs_rs.at[0])
    for k in ORDER:
        block = block + rs_recv[k].astype(f32)
    ag[0, tp] = block.astype(bf16)

    def forward(k):
        remote(ag.at[k, tp], ag.at[k, tp], fw_ss.at[0], fw_rs.at[k], partner)

    forward(0)
    for k in ORDER:
        remote(ag.at[0, tp], ag.at[k, tp], ag_ss.at[0], ag_rs.at[k], dev(k))
    loads[1].wait()
    loads[2].wait()
    seq = [0] + ORDER
    nt = (((1,), (1,)), ((), ()))
    gate = jnp.zeros((128, 448), f32)
    upward = jnp.zeros((128, 448), f32)
    squares = jnp.zeros((128, 128), f32)
    mine = lax.broadcasted_iota(jnp.int32, (8, 128), 0) + tp * 64 + kv * 4
    pick = jnp.where(lax.broadcasted_iota(jnp.int32, (8, 128), 1) == mine, 1.0, 0.0).astype(bf16)
    for n, k in enumerate(seq):
        for later in seq[n + 1 : n + 4] if n == 0 else seq[n + 3 : n + 4]:
            settle(ag.at[later, tp], ag_rs.at[later])
            forward(later)
        settle(ag.at[k, other], fw_rs.at[k])
        src = source_of(x, y, k)
        both = jnp.concatenate([ag[k, 0], ag[k, 1]], axis=1)
        wide = both.astype(f32)
        squares = squares + wide[:, :128] * wide[:, :128] + wide[:, 128:] * wide[:, 128:]
        rows = pl.ds(pl.multiple_of(src * 256, 256), 256)
        normed = (wide * gain_ref[:, rows]).astype(bf16)
        gate = gate + lax.dot_general(normed, wg[:, rows], nt, preferred_element_type=f32)
        upward = upward + lax.dot_general(normed, wu[:, rows], nt, preferred_element_type=f32)
    scale = lax.rsqrt(jnp.sum(squares, axis=1, keepdims=True) / D + norm_eps)
    gate = gate * scale
    upward = upward * scale
    hunits[...] = (gate / (1.0 + jnp.exp(-gate)) * upward).astype(bf16)

    loads[3].wait()
    for c in range(4):
        cols = pl.ds(c * 1024, 1024)
        part = jnp.dot(hunits[...], wd[:, cols], preferred_element_type=f32)
        first, second = part[:64], part[64:]
        dsum[:, cols] = jnp.where(tp == 0, first, second)
        dp_send[c] = jnp.where(tp == 0, second, first).astype(bf16)
        remote(dp_send.at[c], dp_recv.at[c], dp_ss.at[0], dp_rs.at[c], partner)
    for c in range(4):
        settle(dp_recv.at[c], dp_rs.at[c])
        cols = pl.ds(c * 1024, 1024)
        dsum[:, cols] = dsum[:, cols] + dp_recv[c].astype(f32)
    for j in range(16):
        d_send[j] = dsum[4 * j : 4 * j + 4, :].astype(bf16)
    for k in ORDER[::-1]:
        remote(d_send.at[peer_of(x, y, k)], d_recv.at[k], d_ss.at[0], d_rs.at[0], dev(k))
    for c in range(nc):
        settle(xs[c], x_ss.at[c])
        settle(zs[c], z_ss.at[c])
    settle(qa1s.at[pl.ds(0, 3)], q_ss.at[0])
    settle(qb1s.at[pl.ds(0, 3)], q_ss.at[1])
    settle(qa2s.at[pl.ds(0, 3)], q_ss.at[2])
    settle(qb2s.at[pl.ds(0, 3)], q_ss.at[3])
    settle(qfa.at[pl.ds(0, 3), 0], a_ss.at[0])
    settle(qfb.at[pl.ds(0, 3), 0], a_ss.at[1])
    settle(qfa.at[:, pl.ds(0, 3)], a_ss.at[2])
    settle(qfb.at[pl.ds(0, 3)], a_ss.at[3])
    settle(stats.at[pl.ds(0, 15)], s_ss.at[0])
    settle(msend.at[pl.ds(0, 15)], m_ss.at[0])
    settle(wpart, wp_ss.at[0])
    settle(msend, m_ss.at[1])
    settle(rs_send.at[pl.ds(1, 15)], rs_ss.at[0])
    settle(rs_send.at[pl.ds(1, 15)], ag_ss.at[0])
    settle(rs_send, fw_ss.at[0])
    settle(dp_send, dp_ss.at[0])
    settle(fsk, out_sem.at[0])
    settle(fsv, out_sem.at[1])
    for k in range(16):
        for t in range(2):
            cols = pl.ds(pl.multiple_of((source_of(x, y, k) * 2 + t) * 128, 128), 128)
            resrow[:, cols] = jnp.dot(pick, ag[k, t], preferred_element_type=f32)
    total = resrow[...][:4]
    own = jnp.zeros((4, 4096), f32)
    for j in range(16):
        own = jnp.where(kv == j, dsum[4 * j : 4 * j + 4, :], own)
    total = total + own
    settle(d_recv.at[pl.ds(1, 15)], d_rs.at[0])
    for k in ORDER:
        total = total + d_recv[k].astype(f32)
    out_ref[...] = total.astype(bf16)
    settle(d_send.at[pl.ds(0, 15)], d_ss.at[0])


def step(*operands):
    bf16, f32 = jnp.bfloat16, jnp.float32
    smem = pl.BlockSpec(memory_space=pltpu.SMEM)
    vmem = pl.BlockSpec(memory_space=pltpu.VMEM)
    hbm = pl.BlockSpec(memory_space=pl.ANY)
    dma = pltpu.SemaphoreType.DMA
    nc = len(PIECES)

    def chunk(*lead):
        return [pltpu.VMEM((*lead, tokens, 512), bf16) for _, _, tokens in PIECES]

    return pl.pallas_call(
        step_kernel,
        name="step",
        out_shape=(
            jax.ShapeDtypeStruct((4, 4096), bf16),
            jax.ShapeDtypeStruct((16, 2, 128, 512), bf16),
        ),
        in_specs=[smem] * 4 + [vmem] * 5 + [hbm] * 8,
        out_specs=(vmem, hbm),
        scratch_shapes=[
            pltpu.VMEM((256, 2048), bf16),
            pltpu.VMEM((8, 2, 512), bf16),
            pltpu.VMEM((8, 2, 128, 512), bf16),
            pltpu.VMEM((4, 32, 1152), f32),
            pltpu.VMEM((4, 32, 1152), f32),
            pltpu.VMEM((4, 8, 1152), f32),
            pltpu.VMEM((4, 8, 1152), f32),
            pltpu.VMEM((4, 4, 8, 1024), f32),
            pltpu.VMEM((4, 4, 8, 1024), f32),
            pltpu.VMEM((4, 8, 1024), f32),
            pltpu.VMEM((4, 8, 1024), f32),
            pltpu.VMEM((4, 4, 8, 8, 128), f32),
            pltpu.VMEM((4, 4, 8, 8, 128), f32),
            pltpu.VMEM((8, 2048), f32),
            pltpu.VMEM((16, 128, 512), bf16),
            pltpu.VMEM((16, 128, 512), bf16),
            pltpu.VMEM((24, 16, 128), f32),
            pltpu.VMEM((24, 16, 128), f32),
            pltpu.VMEM((16, 16, 512), f32),
            pltpu.VMEM((16, 32, 128), f32),
            pltpu.VMEM((16, 40, 128), f32),
            pltpu.VMEM((16, 32, 128), bf16),
            pltpu.VMEM((2, 16, 32, 128), bf16),
            pltpu.VMEM((128, 4096), bf16),
            pltpu.VMEM((16, 128, 128), bf16),
            pltpu.VMEM((448, 4096), bf16),
            pltpu.VMEM((448, 4096), bf16),
            pltpu.VMEM((448, 4096), bf16),
            pltpu.VMEM((16, 128, 128), bf16),
            pltpu.VMEM((16, 128, 128), bf16),
            pltpu.VMEM((16, 2, 128, 128), bf16),
            pltpu.VMEM((128, 448), bf16),
            pltpu.VMEM((4, 64, 1024), bf16),
            pltpu.VMEM((4, 64, 1024), bf16),
            pltpu.VMEM((64, 4096), f32),
            pltpu.VMEM((16, 4, 4096), bf16),
            pltpu.VMEM((16, 4, 4096), bf16),
            pltpu.VMEM((8, 4096), f32),
            pltpu.SMEM((48,), jnp.int32),
            *chunk(16), *chunk(15), *chunk(16), *chunk(3, 4), *chunk(4, 4),
            dma((2,)), dma((nc,)), dma((1,)), dma((2,)),
            dma((4,)), dma((4,)), dma((4,)), dma((4,)),
            dma((nc,)), dma((nc,)), dma((nc,)), dma((nc,)),
            dma((1,)), dma((1,)), dma((2,)), dma((2,)),
            dma((4,)), dma((1,)), dma((1,)), dma((1,)), dma((1,)), dma((1,)), dma((16,)),
            dma((1,)), dma((16,)), dma((1,)), dma((4,)), dma((1,)), dma((1,)),
        ],
        compiler_params=pltpu.CompilerParams(
            collective_id=0, has_side_effects=True, vmem_limit_bytes=62 * 1024 * 1024
        ),
    )(*operands)


def deliver_kernel(mixed_ref, cache_hbm, out_ref, final_hbm, pages, in_sem, out_sem):
    loads = [pltpu.make_async_copy(cache_hbm.at[i], pages.at[i], in_sem.at[i]) for i in range(16)]
    stores = [pltpu.make_async_copy(pages.at[i], final_hbm.at[i], out_sem.at[i]) for i in range(16)]
    for load in loads:
        load.start()
    out_ref[...] = mixed_ref[...]
    for load, store in zip(loads, stores):
        load.wait()
        store.start()
    for store in stores:
        store.wait()


def deliver(mixed, cache):
    vmem = pl.BlockSpec(memory_space=pltpu.VMEM)
    hbm = pl.BlockSpec(memory_space=pl.ANY)
    dma = pltpu.SemaphoreType.DMA
    return pl.pallas_call(
        deliver_kernel,
        name="deliver",
        out_shape=(
            jax.ShapeDtypeStruct(mixed.shape, mixed.dtype),
            jax.ShapeDtypeStruct(cache.shape, cache.dtype),
        ),
        in_specs=[vmem, hbm],
        out_specs=(vmem, hbm),
        scratch_shapes=[pltpu.VMEM(cache.shape, cache.dtype), dma((16,)), dma((16,))],
        compiler_params=pltpu.CompilerParams(vmem_limit_bytes=62 * 1024 * 1024),
    )(mixed, cache)


def per_device(
    hidden_states,
    attn_gain,
    mlp_gain,
    w_query,
    w_out,
    w_gate,
    w_up,
    w_down,
    kv_pool,
    resident_cache,
    resident_slot,
    resident_len,
    new_owner,
    new_local,
    new_slot,
    new_len,
    token_kv,
):
    mixed, new_pages = step(
        resident_slot,
        resident_len,
        new_slot,
        new_len,
        new_owner,
        new_local,
        hidden_states,
        attn_gain.reshape(1, 256),
        mlp_gain.reshape(1, 4096),
        token_kv,
        w_query,
        kv_pool.reshape(16, 256, 512),
        resident_cache[0],
        w_out.reshape(128, 4096),
        w_gate.T,
        w_up.T,
        w_down,
    )
    mixed, new_pages = deliver(mixed, new_pages)
    return (mixed, new_pages[None])


def solution(mesh):
    return jax.shard_map(
        per_device,
        mesh=mesh,
        in_specs=(
            P("grp", "kv"),
            P("kv"),
            P(),
            P("kv", "tp"),
            P("tp", "kv", None),
            P(None, KV_TP),
            P(None, KV_TP),
            P(KV_TP, None),
            P(GRP_KV, None, None, "tp"),
            P("grp", "kv", None, None, "tp"),
            P("grp", "kv"),
            P("grp", "kv"),
            P(),
            P(),
            P("grp", "kv"),
            P("grp", "kv"),
            P("grp", None, "tp"),
        ),
        out_specs=(P(GRP_KV_TP, None), P("grp", "kv", None, None, "tp")),
        check_vma=False,
    )
```

```python
import jax
import jax.numpy as jnp
from jax import lax
from jax.experimental import pallas as pl
from jax.experimental.pallas import tpu as pltpu
from jax.sharding import PartitionSpec as P

D = 4096
HEADS = 32
KV_HEADS = 8
HEAD_DIM = 128
KV_TP = ("kv", "tp")
GRP_KV = ("grp", "kv")
GRP_KV_TP = ("grp", "kv", "tp")


neg_fill = -1e30
norm_eps = 1e-05
MESH = pl.DeviceIdType.MESH


def peer_of(x, y, k):
    return lax.rem(x + k // 4, 4) * 4 + lax.rem(y + k % 4, 4)


def source_of(x, y, k):
    return lax.rem(x + 4 - k // 4, 4) * 4 + lax.rem(y + 4 - k % 4, 4)


ORDER = sorted(range(1, 16), key=lambda k: (min(k // 4, 4 - k // 4) + min(k % 4, 4 - k % 4), k))


PIECES = [(0, 0, 32), (0, 32, 32), (0, 64, 32), (0, 96, 16), (0, 112, 16)]
PIECES += [(1, 16 * i, 16) for i in range(8)]


def step_kernel(
    res_slot, res_len, arr_slot, arr_len, own_ref, loc_ref, hid_ref, again_ref, gain_ref, tok_hbm, wq_hbm, pool_hbm, res_hbm, wout_hbm, wg_hbm, wu_hbm, wd_hbm,
    out_ref, cache_hbm,
    wq, tok, kept, qa1s, qa1r, qa2s, qa2r, qb1s, qb1r, qb2s, qb2r, qfa, qfb, qflat, fsk, fsv, scores, probs, pvacc, accs, eaccs, stats, msend, esend, mrecv,
    w2, wg, wu, wd, rs_send, rs_recv, ag, hunits,
    dp_send, dp_recv, dsum, d_send, d_recv, resrow, picks, *rest,
):
    f32, bf16, i32 = jnp.float32, jnp.bfloat16, jnp.int32
    nc = len(PIECES)
    pool, xs, xr, zs, zr = (rest[i * nc : (i + 1) * nc] for i in range(5))
    (ld_sem, pool_sem, kept_sem, out_sem, q_ss, q_rs, a_ss, a_rs, x_ss, x_rs, z_ss, z_rs, s_ss, s_rs,
     m_ss, m_rs, w_sem, wp_ss, wp_rs, rs_ss, rs_rs, ag_ss, ag_rs, fw_ss, fw_rs, dp_ss, dp_rs, d_ss,
     d_rs) = rest[5 * nc :]
    grp, kv, tp = lax.axis_index("grp"), lax.axis_index("kv"), lax.axis_index("tp")
    x, y = kv // 4, lax.rem(kv, 4)
    other = 1 - tp
    partner = (grp, kv, other)

    def dev(k):
        return (grp, peer_of(x, y, k), tp)

    def zdev(dz):
        return (lax.rem(grp + dz, 4), kv, tp)

    def remote(src, dst, send, recv, device):
        copy = pltpu.make_async_remote_copy(
            src_ref=src, dst_ref=dst, send_sem=send, recv_sem=recv, device_id=device,
            device_id_type=MESH,
        )
        copy.start()
        return copy

    def settle(ref, sem):
        pltpu.make_async_copy(ref, ref, sem).wait()

    wq_load = pltpu.make_async_copy(wq_hbm, wq, ld_sem.at[0])
    wq_load.start()
    pool_loads = []
    for c in range(nc):
        load = pltpu.make_async_copy(pool_hbm.at[:, pl.ds(PIECES[c][0] * 128 + PIECES[c][1], PIECES[c][2]), :], pool[c], pool_sem.at[c])
        load.start()
        pool_loads.append(load)
    kept_load = pltpu.make_async_copy(res_hbm, kept, kept_sem.at[0])
    kept_load.start()
    tok_load = pltpu.make_async_copy(
        tok_hbm.at[pl.ds(pl.multiple_of(kv * 8, 8), 8)], tok, ld_sem.at[1]
    )
    tok_load.start()

    loads = [
        pltpu.make_async_copy(src, dst, w_sem.at[i])
        for i, (src, dst) in enumerate([(wg_hbm, wg), (wu_hbm, wu), (wd_hbm, wd)])
    ]
    for load in loads:
        load.start()

    barrier = pltpu.get_barrier_semaphore()
    pl.semaphore_signal(barrier, inc=1, device_id=partner, device_id_type=MESH)
    for k in range(1, 16):
        pl.semaphore_signal(barrier, inc=1, device_id=dev(k), device_id_type=MESH)
        pl.semaphore_signal(
            barrier, inc=1, device_id=(grp, peer_of(x, y, k), other), device_id_type=MESH
        )
    for dz in range(1, 4):
        pl.semaphore_signal(barrier, inc=1, device_id=zdev(dz), device_id_type=MESH)

    feats = hid_ref[...].astype(f32)
    normed = (feats * again_ref[...]).astype(bf16)
    squares = jnp.sum(feats * feats, axis=1, keepdims=True)
    wq_load.wait()
    for h in range(2):
        part = jnp.dot(normed, wq[:, h * 512 : h * 512 + 512], preferred_element_type=f32)
        qa1s[:, :, h * 512 : h * 512 + 512] = part.reshape(4, 32, 512)
    qa1s[:, :, 1024:1152] = jnp.broadcast_to(squares, (128, 128)).reshape(4, 32, 128)
    for h in range(2):
        part = jnp.dot(normed, wq[:, 1024 + h * 512 : 1536 + h * 512], preferred_element_type=f32)
        for i in range(16):
            qb1s[i % 4, i // 4, :, h * 512 : h * 512 + 512] = part[8 * i : 8 * i + 8]
    pl.semaphore_wait(barrier, 34)

    for step in (2, 1, 3):
        remote(qa1s.at[lax.rem(x + step, 4)], qa1r.at[step], q_ss.at[0], q_rs.at[0], dev(4 * step))
        remote(qb1s.at[lax.rem(y + step, 4)], qb1r.at[step], q_ss.at[1], q_rs.at[1], dev(step))

    owners = own_ref[...]
    spot = lax.broadcasted_iota(i32, (4, 256), 1)
    group_row = lax.broadcasted_iota(i32, (4, 256), 0)
    mine = jnp.where(owners == grp * 16 + kv, loc_ref[...], 0)
    pick = [jnp.sum(jnp.where(spot // 16 == j, mine, 0)) for j in range(16)]
    from_grp = owners // 16
    rank = jnp.zeros((4, 256), i32)
    for back in range(1, 16):
        earlier = pltpu.roll(from_grp, back, 1) == from_grp
        rank = rank + jnp.where(earlier & (lax.rem(spot, 16) >= back), 1, 0)
    here = spot // 16 == kv
    leaving = here & (from_grp == grp)
    sender = lax.rem(owners, 16)
    onward = [
        [jnp.sum(jnp.where(leaving & (group_row == g) & (rank == r), sender, 0)) for r in range(4)]
        for g in range(4)
    ]
    landed = jnp.where(here & (group_row == grp), from_grp * 4 + rank, 0)
    landing = [jnp.sum(jnp.where(lax.rem(spot, 16) == i, landed, 0)) for i in range(16)]
    del mine
    for j in range(16):
        picks[j] = pick[j]
        picks[32 + j] = landing[j]
    for g in range(4):
        for r in range(4):
            picks[16 + 4 * g + r] = onward[g][r]

    def xy_start(c):
        pool_loads[c].wait()
        xr[c][kv] = pool[c][picks[kv]]
        for k in range(1, 16):
            xs[c][k - 1] = pool[c][picks[peer_of(x, y, k)]]
        for k in ORDER[::-1]:
            remote(xs[c].at[k - 1], xr[c].at[kv], x_ss.at[c], x_rs.at[c], dev(k))

    def z_start(c):
        settle(xs[c], x_rs.at[c])
        for dz in range(4):
            g = lax.rem(grp + dz, 4)
            for r in range(4):
                page = xr[c][picks[16 + g * 4 + r]]
                if dz == 0:
                    zr[c][grp, r] = page
                else:
                    zs[c][dz - 1, r] = page
        for dz in (2, 1, 3):
            remote(zs[c].at[dz - 1], zr[c].at[grp], z_ss.at[c], z_rs.at[c], zdev(dz))

    def finish(c):
        settle(zs[c], z_rs.at[c])
        half, row, tokens = PIECES[c]
        final = (fsk, fsv)[half]
        for i in range(16):
            where = picks[32 + i]
            final[i, row : row + tokens, :] = zr[c][where // 4, lax.rem(where, 4)]
        pltpu.make_async_copy(
            final.at[:, pl.ds(row, tokens), :], cache_hbm.at[:, half, pl.ds(row, tokens), :], out_sem.at[half]
        ).start()

    head_of = lax.broadcasted_iota(i32, (16, 512), 0) // 4
    block_of = lax.broadcasted_iota(i32, (16, 512), 1) // 128
    diag = head_of == block_of
    lanes = lax.broadcasted_iota(i32, (16, 128), 1)

    def page_scores(p, keys, slot, filled):
        place_x, place_y, place_s = slot // 32, lax.rem(slot // 8, 4), lax.rem(slot, 8)
        q = jnp.concatenate([qfa[place_x, place_y, place_s], qfb[place_x, place_y, place_s]], axis=0)
        wide = jnp.where(diag, jnp.concatenate([q, q, q, q], axis=1), 0.0)
        high = wide.astype(bf16)
        left = wide - high.astype(f32)
        mid = left.astype(bf16)
        low = (left - mid.astype(f32)).astype(bf16)
        rows = jnp.concatenate([high, mid, low], axis=0)
        s = lax.dot_general(rows, keys, (((1,), (1,)), ((), ())), preferred_element_type=f32)
        s = s[:16] + s[16:32] + s[32:]
        s = jnp.where(lanes < filled, s, neg_fill)
        scores[p] = s
        top = jnp.max(s, axis=1, keepdims=True)
        total = jnp.sum(jnp.where(lanes < filled, jnp.exp(s - top), 0.0), axis=1, keepdims=True)
        return top, total

    def weighted(p, values, lo, hi):
        w = probs[p][:, lo:hi]
        high = w.astype(bf16)
        low = (w - high.astype(f32)).astype(bf16)
        out = jnp.dot(jnp.concatenate([high, low], axis=0), values, preferred_element_type=f32)
        return out[:16] + out[16:]

    def place(accs, p, acc):
        for h in range(16):
            accs[h, p : p + 1, :] = acc[h : h + 1, (h // 4) * 128 : (h // 4) * 128 + 128]

    lane32 = lax.broadcasted_iota(i32, (32, 128), 1)

    def note(table, p, top, total):
        return jnp.where(lane32 == p, jnp.concatenate([top, total], axis=0), table)

    def query_second():
        settle(qa1r.at[pl.ds(1, 3)], q_rs.at[0])
        qa2s[...] = (qa1s[x] + qa1r[1] + qa1r[2] + qa1r[3]).reshape(4, 8, 1152)
        settle(qb1r.at[pl.ds(1, 3)], q_rs.at[1])
        qb2s[...] = qb1s[y] + qb1r[1] + qb1r[2] + qb1r[3]
        for step in (2, 1, 3):
            remote(qa2s.at[lax.rem(y + step, 4)], qa2r.at[step], q_ss.at[2], q_rs.at[2], dev(step))
            remote(qb2s.at[lax.rem(x + step, 4)], qb2r.at[step], q_ss.at[3], q_rs.at[3], dev(4 * step))

    def query_done():
        settle(qa2r.at[pl.ds(1, 3)], q_rs.at[2])
        first = qa2s[y] + qa2r[1] + qa2r[2] + qa2r[3]
        settle(qb2r.at[pl.ds(1, 3)], q_rs.at[3])
        second = qb2s[x] + qb2r[1] + qb2r[2] + qb2r[3]
        scale = lax.rsqrt(first[:, 1024:1025] / D + norm_eps)
        q8 = jnp.concatenate([first[:, :1024], second], axis=1) * scale * HEAD_DIM ** (-0.5)
        qflat[...] = q8
        for h in range(8):
            qfa[x, y, :, h, :] = q8[:, h * 128 : h * 128 + 128]
            qfb[x, y, :, h, :] = q8[:, 1024 + h * 128 : 1152 + h * 128]
        for step in (2, 1, 3):
            remote(qfa.at[x, y], qfa.at[x, y], a_ss.at[0], a_rs.at[0], dev(4 * step))
            remote(qfb.at[x, y], qfb.at[x, y], a_ss.at[1], a_rs.at[1], dev(step))

    def query_spread():
        settle(qfa.at[pl.ds(0, 3), 0], a_rs.at[0])
        settle(qfb.at[pl.ds(0, 3), 0], a_rs.at[1])
        for step in (2, 1, 3):
            remote(qfa.at[:, y], qfa.at[:, y], a_ss.at[2], a_rs.at[2], dev(step))
            remote(qfb.at[x], qfb.at[x], a_ss.at[3], a_rs.at[3], dev(4 * step))

    xy_start(0)
    query_second()
    for j in range(16):
        near_cols = pl.ds(pl.multiple_of(j * 256 + tp * 128, 128), 128)
        far_cols = pl.ds(pl.multiple_of(j * 256 + other * 128, 128), 128)
        here = pl.ds(j * 128, 128)
        pltpu.make_async_copy(wout_hbm.at[:, near_cols], w2.at[pl.ds(0, 128), here], w_sem.at[3]).start()
        remote(wout_hbm.at[:, far_cols], w2.at[pl.ds(128, 128), here], wp_ss.at[0], wp_rs.at[0], partner)
    xy_start(1)
    xy_start(2)
    z_start(0)
    query_done()
    xy_start(3)
    z_start(1)
    query_spread()
    xy_start(4)
    xy_start(5)
    z_start(2)
    finish(0)
    xy_start(6)
    xy_start(7)
    z_start(3)
    finish(1)
    xy_start(8)
    tok_load.wait()
    own_key, own_value = tok[:, 0, :].astype(f32), tok[:, 1, :].astype(f32)
    lane8 = lax.broadcasted_iota(i32, (8, 128), 1)
    own_rows = jnp.zeros((8, 128), f32)
    for h in range(16):
        s = jnp.sum(
            qflat[:, h * 128 : h * 128 + 128] * own_key[:, (h // 4) * 128 : (h // 4) * 128 + 128],
            axis=1, keepdims=True,
        )
        own_rows = jnp.where(lane8 == h, s, own_rows)
    own_tops = jnp.concatenate([jnp.zeros((24, 128), f32), own_rows, jnp.zeros((96, 128), f32)], axis=0).T[:16]
    slot_row = jnp.zeros((8, 128), i32)
    for p in range(24):
        slot_row = jnp.where(lane8 == p, arr_slot[0, p] if p < 16 else res_slot[0, p - 16], slot_row)
    slot_row = jnp.where(lane8 >= 24, kv * 8 + lane8 - 24, slot_row)
    z_start(4)
    finish(2)
    xy_start(9)
    settle(qfa.at[:, pl.ds(0, 3)], a_rs.at[2])
    settle(qfb.at[pl.ds(0, 3)], a_rs.at[3])
    kept_load.wait()
    table = jnp.zeros((32, 128), f32)
    for p in range(8):
        table = note(table, 16 + p, *page_scores(16 + p, kept[p, 0], res_slot[0, p], res_len[0, p]))
    z_start(5)
    finish(3)
    xy_start(10)
    z_start(6)
    finish(4)
    for p in range(16):
        table = note(table, p, *page_scores(p, fsk[p], arr_slot[0, p], arr_len[0, p]))
    own_lane = lanes >= 24
    mine = jnp.concatenate(
        [
            jnp.where(own_lane, own_tops, table[:16]),
            jnp.where(own_lane, 1.0, table[16:]),
            slot_row.astype(f32),
        ],
        axis=0,
    )
    mine = jnp.where(lax.broadcasted_iota(i32, (40, 128), 1) < 32, mine, 0.0)
    turned = [mine] + [pltpu.roll(mine, 32 * q, 1) for q in range(1, 4)]
    for q in range(1, 4):
        mine = jnp.where(y == q, turned[q], mine)
    stats[kv] = mine
    for k in ORDER[::-1]:
        remote(stats.at[kv], stats.at[kv], s_ss.at[0], s_rs.at[0], dev(k))
    xy_start(11)
    xy_start(12)
    for c in range(7, nc):
        z_start(c)
        finish(c - 2)
    settle(stats.at[pl.ds(0, 15)], s_rs.at[0])
    every = jnp.concatenate(
        [stats[4 * i] + stats[4 * i + 1] + stats[4 * i + 2] + stats[4 * i + 3] for i in range(4)], axis=1
    )
    tops, sums, every_slot = every[:16], every[16:32], every[32:33].astype(i32)
    own_w = jnp.zeros((16, 128), f32)
    for p in range(32):
        slot = arr_slot[0, p] if p < 16 else (res_slot[0, p - 16] if p < 24 else kv * 8 + p - 24)
        same = jnp.broadcast_to(every_slot == slot, (16, 512))
        top = jnp.max(jnp.where(same, tops, neg_fill), axis=1, keepdims=True)
        total = jnp.sum(jnp.where(same, jnp.exp(tops - top) * sums, 0.0), axis=1, keepdims=True)
        if p < 24:
            probs[p] = jnp.exp(scores[p] - top) * (1.0 / total)
        else:
            own_w = jnp.where(lanes == p, jnp.exp(own_tops - top) * (1.0 / total), own_w)
    own_weight = jnp.concatenate([own_w, jnp.zeros((112, 128), f32)], axis=0).T[24:32]
    for h in range(16):
        g = (h // 4) * 128
        eaccs[h, 8:16, :] = own_weight[:, h : h + 1] * own_value[:, g : g + 128]
    rho = lax.broadcasted_iota(i32, (128, 512), 0)
    member = (lax.rem(rho, 64) // 4) * 8 + (rho // 64) * 4 + lax.rem(rho, 4) == every_slot
    member = jnp.where(member, 1.0, 0.0).astype(bf16)

    def swap(accs, msend):
        tiles = [accs[h] for h in range(16)]
        group = lanes // 8
        for bit in (1, 2, 4, 8):
            upper = (group & bit) != 0
            for h in range(16):
                if h & bit == 0:
                    a, b = tiles[h], tiles[h + bit]
                    tiles[h] = jnp.where(upper, pltpu.roll(b, 8 * bit, 1), a)
                    tiles[h + bit] = jnp.where(upper, b, pltpu.roll(a, 128 - 8 * bit, 1))
        for j in range(16):
            msend[j] = tiles[j].astype(bf16)

    def spread(msend, row, n):
        rows = pl.ds(row, 16)
        for k in ORDER[::-1]:
            piece = msend.at[peer_of(x, y, k)]
            remote(piece, mrecv.at[tp, kv, rows], m_ss.at[n], m_rs.at[n], dev(k))
            remote(piece, mrecv.at[tp, kv, rows], m_ss.at[n + 1], m_rs.at[n + 1], (grp, peer_of(x, y, k), other))
        remote(msend.at[kv], mrecv.at[tp, kv, rows], m_ss.at[n + 1], m_rs.at[n + 1], partner)
        mrecv[tp, kv, rows, :] = msend[kv]

    for p in range(8):
        place(eaccs, p, weighted(16 + p, kept[p, 1], 0, 128))
    swap(eaccs, esend)
    spread(esend, 16, 2)
    for p in range(16):
        pvacc[p] = weighted(p, fsv[p, :96, :], 0, 96)
    finish(nc - 2)
    finish(nc - 1)
    for p in range(16):
        place(accs, p, pvacc[p] + weighted(p, fsv[p, 96:, :], 96, 128))
    swap(accs, msend)
    spread(msend, 0, 0)

    rho = lax.broadcasted_iota(jnp.int32, (128, 128), 0)
    col = lax.broadcasted_iota(jnp.int32, (128, 128), 1)
    slot = (lax.rem(rho, 64) // 4) * 8 + (rho // 64) * 4 + lax.rem(rho, 4)
    perm = jnp.where(col == slot, 1.0, 0.0).astype(bf16)
    block = jnp.dot(
        perm, hid_ref[:, pl.ds(pl.multiple_of(tp * 128, 128), 128)], preferred_element_type=f32
    )
    settle(w2.at[pl.ds(0, 128)], w_sem.at[3])
    settle(w2.at[pl.ds(128, 128)], wp_rs.at[0])
    settle(esend.at[pl.ds(0, 15)], m_rs.at[2])
    settle(esend, m_rs.at[3])
    settle(msend.at[pl.ds(0, 15)], m_rs.at[0])
    near = jnp.dot(member, mrecv[tp].reshape(512, 128), preferred_element_type=f32).astype(bf16)
    settle(msend, m_rs.at[1])
    far = jnp.dot(member, mrecv[other].reshape(512, 128), preferred_element_type=f32).astype(bf16)
    slices = jnp.concatenate([near, far], axis=1)

    def share(j, part):
        rs_send[j] = part.astype(bf16)
        remote(rs_send.at[j], rs_recv.at[kv], rs_ss.at[0], rs_rs.at[0], (grp, j, tp))

    for dx in (2, 1, 3):
        row = lax.rem(x + dx, 4)
        for half in range(2):
            cols = pl.ds(pl.multiple_of(row * 512 + half * 256, 256), 256)
            part = jnp.dot(slices, w2[:, cols], preferred_element_type=f32)
            share(row * 4 + 2 * half, part[:, :128])
            share(row * 4 + 2 * half + 1, part[:, 128:])
    for dy in (2, 1, 3, 0):
        j = x * 4 + lax.rem(y + dy, 4)
        part = jnp.dot(slices, w2[:, pl.ds(pl.multiple_of(j * 128, 128), 128)], preferred_element_type=f32)
        if dy:
            share(j, part)
        else:
            block = block + part
    settle(rs_recv.at[pl.ds(0, 15)], rs_rs.at[0])
    for k in ORDER:
        block = block + rs_recv[source_of(x, y, k)].astype(f32)
    ag[0, tp] = block.astype(bf16)

    def forward(k):
        remote(ag.at[k, tp], ag.at[k, tp], fw_ss.at[0], fw_rs.at[k], partner)

    forward(0)
    for k in ORDER:
        remote(ag.at[0, tp], ag.at[k, tp], ag_ss.at[0], ag_rs.at[k], dev(k))
    loads[0].wait()
    loads[1].wait()
    seq = [0] + ORDER
    nt = (((1,), (1,)), ((), ()))
    gate = jnp.zeros((128, 448), f32)
    upward = jnp.zeros((128, 448), f32)
    squares = jnp.zeros((128, 128), f32)
    mine = lax.broadcasted_iota(jnp.int32, (8, 128), 0) + tp * 64 + kv * 4
    pick = jnp.where(lax.broadcasted_iota(jnp.int32, (8, 128), 1) == mine, 1.0, 0.0).astype(bf16)
    for n, k in enumerate(seq):
        for later in seq[n + 1 : n + 4] if n == 0 else seq[n + 3 : n + 4]:
            settle(ag.at[later, tp], ag_rs.at[later])
            forward(later)
        settle(ag.at[k, other], fw_rs.at[k])
        src = source_of(x, y, k)
        both = jnp.concatenate([ag[k, 0], ag[k, 1]], axis=1)
        wide = both.astype(f32)
        squares = squares + wide[:, :128] * wide[:, :128] + wide[:, 128:] * wide[:, 128:]
        rows = pl.ds(pl.multiple_of(src * 256, 256), 256)
        normed = (wide * gain_ref[:, rows]).astype(bf16)
        gate = gate + lax.dot_general(normed, wg[:, rows], nt, preferred_element_type=f32)
        upward = upward + lax.dot_general(normed, wu[:, rows], nt, preferred_element_type=f32)
    scale = lax.rsqrt(jnp.sum(squares, axis=1, keepdims=True) / D + norm_eps)
    gate = gate * scale
    upward = upward * scale
    hunits[...] = (gate / (1.0 + jnp.exp(-gate)) * upward).astype(bf16)

    loads[2].wait()
    for c in range(4):
        cols = pl.ds(c * 1024, 1024)
        part = jnp.dot(hunits[...], wd[:, cols], preferred_element_type=f32)
        first, second = part[:64], part[64:]
        dsum[:, cols] = jnp.where(tp == 0, first, second)
        dp_send[c] = jnp.where(tp == 0, second, first).astype(bf16)
        remote(dp_send.at[c], dp_recv.at[c], dp_ss.at[0], dp_rs.at[c], partner)
    for c in range(4):
        settle(dp_recv.at[c], dp_rs.at[c])
        cols = pl.ds(c * 1024, 1024)
        dsum[:, cols] = dsum[:, cols] + dp_recv[c].astype(f32)
    for j in range(16):
        d_send[j] = dsum[4 * j : 4 * j + 4, :].astype(bf16)
    for k in ORDER[::-1]:
        remote(d_send.at[peer_of(x, y, k)], d_recv.at[k], d_ss.at[0], d_rs.at[0], dev(k))
    for c in range(nc):
        settle(xs[c], x_ss.at[c])
        settle(zs[c], z_ss.at[c])
    settle(qa1s.at[pl.ds(0, 3)], q_ss.at[0])
    settle(qb1s.at[pl.ds(0, 3)], q_ss.at[1])
    settle(qa2s.at[pl.ds(0, 3)], q_ss.at[2])
    settle(qb2s.at[pl.ds(0, 3)], q_ss.at[3])
    settle(qfa.at[pl.ds(0, 3), 0], a_ss.at[0])
    settle(qfb.at[pl.ds(0, 3), 0], a_ss.at[1])
    settle(qfa.at[:, pl.ds(0, 3)], a_ss.at[2])
    settle(qfb.at[pl.ds(0, 3)], a_ss.at[3])
    settle(stats.at[pl.ds(0, 15)], s_ss.at[0])
    settle(msend.at[pl.ds(0, 15)], m_ss.at[0])
    settle(w2.at[pl.ds(0, 128)], wp_ss.at[0])
    settle(msend, m_ss.at[1])
    settle(esend.at[pl.ds(0, 15)], m_ss.at[2])
    settle(esend, m_ss.at[3])
    settle(rs_send.at[pl.ds(1, 15)], rs_ss.at[0])
    settle(rs_send.at[pl.ds(1, 15)], ag_ss.at[0])
    settle(rs_send, fw_ss.at[0])
    settle(dp_send, dp_ss.at[0])
    settle(fsk, out_sem.at[0])
    settle(fsv, out_sem.at[1])
    for k in range(16):
        for t in range(2):
            cols = pl.ds(pl.multiple_of((source_of(x, y, k) * 2 + t) * 128, 128), 128)
            resrow[:, cols] = jnp.dot(pick, ag[k, t], preferred_element_type=f32)
    total = resrow[...][:4]
    own = jnp.zeros((4, 4096), f32)
    for j in range(16):
        own = jnp.where(kv == j, dsum[4 * j : 4 * j + 4, :], own)
    total = total + own
    settle(d_recv.at[pl.ds(1, 15)], d_rs.at[0])
    for k in ORDER:
        total = total + d_recv[k].astype(f32)
    out_ref[...] = total.astype(bf16)
    settle(d_send.at[pl.ds(0, 15)], d_ss.at[0])


def step(*operands):
    bf16, f32 = jnp.bfloat16, jnp.float32
    smem = pl.BlockSpec(memory_space=pltpu.SMEM)
    vmem = pl.BlockSpec(memory_space=pltpu.VMEM)
    hbm = pl.BlockSpec(memory_space=pl.ANY)
    dma = pltpu.SemaphoreType.DMA
    nc = len(PIECES)

    def chunk(*lead):
        return [pltpu.VMEM((*lead, tokens, 512), bf16) for _, _, tokens in PIECES]

    return pl.pallas_call(
        step_kernel,
        name="step",
        out_shape=(
            jax.ShapeDtypeStruct((4, 4096), bf16),
            jax.ShapeDtypeStruct((16, 2, 128, 512), bf16),
        ),
        in_specs=[smem] * 4 + [vmem] * 5 + [hbm] * 8,
        out_specs=(vmem, hbm),
        scratch_shapes=[
            pltpu.VMEM((256, 2048), bf16),
            pltpu.VMEM((8, 2, 512), bf16),
            pltpu.VMEM((8, 2, 128, 512), bf16),
            pltpu.VMEM((4, 32, 1152), f32),
            pltpu.VMEM((4, 32, 1152), f32),
            pltpu.VMEM((4, 8, 1152), f32),
            pltpu.VMEM((4, 8, 1152), f32),
            pltpu.VMEM((4, 4, 8, 1024), f32),
            pltpu.VMEM((4, 4, 8, 1024), f32),
            pltpu.VMEM((4, 8, 1024), f32),
            pltpu.VMEM((4, 8, 1024), f32),
            pltpu.VMEM((4, 4, 8, 8, 128), f32),
            pltpu.VMEM((4, 4, 8, 8, 128), f32),
            pltpu.VMEM((8, 2048), f32),
            pltpu.VMEM((16, 128, 512), bf16),
            pltpu.VMEM((16, 128, 512), bf16),
            pltpu.VMEM((24, 16, 128), f32),
            pltpu.VMEM((24, 16, 128), f32),
            pltpu.VMEM((16, 16, 512), f32),
            pltpu.VMEM((16, 16, 128), f32),
            pltpu.VMEM((16, 16, 128), f32),
            pltpu.VMEM((16, 40, 128), f32),
            pltpu.VMEM((16, 16, 128), bf16),
            pltpu.VMEM((16, 16, 128), bf16),
            pltpu.VMEM((2, 16, 32, 128), bf16),
            pltpu.VMEM((256, 2048), bf16),
            pltpu.VMEM((448, 4096), bf16),
            pltpu.VMEM((448, 4096), bf16),
            pltpu.VMEM((448, 4096), bf16),
            pltpu.VMEM((16, 128, 128), bf16),
            pltpu.VMEM((16, 128, 128), bf16),
            pltpu.VMEM((16, 2, 128, 128), bf16),
            pltpu.VMEM((128, 448), bf16),
            pltpu.VMEM((4, 64, 1024), bf16),
            pltpu.VMEM((4, 64, 1024), bf16),
            pltpu.VMEM((64, 4096), f32),
            pltpu.VMEM((16, 4, 4096), bf16),
            pltpu.VMEM((16, 4, 4096), bf16),
            pltpu.VMEM((8, 4096), f32),
            pltpu.SMEM((48,), jnp.int32),
            *chunk(16), *chunk(15), *chunk(16), *chunk(3, 4), *chunk(4, 4),
            dma((2,)), dma((nc,)), dma((1,)), dma((2,)),
            dma((4,)), dma((4,)), dma((4,)), dma((4,)),
            dma((nc,)), dma((nc,)), dma((nc,)), dma((nc,)),
            dma((1,)), dma((1,)), dma((4,)), dma((4,)),
            dma((4,)), dma((1,)), dma((1,)), dma((1,)), dma((1,)), dma((1,)), dma((16,)),
            dma((1,)), dma((16,)), dma((1,)), dma((4,)), dma((1,)), dma((1,)),
        ],
        compiler_params=pltpu.CompilerParams(
            collective_id=0, has_side_effects=True, vmem_limit_bytes=62 * 1024 * 1024
        ),
    )(*operands)


def deliver_kernel(mixed_ref, cache_hbm, out_ref, final_hbm, pages, in_sem, out_sem):
    loads = [pltpu.make_async_copy(cache_hbm.at[i // 2, i % 2], pages.at[i // 2, i % 2], in_sem.at[i]) for i in range(32)]
    stores = [pltpu.make_async_copy(pages.at[i // 2, i % 2], final_hbm.at[i // 2, i % 2], out_sem.at[0]) for i in range(32)]
    for load in loads:
        load.start()
    out_ref[...] = mixed_ref[...]
    for load, store in zip(loads, stores):
        load.wait()
        store.start()
    pltpu.make_async_copy(pages, pages, out_sem.at[0]).wait()


def deliver(mixed, cache):
    vmem = pl.BlockSpec(memory_space=pltpu.VMEM)
    hbm = pl.BlockSpec(memory_space=pl.ANY)
    dma = pltpu.SemaphoreType.DMA
    return pl.pallas_call(
        deliver_kernel,
        name="deliver",
        out_shape=(
            jax.ShapeDtypeStruct(mixed.shape, mixed.dtype),
            jax.ShapeDtypeStruct(cache.shape, cache.dtype),
        ),
        in_specs=[vmem, hbm],
        out_specs=(vmem, hbm),
        scratch_shapes=[pltpu.VMEM(cache.shape, cache.dtype), dma((32,)), dma((1,))],
        compiler_params=pltpu.CompilerParams(vmem_limit_bytes=62 * 1024 * 1024),
    )(mixed, cache)


def per_device(
    hidden_states,
    attn_gain,
    mlp_gain,
    w_query,
    w_out,
    w_gate,
    w_up,
    w_down,
    kv_pool,
    resident_cache,
    resident_slot,
    resident_len,
    new_owner,
    new_local,
    new_slot,
    new_len,
    token_kv,
):
    mixed, new_pages = step(
        resident_slot,
        resident_len,
        new_slot,
        new_len,
        new_owner,
        new_local,
        hidden_states,
        attn_gain.reshape(1, 256),
        mlp_gain.reshape(1, 4096),
        token_kv,
        w_query,
        kv_pool.reshape(16, 256, 512),
        resident_cache[0],
        w_out.reshape(128, 4096),
        w_gate.T,
        w_up.T,
        w_down,
    )
    mixed, new_pages = deliver(mixed, new_pages)
    return (mixed, new_pages[None])


def solution(mesh):
    return jax.shard_map(
        per_device,
        mesh=mesh,
        in_specs=(
            P("grp", "kv"),
            P("kv"),
            P(),
            P("kv", "tp"),
            P("tp", "kv", None),
            P(None, KV_TP),
            P(None, KV_TP),
            P(KV_TP, None),
            P(GRP_KV, None, None, "tp"),
            P("grp", "kv", None, None, "tp"),
            P("grp", "kv"),
            P("grp", "kv"),
            P(),
            P(),
            P("grp", "kv"),
            P("grp", "kv"),
            P("grp", None, "tp"),
        ),
        out_specs=(P(GRP_KV_TP, None), P("grp", "kv", None, None, "tp")),
        check_vma=False,
    )
```

```python
import jax
import jax.numpy as jnp
from jax import lax
from jax.experimental import pallas as pl
from jax.experimental.pallas import tpu as pltpu
from jax.sharding import PartitionSpec as P

D = 4096
HEADS = 32
KV_HEADS = 8
HEAD_DIM = 128
KV_TP = ("kv", "tp")
GRP_KV = ("grp", "kv")
GRP_KV_TP = ("grp", "kv", "tp")


neg_fill = -1e30
norm_eps = 1e-05
MESH = pl.DeviceIdType.MESH


def peer_of(x, y, k):
    return lax.rem(x + k // 4, 4) * 4 + lax.rem(y + k % 4, 4)


def source_of(x, y, k):
    return lax.rem(x + 4 - k // 4, 4) * 4 + lax.rem(y + 4 - k % 4, 4)


ORDER = sorted(range(1, 16), key=lambda k: (min(k // 4, 4 - k // 4) + min(k % 4, 4 - k % 4), k))


PIECES = [(0, 0, 32), (0, 32, 32), (0, 64, 32), (0, 96, 32), (1, 0, 32), (1, 32, 32), (1, 64, 32), (1, 96, 16), (1, 112, 16)]


def step_kernel(
    res_slot, res_len, arr_slot, arr_len, own_ref, loc_ref, hid_ref, again_ref, gain_ref, tok_hbm, wq_hbm, pool_hbm, res_hbm, wout_hbm, wg_hbm, wu_hbm, wd_hbm,
    out_ref, cache_hbm,
    wq, tok, kept, qa1s, qa1r, qa2s, qa2r, qb1s, qb1r, qb2s, qb2r, qfa, qfb, qflat, fsk, fsv, scores, probs, pvacc, accs, eaccs, stats, msend, esend, mrecv,
    w2, wg, wu, wd, rs_send, rs_recv, ag, hunits,
    dp_send, dp_recv, dsum, d_send, d_recv, resrow, picks, *rest,
):
    f32, bf16, i32 = jnp.float32, jnp.bfloat16, jnp.int32
    nc = len(PIECES)
    pool, xs, xr, zs, zr = (rest[i * nc : (i + 1) * nc] for i in range(5))
    (ld_sem, pool_sem, kept_sem, out_sem, q_ss, q_rs, a_ss, a_rs, x_ss, x_rs, z_ss, z_rs, s_ss, s_rs,
     m_ss, m_rs, w_sem, wp_ss, wp_rs, rs_ss, rs_rs, ag_ss, ag_rs, fw_ss, fw_rs, dp_ss, dp_rs, d_ss,
     d_rs) = rest[5 * nc :]
    grp, kv, tp = lax.axis_index("grp"), lax.axis_index("kv"), lax.axis_index("tp")
    x, y = kv // 4, lax.rem(kv, 4)
    other = 1 - tp
    partner = (grp, kv, other)

    def dev(k):
        return (grp, peer_of(x, y, k), tp)

    def zdev(dz):
        return (lax.rem(grp + dz, 4), kv, tp)

    def remote(src, dst, send, recv, device):
        copy = pltpu.make_async_remote_copy(
            src_ref=src, dst_ref=dst, send_sem=send, recv_sem=recv, device_id=device,
            device_id_type=MESH,
        )
        copy.start()
        return copy

    def settle(ref, sem):
        pltpu.make_async_copy(ref, ref, sem).wait()

    wq_load = pltpu.make_async_copy(wq_hbm, wq, ld_sem.at[0])
    wq_load.start()
    pool_loads = []
    for c in range(nc):
        load = pltpu.make_async_copy(pool_hbm.at[:, pl.ds(PIECES[c][0] * 128 + PIECES[c][1], PIECES[c][2]), :], pool[c], pool_sem.at[c])
        load.start()
        pool_loads.append(load)
    kept_load = pltpu.make_async_copy(res_hbm, kept, kept_sem.at[0])
    kept_load.start()
    tok_load = pltpu.make_async_copy(
        tok_hbm.at[pl.ds(pl.multiple_of(kv * 8, 8), 8)], tok, ld_sem.at[1]
    )
    tok_load.start()

    loads = [
        pltpu.make_async_copy(src, dst, w_sem.at[i])
        for i, (src, dst) in enumerate([(wg_hbm, wg), (wu_hbm, wu), (wd_hbm, wd)])
    ]
    for load in loads:
        load.start()

    barrier = pltpu.get_barrier_semaphore()
    pl.semaphore_signal(barrier, inc=1, device_id=partner, device_id_type=MESH)
    for k in range(1, 16):
        pl.semaphore_signal(barrier, inc=1, device_id=dev(k), device_id_type=MESH)
        pl.semaphore_signal(
            barrier, inc=1, device_id=(grp, peer_of(x, y, k), other), device_id_type=MESH
        )
    for dz in range(1, 4):
        pl.semaphore_signal(barrier, inc=1, device_id=zdev(dz), device_id_type=MESH)

    feats = hid_ref[...].astype(f32)
    normed = (feats * again_ref[...]).astype(bf16)
    squares = jnp.sum(feats * feats, axis=1, keepdims=True)
    wq_load.wait()
    for h in range(2):
        part = jnp.dot(normed, wq[:, h * 512 : h * 512 + 512], preferred_element_type=f32)
        qa1s[:, :, h * 512 : h * 512 + 512] = part.reshape(4, 32, 512)
    qa1s[:, :, 1024:1152] = jnp.broadcast_to(squares, (128, 128)).reshape(4, 32, 128)
    for h in range(2):
        part = jnp.dot(normed, wq[:, 1024 + h * 512 : 1536 + h * 512], preferred_element_type=f32)
        for i in range(16):
            qb1s[i % 4, i // 4, :, h * 512 : h * 512 + 512] = part[8 * i : 8 * i + 8]
    pl.semaphore_wait(barrier, 34)

    for step in (2, 1, 3):
        remote(qa1s.at[lax.rem(x + step, 4)], qa1r.at[step], q_ss.at[0], q_rs.at[0], dev(4 * step))
        remote(qb1s.at[lax.rem(y + step, 4)], qb1r.at[step], q_ss.at[1], q_rs.at[1], dev(step))

    owners = own_ref[...]
    spot = lax.broadcasted_iota(i32, (4, 256), 1)
    group_row = lax.broadcasted_iota(i32, (4, 256), 0)
    mine = jnp.where(owners == grp * 16 + kv, loc_ref[...], 0)
    pick = [jnp.sum(jnp.where(spot // 16 == j, mine, 0)) for j in range(16)]
    from_grp = owners // 16
    rank = jnp.zeros((4, 256), i32)
    for back in range(1, 16):
        earlier = pltpu.roll(from_grp, back, 1) == from_grp
        rank = rank + jnp.where(earlier & (lax.rem(spot, 16) >= back), 1, 0)
    here = spot // 16 == kv
    leaving = here & (from_grp == grp)
    sender = lax.rem(owners, 16)
    onward = [
        [jnp.sum(jnp.where(leaving & (group_row == g) & (rank == r), sender, 0)) for r in range(4)]
        for g in range(4)
    ]
    landed = jnp.where(here & (group_row == grp), from_grp * 4 + rank, 0)
    landing = [jnp.sum(jnp.where(lax.rem(spot, 16) == i, landed, 0)) for i in range(16)]
    del mine
    for j in range(16):
        picks[j] = pick[j]
        picks[32 + j] = landing[j]
    for g in range(4):
        for r in range(4):
            picks[16 + 4 * g + r] = onward[g][r]

    def xy_start(c):
        pool_loads[c].wait()
        xr[c][kv] = pool[c][picks[kv]]
        for k in range(1, 16):
            xs[c][k - 1] = pool[c][picks[peer_of(x, y, k)]]
        for k in ORDER[::-1]:
            remote(xs[c].at[k - 1], xr[c].at[kv], x_ss.at[c], x_rs.at[c], dev(k))

    def z_start(c):
        settle(xs[c], x_rs.at[c])
        for dz in range(4):
            g = lax.rem(grp + dz, 4)
            for r in range(4):
                page = xr[c][picks[16 + g * 4 + r]]
                if dz == 0:
                    zr[c][grp, r] = page
                else:
                    zs[c][dz - 1, r] = page
        for dz in (2, 1, 3):
            remote(zs[c].at[dz - 1], zr[c].at[grp], z_ss.at[c], z_rs.at[c], zdev(dz))

    def finish(c):
        settle(zs[c], z_rs.at[c])
        half, row, tokens = PIECES[c]
        final = (fsk, fsv)[half]
        for i in range(16):
            where = picks[32 + i]
            final[i, row : row + tokens, :] = zr[c][where // 4, lax.rem(where, 4)]
        pltpu.make_async_copy(
            final.at[:, pl.ds(row, tokens), :], cache_hbm.at[:, half, pl.ds(row, tokens), :], out_sem.at[half]
        ).start()

    head_of = lax.broadcasted_iota(i32, (16, 512), 0) // 4
    block_of = lax.broadcasted_iota(i32, (16, 512), 1) // 128
    diag = head_of == block_of
    lanes = lax.broadcasted_iota(i32, (16, 128), 1)

    def page_scores(p, keys, slot, filled):
        place_x, place_y, place_s = slot // 32, lax.rem(slot // 8, 4), lax.rem(slot, 8)
        q = jnp.concatenate([qfa[place_x, place_y, place_s], qfb[place_x, place_y, place_s]], axis=0)
        wide = jnp.where(diag, jnp.concatenate([q, q, q, q], axis=1), 0.0)
        high = wide.astype(bf16)
        left = wide - high.astype(f32)
        mid = left.astype(bf16)
        low = (left - mid.astype(f32)).astype(bf16)
        rows = jnp.concatenate([high, mid, low], axis=0)
        s = lax.dot_general(rows, keys, (((1,), (1,)), ((), ())), preferred_element_type=f32)
        s = s[:16] + s[16:32] + s[32:]
        s = jnp.where(lanes < filled, s, neg_fill)
        scores[p] = s
        top = jnp.max(s, axis=1, keepdims=True)
        total = jnp.sum(jnp.where(lanes < filled, jnp.exp(s - top), 0.0), axis=1, keepdims=True)
        return top, total

    def weighted(p, values, lo, hi):
        w = probs[p][:, lo:hi]
        high = w.astype(bf16)
        low = (w - high.astype(f32)).astype(bf16)
        out = jnp.dot(jnp.concatenate([high, low], axis=0), values, preferred_element_type=f32)
        return out[:16] + out[16:]

    def place(accs, p, acc):
        for h in range(16):
            accs[h, p : p + 1, :] = acc[h : h + 1, (h // 4) * 128 : (h // 4) * 128 + 128]

    lane32 = lax.broadcasted_iota(i32, (32, 128), 1)

    def note(table, p, top, total):
        return jnp.where(lane32 == p, jnp.concatenate([top, total], axis=0), table)

    def query_second():
        settle(qa1r.at[pl.ds(1, 3)], q_rs.at[0])
        qa2s[...] = (qa1s[x] + qa1r[1] + qa1r[2] + qa1r[3]).reshape(4, 8, 1152)
        settle(qb1r.at[pl.ds(1, 3)], q_rs.at[1])
        qb2s[...] = qb1s[y] + qb1r[1] + qb1r[2] + qb1r[3]
        for step in (2, 1, 3):
            remote(qa2s.at[lax.rem(y + step, 4)], qa2r.at[step], q_ss.at[2], q_rs.at[2], dev(step))
            remote(qb2s.at[lax.rem(x + step, 4)], qb2r.at[step], q_ss.at[3], q_rs.at[3], dev(4 * step))

    def query_done():
        settle(qa2r.at[pl.ds(1, 3)], q_rs.at[2])
        first = qa2s[y] + qa2r[1] + qa2r[2] + qa2r[3]
        settle(qb2r.at[pl.ds(1, 3)], q_rs.at[3])
        second = qb2s[x] + qb2r[1] + qb2r[2] + qb2r[3]
        scale = lax.rsqrt(first[:, 1024:1025] / D + norm_eps)
        q8 = jnp.concatenate([first[:, :1024], second], axis=1) * scale * HEAD_DIM ** (-0.5)
        qflat[...] = q8
        for h in range(8):
            qfa[x, y, :, h, :] = q8[:, h * 128 : h * 128 + 128]
            qfb[x, y, :, h, :] = q8[:, 1024 + h * 128 : 1152 + h * 128]
        for step in (2, 1, 3):
            remote(qfa.at[x, y], qfa.at[x, y], a_ss.at[0], a_rs.at[0], dev(4 * step))
            remote(qfb.at[x, y], qfb.at[x, y], a_ss.at[1], a_rs.at[1], dev(step))

    def query_spread():
        settle(qfa.at[pl.ds(0, 3), 0], a_rs.at[0])
        settle(qfb.at[pl.ds(0, 3), 0], a_rs.at[1])
        for step in (2, 1, 3):
            remote(qfa.at[:, y], qfa.at[:, y], a_ss.at[2], a_rs.at[2], dev(step))
            remote(qfb.at[x], qfb.at[x], a_ss.at[3], a_rs.at[3], dev(4 * step))

    xy_start(0)
    query_second()
    for j in range(16):
        near_cols = pl.ds(pl.multiple_of(j * 256 + tp * 128, 128), 128)
        far_cols = pl.ds(pl.multiple_of(j * 256 + other * 128, 128), 128)
        here = pl.ds(j * 128, 128)
        pltpu.make_async_copy(wout_hbm.at[:, near_cols], w2.at[pl.ds(0, 128), here], w_sem.at[3]).start()
        remote(wout_hbm.at[:, far_cols], w2.at[pl.ds(128, 128), here], wp_ss.at[0], wp_rs.at[0], partner)
    xy_start(1)
    xy_start(2)
    z_start(0)
    query_done()
    xy_start(3)
    z_start(1)
    finish(0)
    query_spread()
    xy_start(4)
    z_start(2)
    finish(1)
    xy_start(5)
    z_start(3)
    finish(2)
    xy_start(6)
    tok_load.wait()
    own_key, own_value = tok[:, 0, :].astype(f32), tok[:, 1, :].astype(f32)
    lane8 = lax.broadcasted_iota(i32, (8, 128), 1)
    own_rows = jnp.zeros((8, 128), f32)
    for h in range(16):
        s = jnp.sum(
            qflat[:, h * 128 : h * 128 + 128] * own_key[:, (h // 4) * 128 : (h // 4) * 128 + 128],
            axis=1, keepdims=True,
        )
        own_rows = jnp.where(lane8 == h, s, own_rows)
    own_tops = jnp.concatenate([jnp.zeros((24, 128), f32), own_rows, jnp.zeros((96, 128), f32)], axis=0).T[:16]
    slot_row = jnp.zeros((8, 128), i32)
    for p in range(24):
        slot_row = jnp.where(lane8 == p, arr_slot[0, p] if p < 16 else res_slot[0, p - 16], slot_row)
    slot_row = jnp.where(lane8 >= 24, kv * 8 + lane8 - 24, slot_row)
    settle(qfa.at[:, pl.ds(0, 3)], a_rs.at[2])
    settle(qfb.at[pl.ds(0, 3)], a_rs.at[3])
    kept_load.wait()
    table = jnp.zeros((32, 128), f32)
    for p in range(8):
        table = note(table, 16 + p, *page_scores(16 + p, kept[p, 0], res_slot[0, p], res_len[0, p]))
    z_start(4)
    finish(3)
    xy_start(7)
    xy_start(8)
    for p in range(16):
        table = note(table, p, *page_scores(p, fsk[p], arr_slot[0, p], arr_len[0, p]))
    own_lane = lanes >= 24
    mine = jnp.concatenate(
        [
            jnp.where(own_lane, own_tops, table[:16]),
            jnp.where(own_lane, 1.0, table[16:]),
            slot_row.astype(f32),
        ],
        axis=0,
    )
    mine = jnp.where(lax.broadcasted_iota(i32, (40, 128), 1) < 32, mine, 0.0)
    turned = [mine] + [pltpu.roll(mine, 32 * q, 1) for q in range(1, 4)]
    for q in range(1, 4):
        mine = jnp.where(y == q, turned[q], mine)
    stats[kv] = mine
    for k in ORDER[::-1]:
        remote(stats.at[kv], stats.at[kv], s_ss.at[0], s_rs.at[0], dev(k))
    z_start(5)
    finish(4)
    z_start(6)
    finish(5)
    z_start(7)
    z_start(8)
    settle(stats.at[pl.ds(0, 15)], s_rs.at[0])
    every = jnp.concatenate(
        [stats[4 * i] + stats[4 * i + 1] + stats[4 * i + 2] + stats[4 * i + 3] for i in range(4)], axis=1
    )
    tops, sums, every_slot = every[:16], every[16:32], every[32:33].astype(i32)
    own_w = jnp.zeros((16, 128), f32)
    for p in range(32):
        slot = arr_slot[0, p] if p < 16 else (res_slot[0, p - 16] if p < 24 else kv * 8 + p - 24)
        same = jnp.broadcast_to(every_slot == slot, (16, 512))
        top = jnp.max(jnp.where(same, tops, neg_fill), axis=1, keepdims=True)
        total = jnp.sum(jnp.where(same, jnp.exp(tops - top) * sums, 0.0), axis=1, keepdims=True)
        if p < 24:
            probs[p] = jnp.exp(scores[p] - top) * (1.0 / total)
        else:
            own_w = jnp.where(lanes == p, jnp.exp(own_tops - top) * (1.0 / total), own_w)
    own_weight = jnp.concatenate([own_w, jnp.zeros((112, 128), f32)], axis=0).T[24:32]
    for h in range(16):
        g = (h // 4) * 128
        eaccs[h, 8:16, :] = own_weight[:, h : h + 1] * own_value[:, g : g + 128]
    rho = lax.broadcasted_iota(i32, (128, 512), 0)
    member = (lax.rem(rho, 64) // 4) * 8 + (rho // 64) * 4 + lax.rem(rho, 4) == every_slot
    member = jnp.where(member, 1.0, 0.0).astype(bf16)

    def swap(accs, msend):
        tiles = [accs[h] for h in range(16)]
        group = lanes // 8
        for bit in (1, 2, 4, 8):
            upper = (group & bit) != 0
            for h in range(16):
                if h & bit == 0:
                    a, b = tiles[h], tiles[h + bit]
                    tiles[h] = jnp.where(upper, pltpu.roll(b, 8 * bit, 1), a)
                    tiles[h + bit] = jnp.where(upper, b, pltpu.roll(a, 128 - 8 * bit, 1))
        for j in range(16):
            msend[j] = tiles[j].astype(bf16)

    def spread(msend, row, n):
        rows = pl.ds(row, 16)
        for k in ORDER[::-1]:
            piece = msend.at[peer_of(x, y, k)]
            remote(piece, mrecv.at[tp, kv, rows], m_ss.at[n], m_rs.at[n], dev(k))
            remote(piece, mrecv.at[tp, kv, rows], m_ss.at[n + 1], m_rs.at[n + 1], (grp, peer_of(x, y, k), other))
        remote(msend.at[kv], mrecv.at[tp, kv, rows], m_ss.at[n + 1], m_rs.at[n + 1], partner)
        mrecv[tp, kv, rows, :] = msend[kv]

    for p in range(8):
        place(eaccs, p, weighted(16 + p, kept[p, 1], 0, 128))
    swap(eaccs, esend)
    spread(esend, 16, 2)
    for p in range(16):
        pvacc[p] = weighted(p, fsv[p, :64, :], 0, 64)
    finish(6)
    for p in range(16):
        pvacc[p] = pvacc[p] + weighted(p, fsv[p, 64:96, :], 64, 96)
    finish(7)
    finish(8)
    for p in range(16):
        place(accs, p, pvacc[p] + weighted(p, fsv[p, 96:, :], 96, 128))
    swap(accs, msend)
    spread(msend, 0, 0)

    rho = lax.broadcasted_iota(jnp.int32, (128, 128), 0)
    col = lax.broadcasted_iota(jnp.int32, (128, 128), 1)
    slot = (lax.rem(rho, 64) // 4) * 8 + (rho // 64) * 4 + lax.rem(rho, 4)
    perm = jnp.where(col == slot, 1.0, 0.0).astype(bf16)
    block = jnp.dot(
        perm, hid_ref[:, pl.ds(pl.multiple_of(tp * 128, 128), 128)], preferred_element_type=f32
    )
    settle(w2.at[pl.ds(0, 128)], w_sem.at[3])
    settle(w2.at[pl.ds(128, 128)], wp_rs.at[0])
    settle(esend.at[pl.ds(0, 15)], m_rs.at[2])
    settle(esend, m_rs.at[3])
    settle(msend.at[pl.ds(0, 15)], m_rs.at[0])
    near = jnp.dot(member, mrecv[tp].reshape(512, 128), preferred_element_type=f32).astype(bf16)
    settle(msend, m_rs.at[1])
    far = jnp.dot(member, mrecv[other].reshape(512, 128), preferred_element_type=f32).astype(bf16)
    slices = jnp.concatenate([near, far], axis=1)

    def share(j, part):
        rs_send[j] = part.astype(bf16)
        remote(rs_send.at[j], rs_recv.at[kv], rs_ss.at[0], rs_rs.at[0], (grp, j, tp))

    for half in range(2):
        for dx in (2, 1, 3):
            row = lax.rem(x + dx, 4)
            cols = pl.ds(pl.multiple_of(row * 512 + half * 256, 256), 256)
            part = jnp.dot(slices, w2[:, cols], preferred_element_type=f32)
            share(row * 4 + 2 * half, part[:, :128])
            share(row * 4 + 2 * half + 1, part[:, 128:])
    for dy in (2, 1, 3, 0):
        j = x * 4 + lax.rem(y + dy, 4)
        part = jnp.dot(slices, w2[:, pl.ds(pl.multiple_of(j * 128, 128), 128)], preferred_element_type=f32)
        if dy:
            share(j, part)
        else:
            block = block + part
    settle(rs_recv.at[pl.ds(0, 15)], rs_rs.at[0])
    for k in ORDER:
        block = block + rs_recv[source_of(x, y, k)].astype(f32)
    ag[0, tp] = block.astype(bf16)

    def forward(k):
        remote(ag.at[k, tp], ag.at[k, tp], fw_ss.at[0], fw_rs.at[k], partner)

    forward(0)
    for k in ORDER:
        remote(ag.at[0, tp], ag.at[k, tp], ag_ss.at[0], ag_rs.at[k], dev(k))
    loads[0].wait()
    loads[1].wait()
    seq = [0] + ORDER
    nt = (((1,), (1,)), ((), ()))
    gate = jnp.zeros((128, 448), f32)
    upward = jnp.zeros((128, 448), f32)
    squares = jnp.zeros((128, 128), f32)
    mine = lax.broadcasted_iota(jnp.int32, (8, 128), 0) + tp * 64 + kv * 4
    pick = jnp.where(lax.broadcasted_iota(jnp.int32, (8, 128), 1) == mine, 1.0, 0.0).astype(bf16)
    for n, k in enumerate(seq):
        for later in seq[n + 1 : n + 4] if n == 0 else seq[n + 3 : n + 4]:
            settle(ag.at[later, tp], ag_rs.at[later])
            forward(later)
        settle(ag.at[k, other], fw_rs.at[k])
        src = source_of(x, y, k)
        both = jnp.concatenate([ag[k, 0], ag[k, 1]], axis=1)
        wide = both.astype(f32)
        squares = squares + wide[:, :128] * wide[:, :128] + wide[:, 128:] * wide[:, 128:]
        rows = pl.ds(pl.multiple_of(src * 256, 256), 256)
        normed = (wide * gain_ref[:, rows]).astype(bf16)
        gate = gate + lax.dot_general(normed, wg[:, rows], nt, preferred_element_type=f32)
        upward = upward + lax.dot_general(normed, wu[:, rows], nt, preferred_element_type=f32)
    scale = lax.rsqrt(jnp.sum(squares, axis=1, keepdims=True) / D + norm_eps)
    gate = gate * scale
    upward = upward * scale
    hunits[...] = (gate / (1.0 + jnp.exp(-gate)) * upward).astype(bf16)

    loads[2].wait()
    for c in range(4):
        cols = pl.ds(c * 1024, 1024)
        part = jnp.dot(hunits[...], wd[:, cols], preferred_element_type=f32)
        first, second = part[:64], part[64:]
        dsum[:, cols] = jnp.where(tp == 0, first, second)
        dp_send[c] = jnp.where(tp == 0, second, first).astype(bf16)
        remote(dp_send.at[c], dp_recv.at[c], dp_ss.at[0], dp_rs.at[c], partner)
    for c in range(4):
        settle(dp_recv.at[c], dp_rs.at[c])
        cols = pl.ds(c * 1024, 1024)
        dsum[:, cols] = dsum[:, cols] + dp_recv[c].astype(f32)
    for j in range(16):
        d_send[j] = dsum[4 * j : 4 * j + 4, :].astype(bf16)
    for k in ORDER[::-1]:
        remote(d_send.at[peer_of(x, y, k)], d_recv.at[k], d_ss.at[0], d_rs.at[0], dev(k))
    for c in range(nc):
        settle(xs[c], x_ss.at[c])
        settle(zs[c], z_ss.at[c])
    settle(qa1s.at[pl.ds(0, 3)], q_ss.at[0])
    settle(qb1s.at[pl.ds(0, 3)], q_ss.at[1])
    settle(qa2s.at[pl.ds(0, 3)], q_ss.at[2])
    settle(qb2s.at[pl.ds(0, 3)], q_ss.at[3])
    settle(qfa.at[pl.ds(0, 3), 0], a_ss.at[0])
    settle(qfb.at[pl.ds(0, 3), 0], a_ss.at[1])
    settle(qfa.at[:, pl.ds(0, 3)], a_ss.at[2])
    settle(qfb.at[pl.ds(0, 3)], a_ss.at[3])
    settle(stats.at[pl.ds(0, 15)], s_ss.at[0])
    settle(msend.at[pl.ds(0, 15)], m_ss.at[0])
    settle(w2.at[pl.ds(0, 128)], wp_ss.at[0])
    settle(msend, m_ss.at[1])
    settle(esend.at[pl.ds(0, 15)], m_ss.at[2])
    settle(esend, m_ss.at[3])
    settle(rs_send.at[pl.ds(1, 15)], rs_ss.at[0])
    settle(rs_send.at[pl.ds(1, 15)], ag_ss.at[0])
    settle(rs_send, fw_ss.at[0])
    settle(dp_send, dp_ss.at[0])
    settle(fsk, out_sem.at[0])
    settle(fsv, out_sem.at[1])
    for k in range(16):
        for t in range(2):
            cols = pl.ds(pl.multiple_of((source_of(x, y, k) * 2 + t) * 128, 128), 128)
            resrow[:, cols] = jnp.dot(pick, ag[k, t], preferred_element_type=f32)
    total = resrow[...][:4]
    own = jnp.zeros((4, 4096), f32)
    for j in range(16):
        own = jnp.where(kv == j, dsum[4 * j : 4 * j + 4, :], own)
    total = total + own
    settle(d_recv.at[pl.ds(1, 15)], d_rs.at[0])
    for k in ORDER:
        total = total + d_recv[k].astype(f32)
    out_ref[...] = total.astype(bf16)
    settle(d_send.at[pl.ds(0, 15)], d_ss.at[0])


def step(*operands):
    bf16, f32 = jnp.bfloat16, jnp.float32
    smem = pl.BlockSpec(memory_space=pltpu.SMEM)
    vmem = pl.BlockSpec(memory_space=pltpu.VMEM)
    hbm = pl.BlockSpec(memory_space=pl.ANY)
    dma = pltpu.SemaphoreType.DMA
    nc = len(PIECES)

    def chunk(*lead):
        return [pltpu.VMEM((*lead, tokens, 512), bf16) for _, _, tokens in PIECES]

    return pl.pallas_call(
        step_kernel,
        name="step",
        out_shape=(
            jax.ShapeDtypeStruct((4, 4096), bf16),
            jax.ShapeDtypeStruct((16, 2, 128, 512), bf16),
        ),
        in_specs=[smem] * 4 + [vmem] * 5 + [hbm] * 8,
        out_specs=(vmem, hbm),
        scratch_shapes=[
            pltpu.VMEM((256, 2048), bf16),
            pltpu.VMEM((8, 2, 512), bf16),
            pltpu.VMEM((8, 2, 128, 512), bf16),
            pltpu.VMEM((4, 32, 1152), f32),
            pltpu.VMEM((4, 32, 1152), f32),
            pltpu.VMEM((4, 8, 1152), f32),
            pltpu.VMEM((4, 8, 1152), f32),
            pltpu.VMEM((4, 4, 8, 1024), f32),
            pltpu.VMEM((4, 4, 8, 1024), f32),
            pltpu.VMEM((4, 8, 1024), f32),
            pltpu.VMEM((4, 8, 1024), f32),
            pltpu.VMEM((4, 4, 8, 8, 128), f32),
            pltpu.VMEM((4, 4, 8, 8, 128), f32),
            pltpu.VMEM((8, 2048), f32),
            pltpu.VMEM((16, 128, 512), bf16),
            pltpu.VMEM((16, 128, 512), bf16),
            pltpu.VMEM((24, 16, 128), f32),
            pltpu.VMEM((24, 16, 128), f32),
            pltpu.VMEM((16, 16, 512), f32),
            pltpu.VMEM((16, 16, 128), f32),
            pltpu.VMEM((16, 16, 128), f32),
            pltpu.VMEM((16, 40, 128), f32),
            pltpu.VMEM((16, 16, 128), bf16),
            pltpu.VMEM((16, 16, 128), bf16),
            pltpu.VMEM((2, 16, 32, 128), bf16),
            pltpu.VMEM((256, 2048), bf16),
            pltpu.VMEM((448, 4096), bf16),
            pltpu.VMEM((448, 4096), bf16),
            pltpu.VMEM((448, 4096), bf16),
            pltpu.VMEM((16, 128, 128), bf16),
            pltpu.VMEM((16, 128, 128), bf16),
            pltpu.VMEM((16, 2, 128, 128), bf16),
            pltpu.VMEM((128, 448), bf16),
            pltpu.VMEM((4, 64, 1024), bf16),
            pltpu.VMEM((4, 64, 1024), bf16),
            pltpu.VMEM((64, 4096), f32),
            pltpu.VMEM((16, 4, 4096), bf16),
            pltpu.VMEM((16, 4, 4096), bf16),
            pltpu.VMEM((8, 4096), f32),
            pltpu.SMEM((48,), jnp.int32),
            *chunk(16), *chunk(15), *chunk(16), *chunk(3, 4), *chunk(4, 4),
            dma((2,)), dma((nc,)), dma((1,)), dma((2,)),
            dma((4,)), dma((4,)), dma((4,)), dma((4,)),
            dma((nc,)), dma((nc,)), dma((nc,)), dma((nc,)),
            dma((1,)), dma((1,)), dma((4,)), dma((4,)),
            dma((4,)), dma((1,)), dma((1,)), dma((1,)), dma((1,)), dma((1,)), dma((16,)),
            dma((1,)), dma((16,)), dma((1,)), dma((4,)), dma((1,)), dma((1,)),
        ],
        compiler_params=pltpu.CompilerParams(
            collective_id=0, has_side_effects=True, vmem_limit_bytes=62 * 1024 * 1024
        ),
    )(*operands)


def deliver_kernel(mixed_ref, cache_hbm, out_ref, final_hbm, pages, in_sem, out_sem):
    loads = [pltpu.make_async_copy(cache_hbm.at[i], pages.at[i], in_sem.at[i]) for i in range(16)]
    stores = [pltpu.make_async_copy(pages.at[i], final_hbm.at[i], out_sem.at[0]) for i in range(16)]
    for load in loads:
        load.start()
    out_ref[...] = mixed_ref[...]
    for load, store in zip(loads, stores):
        load.wait()
        store.start()
    pltpu.make_async_copy(pages, pages, out_sem.at[0]).wait()


def deliver(mixed, cache):
    vmem = pl.BlockSpec(memory_space=pltpu.VMEM)
    hbm = pl.BlockSpec(memory_space=pl.ANY)
    dma = pltpu.SemaphoreType.DMA
    return pl.pallas_call(
        deliver_kernel,
        name="deliver",
        out_shape=(
            jax.ShapeDtypeStruct(mixed.shape, mixed.dtype),
            jax.ShapeDtypeStruct(cache.shape, cache.dtype),
        ),
        in_specs=[vmem, hbm],
        out_specs=(vmem, hbm),
        scratch_shapes=[pltpu.VMEM(cache.shape, cache.dtype), dma((16,)), dma((1,))],
        compiler_params=pltpu.CompilerParams(vmem_limit_bytes=62 * 1024 * 1024),
    )(mixed, cache)


def per_device(
    hidden_states,
    attn_gain,
    mlp_gain,
    w_query,
    w_out,
    w_gate,
    w_up,
    w_down,
    kv_pool,
    resident_cache,
    resident_slot,
    resident_len,
    new_owner,
    new_local,
    new_slot,
    new_len,
    token_kv,
):
    mixed, new_pages = step(
        resident_slot,
        resident_len,
        new_slot,
        new_len,
        new_owner,
        new_local,
        hidden_states,
        attn_gain.reshape(1, 256),
        mlp_gain.reshape(1, 4096),
        token_kv,
        w_query,
        kv_pool.reshape(16, 256, 512),
        resident_cache[0],
        w_out.reshape(128, 4096),
        w_gate.T,
        w_up.T,
        w_down,
    )
    mixed, new_pages = deliver(mixed, new_pages)
    return (mixed, new_pages[None])


def solution(mesh):
    return jax.shard_map(
        per_device,
        mesh=mesh,
        in_specs=(
            P("grp", "kv"),
            P("kv"),
            P(),
            P("kv", "tp"),
            P("tp", "kv", None),
            P(None, KV_TP),
            P(None, KV_TP),
            P(KV_TP, None),
            P(GRP_KV, None, None, "tp"),
            P("grp", "kv", None, None, "tp"),
            P("grp", "kv"),
            P("grp", "kv"),
            P(),
            P(),
            P("grp", "kv"),
            P("grp", "kv"),
            P("grp", None, "tp"),
        ),
        out_specs=(P(GRP_KV_TP, None), P("grp", "kv", None, None, "tp")),
        check_vma=False,
    )
```

```python
import jax
import jax.numpy as jnp
from jax import lax
from jax.experimental import pallas as pl
from jax.experimental.pallas import tpu as pltpu
from jax.sharding import PartitionSpec as P

D = 4096
HEADS = 32
KV_HEADS = 8
HEAD_DIM = 128
KV_TP = ("kv", "tp")
GRP_KV = ("grp", "kv")
GRP_KV_TP = ("grp", "kv", "tp")


neg_fill = -1e30
norm_eps = 1e-05
MESH = pl.DeviceIdType.MESH


def peer_of(x, y, k):
    return lax.rem(x + k // 4, 4) * 4 + lax.rem(y + k % 4, 4)


def source_of(x, y, k):
    return lax.rem(x + 4 - k // 4, 4) * 4 + lax.rem(y + 4 - k % 4, 4)


ORDER = sorted(range(1, 16), key=lambda k: (min(k // 4, 4 - k // 4) + min(k % 4, 4 - k % 4), k))


PIECES = [(0, 0, 32), (0, 32, 32), (0, 64, 32), (0, 96, 32), (1, 0, 32), (1, 32, 32), (1, 64, 32), (1, 96, 16), (1, 112, 16)]


def step_kernel(
    res_slot, res_len, arr_slot, arr_len, own_ref, loc_ref, hid_ref, again_ref, gain_ref, tok_hbm, wq_hbm, pool_hbm, res_hbm, wout_hbm, wg_hbm, wu_hbm, wd_hbm,
    out_ref, cache_ref,
    wq, tok, kept, qa1s, qa1r, qa2s, qa2r, qb1s, qb1r, qb2s, qb2r, qfa, qfb, qflat, scores, probs, pvacc, accs, eaccs, stats, msend, esend, mrecv,
    w2, wg, wu, wd, rs_send, rs_recv, ag, hunits,
    dp_send, dp_recv, dsum, d_send, d_recv, resrow, picks, *rest,
):
    f32, bf16, i32 = jnp.float32, jnp.bfloat16, jnp.int32
    nc = len(PIECES)
    pool, xs, xr, zs, zr = (rest[i * nc : (i + 1) * nc] for i in range(5))
    (ld_sem, pool_sem, kept_sem, q_ss, q_rs, a_ss, a_rs, x_ss, x_rs, z_ss, z_rs, s_ss, s_rs,
     m_ss, m_rs, w_sem, wp_ss, wp_rs, rs_ss, rs_rs, ag_ss, ag_rs, fw_ss, fw_rs, dp_ss, dp_rs, d_ss,
     d_rs) = rest[5 * nc :]
    grp, kv, tp = lax.axis_index("grp"), lax.axis_index("kv"), lax.axis_index("tp")
    x, y = kv // 4, lax.rem(kv, 4)
    other = 1 - tp
    partner = (grp, kv, other)

    def dev(k):
        return (grp, peer_of(x, y, k), tp)

    def zdev(dz):
        return (lax.rem(grp + dz, 4), kv, tp)

    def remote(src, dst, send, recv, device):
        copy = pltpu.make_async_remote_copy(
            src_ref=src, dst_ref=dst, send_sem=send, recv_sem=recv, device_id=device,
            device_id_type=MESH,
        )
        copy.start()
        return copy

    def settle(ref, sem):
        pltpu.make_async_copy(ref, ref, sem).wait()

    wq_load = pltpu.make_async_copy(wq_hbm, wq, ld_sem.at[0])
    wq_load.start()
    pool_loads = []
    for c in range(nc):
        load = pltpu.make_async_copy(pool_hbm.at[:, pl.ds(PIECES[c][0] * 128 + PIECES[c][1], PIECES[c][2]), :], pool[c], pool_sem.at[c])
        load.start()
        pool_loads.append(load)
    kept_load = pltpu.make_async_copy(res_hbm, kept, kept_sem.at[0])
    kept_load.start()
    tok_load = pltpu.make_async_copy(
        tok_hbm.at[pl.ds(pl.multiple_of(kv * 8, 8), 8)], tok, ld_sem.at[1]
    )
    tok_load.start()

    loads = [
        pltpu.make_async_copy(src, dst, w_sem.at[i])
        for i, (src, dst) in enumerate([(wg_hbm, wg), (wu_hbm, wu), (wd_hbm, wd)])
    ]
    for load in loads:
        load.start()

    barrier = pltpu.get_barrier_semaphore()
    pl.semaphore_signal(barrier, inc=1, device_id=partner, device_id_type=MESH)
    for k in range(1, 16):
        pl.semaphore_signal(barrier, inc=1, device_id=dev(k), device_id_type=MESH)
        pl.semaphore_signal(
            barrier, inc=1, device_id=(grp, peer_of(x, y, k), other), device_id_type=MESH
        )
    for dz in range(1, 4):
        pl.semaphore_signal(barrier, inc=1, device_id=zdev(dz), device_id_type=MESH)

    feats = hid_ref[...].astype(f32)
    normed = (feats * again_ref[...]).astype(bf16)
    squares = jnp.sum(feats * feats, axis=1, keepdims=True)
    wq_load.wait()
    for h in range(2):
        part = jnp.dot(normed, wq[:, h * 512 : h * 512 + 512], preferred_element_type=f32)
        qa1s[:, :, h * 512 : h * 512 + 512] = part.reshape(4, 32, 512)
    qa1s[:, :, 1024:1152] = jnp.broadcast_to(squares, (128, 128)).reshape(4, 32, 128)
    for h in range(2):
        part = jnp.dot(normed, wq[:, 1024 + h * 512 : 1536 + h * 512], preferred_element_type=f32)
        for i in range(16):
            qb1s[i % 4, i // 4, :, h * 512 : h * 512 + 512] = part[8 * i : 8 * i + 8]
    pl.semaphore_wait(barrier, 34)

    for step in (2, 1, 3):
        remote(qa1s.at[lax.rem(x + step, 4)], qa1r.at[step], q_ss.at[0], q_rs.at[0], dev(4 * step))
        remote(qb1s.at[lax.rem(y + step, 4)], qb1r.at[step], q_ss.at[1], q_rs.at[1], dev(step))

    owners = own_ref[...]
    spot = lax.broadcasted_iota(i32, (4, 256), 1)
    group_row = lax.broadcasted_iota(i32, (4, 256), 0)
    mine = jnp.where(owners == grp * 16 + kv, loc_ref[...], 0)
    pick = [jnp.sum(jnp.where(spot // 16 == j, mine, 0)) for j in range(16)]
    from_grp = owners // 16
    rank = jnp.zeros((4, 256), i32)
    for back in range(1, 16):
        earlier = pltpu.roll(from_grp, back, 1) == from_grp
        rank = rank + jnp.where(earlier & (lax.rem(spot, 16) >= back), 1, 0)
    here = spot // 16 == kv
    leaving = here & (from_grp == grp)
    sender = lax.rem(owners, 16)
    onward = [
        [jnp.sum(jnp.where(leaving & (group_row == g) & (rank == r), sender, 0)) for r in range(4)]
        for g in range(4)
    ]
    landed = jnp.where(here & (group_row == grp), from_grp * 4 + rank, 0)
    landing = [jnp.sum(jnp.where(lax.rem(spot, 16) == i, landed, 0)) for i in range(16)]
    del mine
    for j in range(16):
        picks[j] = pick[j]
        picks[32 + j] = landing[j]
    for g in range(4):
        for r in range(4):
            picks[16 + 4 * g + r] = onward[g][r]

    def xy_start(c):
        pool_loads[c].wait()
        xr[c][kv] = pool[c][picks[kv]]
        for k in range(1, 16):
            xs[c][k - 1] = pool[c][picks[peer_of(x, y, k)]]
        for k in ORDER[::-1]:
            remote(xs[c].at[k - 1], xr[c].at[kv], x_ss.at[c], x_rs.at[c], dev(k))

    def z_start(c):
        settle(xs[c], x_rs.at[c])
        for dz in range(4):
            g = lax.rem(grp + dz, 4)
            for r in range(4):
                page = xr[c][picks[16 + g * 4 + r]]
                if dz == 0:
                    zr[c][grp, r] = page
                else:
                    zs[c][dz - 1, r] = page
        for dz in (2, 1, 3):
            remote(zs[c].at[dz - 1], zr[c].at[grp], z_ss.at[c], z_rs.at[c], zdev(dz))

    def finish(c):
        settle(zs[c], z_rs.at[c])
        half, row, tokens = PIECES[c]
        for i in range(16):
            where = picks[32 + i]
            cache_ref[i, half, row : row + tokens, :] = zr[c][where // 4, lax.rem(where, 4)]

    head_of = lax.broadcasted_iota(i32, (16, 512), 0) // 4
    block_of = lax.broadcasted_iota(i32, (16, 512), 1) // 128
    diag = head_of == block_of
    lanes = lax.broadcasted_iota(i32, (16, 128), 1)

    def page_scores(p, keys, slot, filled):
        place_x, place_y, place_s = slot // 32, lax.rem(slot // 8, 4), lax.rem(slot, 8)
        q = jnp.concatenate([qfa[place_x, place_y, place_s], qfb[place_x, place_y, place_s]], axis=0)
        wide = jnp.where(diag, jnp.concatenate([q, q, q, q], axis=1), 0.0)
        high = wide.astype(bf16)
        left = wide - high.astype(f32)
        mid = left.astype(bf16)
        low = (left - mid.astype(f32)).astype(bf16)
        rows = jnp.concatenate([high, mid, low], axis=0)
        s = lax.dot_general(rows, keys, (((1,), (1,)), ((), ())), preferred_element_type=f32)
        s = s[:16] + s[16:32] + s[32:]
        s = jnp.where(lanes < filled, s, neg_fill)
        scores[p] = s
        top = jnp.max(s, axis=1, keepdims=True)
        total = jnp.sum(jnp.where(lanes < filled, jnp.exp(s - top), 0.0), axis=1, keepdims=True)
        return top, total

    def weighted(p, values, lo, hi):
        w = probs[p][:, lo:hi]
        high = w.astype(bf16)
        low = (w - high.astype(f32)).astype(bf16)
        out = jnp.dot(jnp.concatenate([high, low], axis=0), values, preferred_element_type=f32)
        return out[:16] + out[16:]

    def place(accs, p, acc):
        for h in range(16):
            accs[h, p : p + 1, :] = acc[h : h + 1, (h // 4) * 128 : (h // 4) * 128 + 128]

    lane32 = lax.broadcasted_iota(i32, (32, 128), 1)

    def note(table, p, top, total):
        return jnp.where(lane32 == p, jnp.concatenate([top, total], axis=0), table)

    def query_second():
        settle(qa1r.at[pl.ds(1, 3)], q_rs.at[0])
        qa2s[...] = (qa1s[x] + qa1r[1] + qa1r[2] + qa1r[3]).reshape(4, 8, 1152)
        settle(qb1r.at[pl.ds(1, 3)], q_rs.at[1])
        qb2s[...] = qb1s[y] + qb1r[1] + qb1r[2] + qb1r[3]
        for step in (2, 1, 3):
            remote(qa2s.at[lax.rem(y + step, 4)], qa2r.at[step], q_ss.at[2], q_rs.at[2], dev(step))
            remote(qb2s.at[lax.rem(x + step, 4)], qb2r.at[step], q_ss.at[3], q_rs.at[3], dev(4 * step))

    def query_done():
        settle(qa2r.at[pl.ds(1, 3)], q_rs.at[2])
        first = qa2s[y] + qa2r[1] + qa2r[2] + qa2r[3]
        settle(qb2r.at[pl.ds(1, 3)], q_rs.at[3])
        second = qb2s[x] + qb2r[1] + qb2r[2] + qb2r[3]
        scale = lax.rsqrt(first[:, 1024:1025] / D + norm_eps)
        q8 = jnp.concatenate([first[:, :1024], second], axis=1) * scale * HEAD_DIM ** (-0.5)
        qflat[...] = q8
        for h in range(8):
            qfa[x, y, :, h, :] = q8[:, h * 128 : h * 128 + 128]
            qfb[x, y, :, h, :] = q8[:, 1024 + h * 128 : 1152 + h * 128]
        for step in (2, 1, 3):
            remote(qfa.at[x, y], qfa.at[x, y], a_ss.at[0], a_rs.at[0], dev(4 * step))
            remote(qfb.at[x, y], qfb.at[x, y], a_ss.at[1], a_rs.at[1], dev(step))

    def query_spread():
        settle(qfa.at[pl.ds(0, 3), 0], a_rs.at[0])
        settle(qfb.at[pl.ds(0, 3), 0], a_rs.at[1])
        for step in (2, 1, 3):
            remote(qfa.at[:, y], qfa.at[:, y], a_ss.at[2], a_rs.at[2], dev(step))
            remote(qfb.at[x], qfb.at[x], a_ss.at[3], a_rs.at[3], dev(4 * step))

    xy_start(0)
    query_second()
    for j in range(16):
        near_cols = pl.ds(pl.multiple_of(j * 256 + tp * 128, 128), 128)
        far_cols = pl.ds(pl.multiple_of(j * 256 + other * 128, 128), 128)
        here = pl.ds(j * 128, 128)
        pltpu.make_async_copy(wout_hbm.at[:, near_cols], w2.at[pl.ds(0, 128), here], w_sem.at[3]).start()
        remote(wout_hbm.at[:, far_cols], w2.at[pl.ds(128, 128), here], wp_ss.at[0], wp_rs.at[0], partner)
    xy_start(1)
    xy_start(2)
    z_start(0)
    query_done()
    xy_start(3)
    z_start(1)
    finish(0)
    query_spread()
    xy_start(4)
    z_start(2)
    finish(1)
    xy_start(5)
    z_start(3)
    finish(2)
    xy_start(6)
    tok_load.wait()
    own_key, own_value = tok[:, 0, :].astype(f32), tok[:, 1, :].astype(f32)
    lane8 = lax.broadcasted_iota(i32, (8, 128), 1)
    own_rows = jnp.zeros((8, 128), f32)
    for h in range(16):
        s = jnp.sum(
            qflat[:, h * 128 : h * 128 + 128] * own_key[:, (h // 4) * 128 : (h // 4) * 128 + 128],
            axis=1, keepdims=True,
        )
        own_rows = jnp.where(lane8 == h, s, own_rows)
    own_tops = jnp.concatenate([jnp.zeros((24, 128), f32), own_rows, jnp.zeros((96, 128), f32)], axis=0).T[:16]
    slot_row = jnp.zeros((8, 128), i32)
    for p in range(24):
        slot_row = jnp.where(lane8 == p, arr_slot[0, p] if p < 16 else res_slot[0, p - 16], slot_row)
    slot_row = jnp.where(lane8 >= 24, kv * 8 + lane8 - 24, slot_row)
    settle(qfa.at[:, pl.ds(0, 3)], a_rs.at[2])
    settle(qfb.at[pl.ds(0, 3)], a_rs.at[3])
    kept_load.wait()
    table = jnp.zeros((32, 128), f32)
    for p in range(8):
        table = note(table, 16 + p, *page_scores(16 + p, kept[p, 0], res_slot[0, p], res_len[0, p]))
    z_start(4)
    finish(3)
    xy_start(7)
    xy_start(8)
    for p in range(16):
        table = note(table, p, *page_scores(p, cache_ref[p, 0], arr_slot[0, p], arr_len[0, p]))
    own_lane = lanes >= 24
    mine = jnp.concatenate(
        [
            jnp.where(own_lane, own_tops, table[:16]),
            jnp.where(own_lane, 1.0, table[16:]),
            slot_row.astype(f32),
        ],
        axis=0,
    )
    mine = jnp.where(lax.broadcasted_iota(i32, (40, 128), 1) < 32, mine, 0.0)
    turned = [mine] + [pltpu.roll(mine, 32 * q, 1) for q in range(1, 4)]
    for q in range(1, 4):
        mine = jnp.where(y == q, turned[q], mine)
    stats[kv] = mine
    for k in ORDER[::-1]:
        remote(stats.at[kv], stats.at[kv], s_ss.at[0], s_rs.at[0], dev(k))
    z_start(5)
    finish(4)
    z_start(6)
    finish(5)
    z_start(7)
    z_start(8)
    settle(stats.at[pl.ds(0, 15)], s_rs.at[0])
    every = jnp.concatenate(
        [stats[4 * i] + stats[4 * i + 1] + stats[4 * i + 2] + stats[4 * i + 3] for i in range(4)], axis=1
    )
    tops, sums, every_slot = every[:16], every[16:32], every[32:33].astype(i32)
    own_w = jnp.zeros((16, 128), f32)
    for p in range(32):
        slot = arr_slot[0, p] if p < 16 else (res_slot[0, p - 16] if p < 24 else kv * 8 + p - 24)
        same = jnp.broadcast_to(every_slot == slot, (16, 512))
        top = jnp.max(jnp.where(same, tops, neg_fill), axis=1, keepdims=True)
        total = jnp.sum(jnp.where(same, jnp.exp(tops - top) * sums, 0.0), axis=1, keepdims=True)
        if p < 24:
            probs[p] = jnp.exp(scores[p] - top) * (1.0 / total)
        else:
            own_w = jnp.where(lanes == p, jnp.exp(own_tops - top) * (1.0 / total), own_w)
    own_weight = jnp.concatenate([own_w, jnp.zeros((112, 128), f32)], axis=0).T[24:32]
    for h in range(16):
        g = (h // 4) * 128
        eaccs[h, 8:16, :] = own_weight[:, h : h + 1] * own_value[:, g : g + 128]
    rho = lax.broadcasted_iota(i32, (128, 512), 0)
    member = (lax.rem(rho, 64) // 4) * 8 + (rho // 64) * 4 + lax.rem(rho, 4) == every_slot
    member = jnp.where(member, 1.0, 0.0).astype(bf16)

    def swap(accs, msend):
        tiles = [accs[h] for h in range(16)]
        group = lanes // 8
        for bit in (1, 2, 4, 8):
            upper = (group & bit) != 0
            for h in range(16):
                if h & bit == 0:
                    a, b = tiles[h], tiles[h + bit]
                    tiles[h] = jnp.where(upper, pltpu.roll(b, 8 * bit, 1), a)
                    tiles[h + bit] = jnp.where(upper, b, pltpu.roll(a, 128 - 8 * bit, 1))
        for j in range(16):
            msend[j] = tiles[j].astype(bf16)

    def spread(msend, row, n):
        rows = pl.ds(row, 16)
        for k in ORDER[::-1]:
            piece = msend.at[peer_of(x, y, k)]
            remote(piece, mrecv.at[tp, kv, rows], m_ss.at[n], m_rs.at[n], dev(k))
            remote(piece, mrecv.at[tp, kv, rows], m_ss.at[n + 1], m_rs.at[n + 1], (grp, peer_of(x, y, k), other))
        remote(msend.at[kv], mrecv.at[tp, kv, rows], m_ss.at[n + 1], m_rs.at[n + 1], partner)
        mrecv[tp, kv, rows, :] = msend[kv]

    for p in range(8):
        place(eaccs, p, weighted(16 + p, kept[p, 1], 0, 128))
    swap(eaccs, esend)
    spread(esend, 16, 2)
    for p in range(16):
        pvacc[p] = weighted(p, cache_ref[p, 1, :64, :], 0, 64)
    finish(6)
    for p in range(16):
        pvacc[p] = pvacc[p] + weighted(p, cache_ref[p, 1, 64:96, :], 64, 96)
    finish(7)
    finish(8)
    for p in range(16):
        place(accs, p, pvacc[p] + weighted(p, cache_ref[p, 1, 96:, :], 96, 128))
    swap(accs, msend)
    spread(msend, 0, 0)

    rho = lax.broadcasted_iota(jnp.int32, (128, 128), 0)
    col = lax.broadcasted_iota(jnp.int32, (128, 128), 1)
    slot = (lax.rem(rho, 64) // 4) * 8 + (rho // 64) * 4 + lax.rem(rho, 4)
    perm = jnp.where(col == slot, 1.0, 0.0).astype(bf16)
    block = jnp.dot(
        perm, hid_ref[:, pl.ds(pl.multiple_of(tp * 128, 128), 128)], preferred_element_type=f32
    )
    settle(w2.at[pl.ds(0, 128)], w_sem.at[3])
    settle(w2.at[pl.ds(128, 128)], wp_rs.at[0])
    settle(esend.at[pl.ds(0, 15)], m_rs.at[2])
    settle(esend, m_rs.at[3])
    settle(msend.at[pl.ds(0, 15)], m_rs.at[0])
    near = jnp.dot(member, mrecv[tp].reshape(512, 128), preferred_element_type=f32).astype(bf16)
    settle(msend, m_rs.at[1])
    far = jnp.dot(member, mrecv[other].reshape(512, 128), preferred_element_type=f32).astype(bf16)
    slices = jnp.concatenate([near, far], axis=1)

    def share(j, part):
        rs_send[j] = part.astype(bf16)
        remote(rs_send.at[j], rs_recv.at[kv], rs_ss.at[0], rs_rs.at[0], (grp, j, tp))

    for k in ORDER[::-1] + [0]:
        j = peer_of(x, y, k)
        part = jnp.dot(slices, w2[:, pl.ds(pl.multiple_of(j * 128, 128), 128)], preferred_element_type=f32)
        if k:
            share(j, part)
        else:
            block = block + part
    settle(rs_recv.at[pl.ds(0, 15)], rs_rs.at[0])
    for k in ORDER:
        block = block + rs_recv[source_of(x, y, k)].astype(f32)
    ag[0, tp] = block.astype(bf16)

    def forward(k):
        remote(ag.at[k, tp], ag.at[k, tp], fw_ss.at[0], fw_rs.at[k], partner)

    forward(0)
    for k in ORDER:
        remote(ag.at[0, tp], ag.at[k, tp], ag_ss.at[0], ag_rs.at[k], dev(k))
    loads[0].wait()
    loads[1].wait()
    seq = [0] + ORDER
    nt = (((1,), (1,)), ((), ()))
    gate = jnp.zeros((128, 448), f32)
    upward = jnp.zeros((128, 448), f32)
    squares = jnp.zeros((128, 128), f32)
    mine = lax.broadcasted_iota(jnp.int32, (8, 128), 0) + tp * 64 + kv * 4
    pick = jnp.where(lax.broadcasted_iota(jnp.int32, (8, 128), 1) == mine, 1.0, 0.0).astype(bf16)
    for n, k in enumerate(seq):
        for later in seq[n + 1 : n + 4] if n == 0 else seq[n + 3 : n + 4]:
            settle(ag.at[later, tp], ag_rs.at[later])
            forward(later)
        settle(ag.at[k, other], fw_rs.at[k])
        src = source_of(x, y, k)
        both = jnp.concatenate([ag[k, 0], ag[k, 1]], axis=1)
        wide = both.astype(f32)
        squares = squares + wide[:, :128] * wide[:, :128] + wide[:, 128:] * wide[:, 128:]
        rows = pl.ds(pl.multiple_of(src * 256, 256), 256)
        normed = (wide * gain_ref[:, rows]).astype(bf16)
        gate = gate + lax.dot_general(normed, wg[:, rows], nt, preferred_element_type=f32)
        upward = upward + lax.dot_general(normed, wu[:, rows], nt, preferred_element_type=f32)
    scale = lax.rsqrt(jnp.sum(squares, axis=1, keepdims=True) / D + norm_eps)
    gate = gate * scale
    upward = upward * scale
    hunits[...] = (gate / (1.0 + jnp.exp(-gate)) * upward).astype(bf16)

    loads[2].wait()
    for c in range(4):
        cols = pl.ds(c * 1024, 1024)
        part = jnp.dot(hunits[...], wd[:, cols], preferred_element_type=f32)
        first, second = part[:64], part[64:]
        dsum[:, cols] = jnp.where(tp == 0, first, second)
        dp_send[c] = jnp.where(tp == 0, second, first).astype(bf16)
        remote(dp_send.at[c], dp_recv.at[c], dp_ss.at[0], dp_rs.at[c], partner)
    for c in range(4):
        settle(dp_recv.at[c], dp_rs.at[c])
        cols = pl.ds(c * 1024, 1024)
        dsum[:, cols] = dsum[:, cols] + dp_recv[c].astype(f32)
    for j in range(16):
        d_send[j] = dsum[4 * j : 4 * j + 4, :].astype(bf16)
    for k in ORDER[::-1]:
        remote(d_send.at[peer_of(x, y, k)], d_recv.at[k], d_ss.at[0], d_rs.at[0], dev(k))
    for c in range(nc):
        settle(xs[c], x_ss.at[c])
        settle(zs[c], z_ss.at[c])
    settle(qa1s.at[pl.ds(0, 3)], q_ss.at[0])
    settle(qb1s.at[pl.ds(0, 3)], q_ss.at[1])
    settle(qa2s.at[pl.ds(0, 3)], q_ss.at[2])
    settle(qb2s.at[pl.ds(0, 3)], q_ss.at[3])
    settle(qfa.at[pl.ds(0, 3), 0], a_ss.at[0])
    settle(qfb.at[pl.ds(0, 3), 0], a_ss.at[1])
    settle(qfa.at[:, pl.ds(0, 3)], a_ss.at[2])
    settle(qfb.at[pl.ds(0, 3)], a_ss.at[3])
    settle(stats.at[pl.ds(0, 15)], s_ss.at[0])
    settle(msend.at[pl.ds(0, 15)], m_ss.at[0])
    settle(w2.at[pl.ds(0, 128)], wp_ss.at[0])
    settle(msend, m_ss.at[1])
    settle(esend.at[pl.ds(0, 15)], m_ss.at[2])
    settle(esend, m_ss.at[3])
    settle(rs_send.at[pl.ds(1, 15)], rs_ss.at[0])
    settle(rs_send.at[pl.ds(1, 15)], ag_ss.at[0])
    settle(rs_send, fw_ss.at[0])
    settle(dp_send, dp_ss.at[0])
    for k in range(16):
        for t in range(2):
            cols = pl.ds(pl.multiple_of((source_of(x, y, k) * 2 + t) * 128, 128), 128)
            resrow[:, cols] = jnp.dot(pick, ag[k, t], preferred_element_type=f32)
    total = resrow[...][:4]
    own = jnp.zeros((4, 4096), f32)
    for j in range(16):
        own = jnp.where(kv == j, dsum[4 * j : 4 * j + 4, :], own)
    total = total + own
    settle(d_recv.at[pl.ds(1, 15)], d_rs.at[0])
    for k in ORDER:
        total = total + d_recv[k].astype(f32)
    out_ref[...] = total.astype(bf16)
    settle(d_send.at[pl.ds(0, 15)], d_ss.at[0])


def step(*operands):
    bf16, f32 = jnp.bfloat16, jnp.float32
    smem = pl.BlockSpec(memory_space=pltpu.SMEM)
    vmem = pl.BlockSpec(memory_space=pltpu.VMEM)
    hbm = pl.BlockSpec(memory_space=pl.ANY)
    dma = pltpu.SemaphoreType.DMA
    nc = len(PIECES)

    def chunk(*lead):
        return [pltpu.VMEM((*lead, tokens, 512), bf16) for _, _, tokens in PIECES]

    return pl.pallas_call(
        step_kernel,
        name="step",
        out_shape=(
            pltpu.VMEM((4, 4096), bf16),
            pltpu.VMEM((16, 2, 128, 512), bf16),
        ),
        in_specs=[smem] * 4 + [vmem] * 5 + [hbm] * 8,
        out_specs=(vmem, vmem),
        scratch_shapes=[
            pltpu.VMEM((256, 2048), bf16),
            pltpu.VMEM((8, 2, 512), bf16),
            pltpu.VMEM((8, 2, 128, 512), bf16),
            pltpu.VMEM((4, 32, 1152), f32),
            pltpu.VMEM((4, 32, 1152), f32),
            pltpu.VMEM((4, 8, 1152), f32),
            pltpu.VMEM((4, 8, 1152), f32),
            pltpu.VMEM((4, 4, 8, 1024), f32),
            pltpu.VMEM((4, 4, 8, 1024), f32),
            pltpu.VMEM((4, 8, 1024), f32),
            pltpu.VMEM((4, 8, 1024), f32),
            pltpu.VMEM((4, 4, 8, 8, 128), f32),
            pltpu.VMEM((4, 4, 8, 8, 128), f32),
            pltpu.VMEM((8, 2048), f32),
            pltpu.VMEM((24, 16, 128), f32),
            pltpu.VMEM((24, 16, 128), f32),
            pltpu.VMEM((16, 16, 512), f32),
            pltpu.VMEM((16, 16, 128), f32),
            pltpu.VMEM((16, 16, 128), f32),
            pltpu.VMEM((16, 40, 128), f32),
            pltpu.VMEM((16, 16, 128), bf16),
            pltpu.VMEM((16, 16, 128), bf16),
            pltpu.VMEM((2, 16, 32, 128), bf16),
            pltpu.VMEM((256, 2048), bf16),
            pltpu.VMEM((448, 4096), bf16),
            pltpu.VMEM((448, 4096), bf16),
            pltpu.VMEM((448, 4096), bf16),
            pltpu.VMEM((16, 128, 128), bf16),
            pltpu.VMEM((16, 128, 128), bf16),
            pltpu.VMEM((16, 2, 128, 128), bf16),
            pltpu.VMEM((128, 448), bf16),
            pltpu.VMEM((4, 64, 1024), bf16),
            pltpu.VMEM((4, 64, 1024), bf16),
            pltpu.VMEM((64, 4096), f32),
            pltpu.VMEM((16, 4, 4096), bf16),
            pltpu.VMEM((16, 4, 4096), bf16),
            pltpu.VMEM((8, 4096), f32),
            pltpu.SMEM((48,), jnp.int32),
            *chunk(16), *chunk(15), *chunk(16), *chunk(3, 4), *chunk(4, 4),
            dma((2,)), dma((nc,)), dma((1,)),
            dma((4,)), dma((4,)), dma((4,)), dma((4,)),
            dma((nc,)), dma((nc,)), dma((nc,)), dma((nc,)),
            dma((1,)), dma((1,)), dma((4,)), dma((4,)),
            dma((4,)), dma((1,)), dma((1,)), dma((1,)), dma((1,)), dma((1,)), dma((16,)),
            dma((1,)), dma((16,)), dma((1,)), dma((4,)), dma((1,)), dma((1,)),
        ],
        compiler_params=pltpu.CompilerParams(
            collective_id=0, has_side_effects=True, vmem_limit_bytes=58 * 1024 * 1024
        ),
    )(*operands)


def per_device(
    hidden_states,
    attn_gain,
    mlp_gain,
    w_query,
    w_out,
    w_gate,
    w_up,
    w_down,
    kv_pool,
    resident_cache,
    resident_slot,
    resident_len,
    new_owner,
    new_local,
    new_slot,
    new_len,
    token_kv,
):
    mixed, new_pages = step(
        resident_slot,
        resident_len,
        new_slot,
        new_len,
        new_owner,
        new_local,
        hidden_states,
        attn_gain.reshape(1, 256),
        mlp_gain.reshape(1, 4096),
        token_kv,
        w_query,
        kv_pool.reshape(16, 256, 512),
        resident_cache[0],
        w_out.reshape(128, 4096),
        w_gate.T,
        w_up.T,
        w_down,
    )
    return (mixed, new_pages[None])


def solution(mesh):
    return jax.shard_map(
        per_device,
        mesh=mesh,
        in_specs=(
            P("grp", "kv"),
            P("kv"),
            P(),
            P("kv", "tp"),
            P("tp", "kv", None),
            P(None, KV_TP),
            P(None, KV_TP),
            P(KV_TP, None),
            P(GRP_KV, None, None, "tp"),
            P("grp", "kv", None, None, "tp"),
            P("grp", "kv"),
            P("grp", "kv"),
            P(),
            P(),
            P("grp", "kv"),
            P("grp", "kv"),
            P("grp", None, "tp"),
        ),
        out_specs=(P(GRP_KV_TP, None), P("grp", "kv", None, None, "tp")),
        check_vma=False,
    )
```
